32 devices in a mesh: dp: 8 (over z, x), ep: 4 (over y, core).
Axes of the slice: x: 2, y: 2, z: 4, core: 2. Of those that a mesh axis runs over, the one named last changes fastest.
Arguments:
- tokens: bfloat16 [64, 197, 768], P(('dp', 'ep')), may hold values from -6 to 6
- live_images: int32 [32], P(('dp', 'ep')), may hold values from 1 to 2, as said below
- routes: int32 [64, 197, 2], P(('dp', 'ep')), may hold values from 0 to 3, all different within a row; in each aligned block of 394 rows (0 to 393, 394 to 787, ..., all dimensions but the last counted through in order) at most 248 rows name the same one
- ln1_gain: float32 [768], replicated, may hold values from 0.1 to 1.9
- ln1_bias: float32 [768], replicated, may hold values from -3 to 3
- query_key_value_weight: bfloat16 [768, 2304], replicated, may hold values from -0.21875 to 0.21875
- attention_output_weight: bfloat16 [768, 768], replicated, may hold values from -0.625 to 0.625
- ln2_gain: float32 [768], replicated, may hold values from 0.1 to 1.9
- ln2_bias: float32 [768], replicated, may hold values from -3 to 3
- w_router: bfloat16 [768, 4], replicated, may hold values from -0.4375 to 0.4375
- w_in: bfloat16 [4, 768, 3072], P('ep'), may hold values from -0.21875 to 0.21875
- w_out: bfloat16 [4, 3072, 768], P('ep'), may hold values from -0.875 to 0.875
- cotangent: bfloat16 [64, 197, 768], P(('dp', 'ep')), may hold values from -6 to 6
Outputs:
- block_out: bfloat16 [64, 197, 768], P(('dp', 'ep'))
- grad_tokens: float32 [64, 197, 768], P(('dp', 'ep'))
- grad_ln1_gain: float32 [768], P('ep')
- grad_ln1_bias: float32 [768], P('ep')
- grad_w_qkv: float32 [768, 2304], P('ep')
- grad_w_attn_out: float32 [768, 768], P('ep')
- grad_ln2_gain: float32 [768], P('ep')
- grad_ln2_bias: float32 [768], P('ep')
- grad_w_router: float32 [768, 4], P('ep')
- grad_w_in: float32 [4, 768, 3072], P('ep', 'dp')
- grad_w_out: float32 [4, 3072, 768], P('ep', 'dp')
The draws below stay inside these ranges and needn't reach their ends.
Inputs may be any that keep to these rules, and one draw needn't show every extreme that they name: Each device holds 2 image slots of which the first live_images are images; some device holds 2, some holds one. `routes`: each token names two different experts. Among the 394 tokens of one device, slots live or not, no expert is named more than 248 times, a bound that some block reaches.
All inputs are finite; a program needn't handle non-finite values.
Results may differ from the reference program's by a relative error of at most 0.024.
Values may be sent and summed in bfloat16 or wider, within the bound.
A program may use at most 192 MiB of HBM per device.

```python
import math
import jax
import jax.numpy as jnp
import numpy as np
from jax import lax

D = 768
HEADS = 12
HEAD_DIM = 64
F = 3072
SEQ = 197
SLOTS = 2
EXPERTS = 4
IMAGES = 64
CAP = 248
N_DP = 8
N_EP = 4


def draw_live_images(key, part):
    first_key, second_key = jax.random.split(jax.random.fold_in(key, 17))
    counts = jax.random.randint(first_key, (N_DP * N_EP,), 1, SLOTS + 1)
    order = jax.random.permutation(second_key, N_DP * N_EP)
    counts = counts.at[order[0]].set(SLOTS)
    counts = counts.at[order[1]].set(1)
    return counts.astype(jnp.int32)


def steps_of(stream_key, shape, shards, low, high):
    level = 1.0
    for dim, blocks in shards:
        draws = jax.random.uniform(jax.random.fold_in(jax.random.fold_in(stream_key, 6), dim), (blocks,), jnp.float32, low / len(shards), high / len(shards))
        level = level * jnp.repeat(jnp.exp(draws), shape[dim] // blocks).reshape((-1,) + (1,) * (len(shape) - 1 - dim))
    return level


def deal_out(rng, own, number, rows, amount, top, reach, lean):
    ranking = jax.random.permutation(rng, amount)
    heavy_load, usual = shares(amount, rows * top, reach, lean, True), shares(amount, rows * top, reach, lean, False)
    places = jnp.arange(amount)

    def named(sizes, turn):
        used = int((sizes > 0).sum())
        fixed = max(1, used // 4)
        passed = fixed + (places - fixed + turn * (used - fixed)) % max(1, amount - fixed)
        return jnp.zeros((amount,), jnp.int32).at[ranking[jnp.where(places < fixed, places, passed)]].set(jnp.asarray(sizes, jnp.int32))

    sizes = jnp.where(number % 4 == 0, named(heavy_load, number // 4), named(usual, number - number // 4 - 1))
    mixed = jax.random.permutation(jax.random.fold_in(own, 3), amount)
    giver, receiver = mixed[0:amount // 2 * 2:2], mixed[1:amount // 2 * 2:2]
    margin = jnp.minimum(sizes[giver] - 1, reach - sizes[receiver]) // 2
    margin = jnp.where((giver == ranking[0]) | (receiver == ranking[0]) | (sizes[receiver] == 0), 0, jnp.maximum(margin, 0))
    passed = jax.random.randint(jax.random.fold_in(own, 4), (amount // 2,), 0, 1 << 20) % (margin + 1)
    sizes = sizes.at[giver].add(-passed).at[receiver].add(passed)
    labels = jnp.searchsorted(jnp.cumsum(sizes), jnp.arange(rows * top), side="right").astype(jnp.int32)
    table = labels.reshape(top, rows).T
    table = table[jax.random.permutation(jax.random.fold_in(own, 1), rows)]
    turn = jax.random.randint(jax.random.fold_in(own, 2), (rows, 1), 0, top)
    return jnp.take_along_axis(table, (jnp.arange(top)[None, :] + turn) % top, axis=1)


def shares(amount, total, bound, slope, full):
    weights = [(1 << 20) // math.isqrt(grade ** slope) + 1 for grade in range(1, amount + 1)]
    largest = bound if full else min(bound, max(-(-total // amount), total * weights[0] // sum(weights)))
    least = 1 if total - largest >= amount - 1 else 0
    given, spare = [largest] + [least] * (amount - 1), total - largest - least * (amount - 1)
    while spare > 0:
        free = [i for i in range(1, amount) if given[i] < largest] or [i for i in range(1, amount) if given[i] < bound]
        whole, left = sum([weights[i] for i in free]), spare
        for i in free:
            extra = min(bound - given[i], max(1, left * weights[i] // whole), spare)
            given[i] = given[i] + extra
            spare = spare - extra
    return np.array(given)


def centred(own_key, extent, scale, most, shards=(), held_as=jnp.bfloat16):
    drawn = jax.random.normal(own_key, extent, jnp.float32) * scale
    if len(shards) > 0:
        drawn = steps_of(own_key, extent, shards, -0.22, 0.18) * drawn
    return jnp.clip(drawn, min=-most, max=most).astype(held_as)


def setup_inputs(seed: int = 0) -> dict:
    key_list = jax.random.split(jax.random.key(seed), 14)
    tokens = centred(key_list[0], (IMAGES, SEQ, D), 1.0, 6.0, ((0, 32),))
    live_images = draw_live_images(jax.random.fold_in(key_list[13], 71), 0)
    routes_keys = jax.random.split(jax.random.fold_in(key_list[2], 1), IMAGES * SEQ // (SLOTS * SEQ))
    routes_turns = jax.random.permutation(jax.random.fold_in(key_list[2], 3), IMAGES * SEQ // (SLOTS * SEQ))
    routes = jax.vmap(lambda own, number: deal_out(jax.random.fold_in(key_list[2], 2), own, number, SLOTS * SEQ, EXPERTS, 2, CAP, 2))(routes_keys, routes_turns).reshape((IMAGES, SEQ, 2))
    ln1_gain = jnp.clip(1.0 + 0.18 * jax.random.normal(key_list[3], (D,), jnp.float32), 0.1, 1.9)
    ln1_bias = centred(key_list[4], (D,), 0.5, 3.0, (), jnp.float32)
    query_key_value_weight = centred(key_list[5], (D, 3 * D), D ** -0.5, 0.21875)
    attention_output_weight = centred(key_list[6], (D, D), (D // 8) ** -0.5, 0.625)
    ln2_gain = jnp.clip(1.0 + 0.18 * jax.random.normal(key_list[7], (D,), jnp.float32), 0.1, 1.9)
    ln2_bias = centred(key_list[8], (D,), 0.5, 3.0, (), jnp.float32)
    w_router = centred(key_list[9], (D, EXPERTS), (D // 4) ** -0.5, 0.4375)
    w_in = centred(key_list[10], (EXPERTS, D, F), D ** -0.5, 0.21875, ((0, 4),))
    w_out = centred(key_list[11], (EXPERTS, F, D), (F // 64) ** -0.5, 0.875, ((0, 4),))
    cotangent = centred(key_list[12], (IMAGES, SEQ, D), 1.0, 6.0, ((0, 32),))
    return dict(tokens=tokens, live_images=live_images, routes=routes, ln1_gain=ln1_gain, ln1_bias=ln1_bias, query_key_value_weight=query_key_value_weight, attention_output_weight=attention_output_weight, ln2_gain=ln2_gain, ln2_bias=ln2_bias, w_router=w_router, w_in=w_in, w_out=w_out, cotangent=cotangent)


@jax.custom_vjp
def lowered_precision(v):
    return lax.optimization_barrier(v.astype(jnp.bfloat16)).astype(jnp.float32)

@jax.custom_vjp
def lowered_backward(v):
    return v

def low_keep(v):
    return (lowered_precision(v), None)

def low_pass(kept, grad):
    return (grad,)

def back_keep(v):
    return (v, None)

def back_low(kept, grad):
    return (lowered_precision(grad),)
lowered_precision.defvjp(low_keep, low_pass)
lowered_backward.defvjp(back_keep, back_low)
eps = 1e-06
highest_precision = lax.Precision.HIGHEST

def layer_norm(values, gain, bias):
    centre = lax.optimization_barrier(jnp.mean(values, axis=-1, keepdims=True))
    shifted = values - centre
    variance = lax.optimization_barrier(jnp.mean(shifted * shifted, axis=-1, keepdims=True))
    return shifted * lax.rsqrt(variance + eps) * gain + bias

def attention_block(image_batch, gain1, bias1, query_key_value_weight, attention_output_weight):
    number = image_batch.shape[0]
    normalized_input = lowered_precision(layer_norm(image_batch, gain1, bias1))
    query_key_value_rows = lowered_backward(lowered_precision(jnp.einsum('gpc,ch->gph', normalized_input, query_key_value_weight, precision=highest_precision)))
    qkv_heads = query_key_value_rows.reshape(number, SEQ, 3, HEADS, HEAD_DIM)
    queries = qkv_heads[:, :, 0]
    keys_all = qkv_heads[:, :, 1]
    values_all = qkv_heads[:, :, 2]
    scores = lowered_backward(jnp.einsum('sqhc,skhc->shqk', queries, keys_all, precision=highest_precision) * HEAD_DIM ** (-0.5))
    weights = lowered_precision(jax.nn.softmax(scores, axis=-1))
    attended_context = jnp.einsum('shqk,skhc->sqhc', weights, values_all, precision=highest_precision).reshape(number, SEQ, D)
    attended_context = lowered_backward(lowered_precision(attended_context))
    return image_batch + lowered_backward(jnp.einsum('gpc,ch->gph', attended_context, attention_output_weight, precision=highest_precision))

def expert_apply(packed):
    rows_in, first_w, second_w = packed
    pre_act = lowered_backward(jnp.dot(rows_in, first_w, precision=highest_precision))
    activated = lowered_precision(jax.nn.gelu(pre_act))
    return lowered_backward(lowered_precision(jnp.dot(activated, second_w, precision=highest_precision)))

def block(inputs, gain1, bias1, query_key_value_weight, attention_output_weight, gain2, bias2, w_router, w_in, w_out, live_images, routes):
    image_batch = inputs.shape[0]
    devices = live_images.shape[0]
    slot_count = image_batch // devices
    row_count = slot_count * SEQ
    total_rows = image_batch * SEQ
    expert_count = w_router.shape[1]
    groups = inputs.reshape(devices // 4, 4 * slot_count, SEQ, D)

    def attend(group):
        return attention_block(group, gain1, bias1, query_key_value_weight, attention_output_weight)
    hidden1 = lax.map(jax.checkpoint(attend), groups).reshape(total_rows, D)
    moe_in = lowered_precision(layer_norm(hidden1, gain2, bias2))
    logits = lowered_backward(jnp.dot(moe_in, w_router, precision=highest_precision))
    router = jax.nn.softmax(logits, axis=-1)
    chosen = routes.reshape(total_rows, 2).astype(jnp.int32)
    gates = jnp.take_along_axis(router, chosen, axis=1)
    token_index = jnp.arange(total_rows, dtype=jnp.int32)
    slot_of = token_index % row_count // SEQ
    token_live = (slot_of < jnp.repeat(live_images.astype(jnp.int32), row_count)).astype(jnp.float32)
    pair_ids = chosen.reshape(2 * total_rows)
    pair_live = jnp.repeat(token_live, 2) > 0.5
    expert_ids = jnp.arange(expert_count, dtype=jnp.int32)
    member = ((pair_ids[:, None] == expert_ids[None, :]) & pair_live[:, None]).astype(jnp.int32)
    member = member.reshape(devices, 2 * row_count, expert_count)
    position = lax.optimization_barrier(jnp.sum((jnp.cumsum(member, axis=1) - 1) * member, axis=-1)).reshape(2 * total_rows)
    device_of = jnp.arange(2 * total_rows, dtype=jnp.int32) // (2 * row_count)
    slot_index = device_of * CAP + position
    target = jnp.where(pair_live, pair_ids, expert_count)
    buffers = jnp.zeros((expert_count, devices * CAP, D), jnp.float32)
    buffers = buffers.at[target, slot_index].set(jnp.repeat(moe_in, 2, axis=0), mode='drop')
    buffers = lowered_backward(buffers)
    produced = lax.map(jax.checkpoint(expert_apply), (buffers, w_in, w_out))
    safe_target = jnp.minimum(target, expert_count - 1)
    safe_slot = jnp.where(pair_live, slot_index, 0)
    taken = produced[safe_target, safe_slot] * pair_live[:, None].astype(jnp.float32)
    taken = taken.reshape(total_rows, 2, D)
    mixture = lax.optimization_barrier(jnp.sum(gates[:, :, None] * taken, axis=1))
    result = (hidden1 + mixture) * token_live[:, None]
    return result.reshape(image_batch, SEQ, D)

def reference(tokens, live_images, routes, ln1_gain, ln1_bias, query_key_value_weight, attention_output_weight, ln2_gain, ln2_bias, w_router, w_in, w_out, cotangent):

    def forward(inputs, gain1, bias1, qkv_w, attn_w, gain2, bias2, router_w, first_w, second_w):
        return block(inputs, gain1, bias1, qkv_w, attn_w, gain2, bias2, router_w, first_w, second_w, live_images, routes)
    result, pull = jax.vjp(forward, tokens.astype(jnp.float32), ln1_gain.astype(jnp.float32), ln1_bias.astype(jnp.float32), query_key_value_weight.astype(jnp.float32), attention_output_weight.astype(jnp.float32), ln2_gain.astype(jnp.float32), ln2_bias.astype(jnp.float32), w_router.astype(jnp.float32), w_in.astype(jnp.float32), w_out.astype(jnp.float32))
    grads = pull(cotangent.astype(jnp.float32))
    return (result.astype(jnp.bfloat16), grads[0], grads[1], grads[2], grads[3], grads[4], grads[5], grads[6], grads[7], grads[8], grads[9])
```

```python
import functools

import jax
import jax.numpy as jnp
from jax import lax
from jax.experimental import pallas as pl
from jax.experimental.pallas import tpu as pltpu
from jax.sharding import PartitionSpec as P

HEADS = 12
HEAD_DIM = 64
MESH = pl.DeviceIdType.MESH
BF = jnp.bfloat16
F32 = jnp.float32
eps = 1e-06
NEG = -1e30
LP = 256


def dot(a, b):
    return jnp.dot(a, b, preferred_element_type=F32)


def dot_nt(a, b):
    return lax.dot_general(a, b, (((1,), (1,)), ((), ())), preferred_element_type=F32)


def dot_tn(a, b):
    return lax.dot_general(a, b, (((0,), (0,)), ((), ())), preferred_element_type=F32)


def lane(shape):
    return lax.broadcasted_iota(jnp.int32, shape, len(shape) - 1)


def sub(shape):
    return lax.broadcasted_iota(jnp.int32, shape, len(shape) - 2)


def norm_parts(v):
    centre = jnp.mean(v, axis=-1, keepdims=True)
    shifted = v - centre
    inverse = lax.rsqrt(jnp.mean(shifted * shifted, axis=-1, keepdims=True) + eps)
    return shifted * inverse, inverse


def norm_backward(y, n, inverse):
    middle = jnp.mean(y, axis=-1, keepdims=True)
    along = jnp.mean(y * n, axis=-1, keepdims=True)
    return (y - middle - n * along) * inverse


def forward_kernel(
    seq, experts, tok, cot, routes, live, g1, b1, wqkv, wo, g2, b2, wr,
    xb_o, a_o, qkv_o, c_o, h1_o, u_o, gl_o, lse_o, slot_o, wr_o, xs,
):
    slots, sp, width = xs.shape
    rows = slots * sp
    pad = sp - seq
    for i in range(slots):
        xs[i, :seq, :] = tok[i].astype(F32)
        xs[i, seq:, :] = jnp.zeros((pad, width), F32)
        xb_o[i, :seq, :] = tok[i]
        xb_o[i, seq:, :] = jnp.zeros((pad, width), BF)
        on = (live[0] > i).astype(F32)
        gl_o[i, :seq, :] = (cot[i].astype(F32) * on).astype(BF)
        gl_o[i, seq:, :] = jnp.zeros((pad, width), BF)
    wr_o[...] = jnp.zeros(wr_o.shape, BF)
    wr_o[:, :experts] = wr[...]

    shape = slot_o.shape[1:]
    before = (sub((LP, LP)) < lane((LP, LP))).astype(BF)
    base = jnp.zeros((shape[0], 1), F32)
    for i in range(slots):
        r = jnp.concatenate([routes[i], jnp.full((2, LP - seq), -1, jnp.int32)], axis=1)
        member = (r[0:1, :] == sub(shape)) | (r[1:2, :] == sub(shape))
        member = member & (live[0] > i)
        m = member.astype(F32)
        place = dot(m.astype(BF), before) + base
        slot_o[i] = jnp.where(member, place, -1.0)
        base = base + jnp.sum(m, axis=1, keepdims=True)

    for i in range(slots):
        n1, _ = norm_parts(xs[i])
        a_o[i] = (n1 * g1[...] + b1[...]).astype(BF)
    a = a_o[...].reshape(rows, width)
    for n in range(3):
        qkv_o[n] = dot(a, wqkv[:, n * width:(n + 1) * width]).astype(BF).reshape(slots, sp, width)

    low = lane((sp, 128)) < HEAD_DIM
    keys = lane((sp, sp)) < seq
    lse_o[...] = jnp.zeros(lse_o.shape, F32)

    def pair(h, carry):
        cols = pl.ds(pl.multiple_of(h * 128, 128), 128)
        for i in range(slots):
            q, k, v = qkv_o[0, i, :, cols], qkv_o[1, i, :, cols], qkv_o[2, i, :, cols]
            outs = []
            lse = lse_o[i]
            for half in range(2):
                mine = low if half == 0 else ~low
                s = dot_nt(jnp.where(mine, q, jnp.zeros_like(q)), k) * (HEAD_DIM ** -0.5)
                s = jnp.where(keys, s, NEG)
                top = jnp.max(s, axis=-1, keepdims=True)
                e = jnp.exp(s - top)
                total = jnp.sum(e, axis=-1, keepdims=True)
                lse = jnp.where(lane((sp, 128)) == 2 * h + half, top + jnp.log(total), lse)
                outs.append(dot((e / total).astype(BF), v))
            lse_o[i] = lse
            c_o[i, :, cols] = jnp.where(low, outs[0], outs[1]).astype(BF)
        return carry

    lax.fori_loop(0, width // 128, pair, 0)
    h1 = xs[...].reshape(rows, width) + dot(c_o[...].reshape(rows, width), wo[...])
    h1_o[...] = h1.reshape(slots, sp, width)
    for i in range(slots):
        n2, _ = norm_parts(h1_o[i])
        u_o[i] = (n2 * g2[...] + b2[...]).astype(BF)


def run_forward(tokens, live, routes, g1, b1, wqkv, wo, g2, b2, wr, cot):
    slots, seq, width = tokens.shape
    sp = (seq + 15) // 16 * 16
    experts = wr.shape[1]
    sds = jax.ShapeDtypeStruct
    tall = (slots, sp, width)
    vm = pl.BlockSpec(memory_space=pltpu.VMEM)
    return pl.pallas_call(
        functools.partial(forward_kernel, seq, experts),
        name="attention_forward",
        out_shape=(
            sds(tall, BF), sds(tall, BF), sds((3,) + tall, BF), sds(tall, BF), sds(tall, F32), sds(tall, BF), sds(tall, BF),
            sds((slots, sp, 128), F32), sds((slots, 8, LP), F32), sds((width, 128), BF),
        ),
        in_specs=[vm, vm, vm, pl.BlockSpec(memory_space=pltpu.SMEM)] + [vm] * 7,
        out_specs=[vm] * 10,
        scratch_shapes=[pltpu.VMEM(tall, F32)],
        compiler_params=pltpu.CompilerParams(vmem_limit_bytes=48 << 20),
    )(
        tokens, cot, jnp.transpose(routes, (0, 2, 1)), live,
        g1.reshape(1, width), b1.reshape(1, width), wqkv, wo,
        g2.reshape(1, width), b2.reshape(1, width), wr,
    )


COPIES = {}
for _name, _count in (
    ("uP", 2), ("uO", 2), ("uF", 2), ("sP", 1), ("sO", 1), ("sF", 1), ("gP", 2), ("gO", 2), ("gF", 2),
    ("ox", 4), ("oz", 3), ("ix", 4), ("iz", 12),
    ("dP", 2), ("dD", 2), ("dO", 2), ("eP", 1), ("eD", 1), ("eO", 1), ("yP", 2), ("yD", 2), ("yO", 2),
):
    COPIES[_name] = sum(n for _, n in COPIES.values()), _count
N_COPIES = sum(n for _, n in COPIES.values())


def expert_kernel(
    experts, seq, live, wr, g1, g2, u, gl, slot, w_in, w_out, xb, a, qkv, c, h1, lse, wqkv, wo,
    bo_o, DH, sm_o, wo_o, wi_o, sg_o,
    U, G, SL, WI, WO, M, D, X, GE, DT,
    GOs, GOk, GOx, GOz, GIs, GIk, GIx, GIz,
    H, LS, GD, RP, RD, RO, EP, ED, EO, ES, YP, YD, YO,
    ssem, rsem, lsem,
):
    f, width = WO.shape
    sp, rows, half_rows = 208, 416, 512
    dp, ep = lax.axis_index("dp"), lax.axis_index("ep")
    z, x = dp // 2, dp % 2
    y, core = ep // 2, ep % 2
    to_p = {"ep": y * 2 + 1 - core}
    to_o = {"ep": (1 - y) * 2 + core}
    to_x = {"dp": z * 2 + 1 - x}
    zs = [lax.rem(z + k, 4) for k in range(4)]
    to_z = [{"dp": zs[k] * 2 + x} for k in range(4)]

    def rc(name, i, src, dst, dev):
        at = COPIES[name][0] + i
        return pltpu.make_async_remote_copy(
            src_ref=src, dst_ref=dst, send_sem=ssem.at[at], recv_sem=rsem.at[at], device_id=dev, device_id_type=MESH)

    def lc(i, src, dst):
        return pltpu.make_async_copy(src, dst, lsem.at[i])

    top = pl.ds(0, sp)
    loads = [
        lc(0, u.at[0], U.at[0, 0, top]), lc(1, u.at[1], U.at[0, 1, top]), lc(2, slot, SL.at[0]),
        lc(3, gl.at[0], G.at[0, 0, top]), lc(4, gl.at[1], G.at[0, 1, top]),
        lc(5, w_in.at[0], WI), lc(6, w_out.at[0], WO), lc(7, h1, H), lc(25, lse, LS),
    ]
    for cp in loads:
        cp.start()

    barrier = pltpu.get_barrier_semaphore()
    for dev in (to_p, to_o, to_x, to_z[1], to_z[2], to_z[3]):
        pl.semaphore_signal(barrier, inc=1, device_id=dev, device_id_type=MESH)
    for s in range(4):
        for i in range(2):
            U[s, i, sp:, :] = jnp.zeros((LP - sp, width), BF)
            G[s, i, sp:, :] = jnp.zeros((LP - sp, width), BF)
    pl.semaphore_wait(barrier, 6)

    uP = [rc("uP", i, U.at[0, i, top], U.at[1, i, top], to_p) for i in range(2)]
    uO = [rc("uO", i, U.at[0, i, top], U.at[2, i, top], to_o) for i in range(2)]
    uF = [rc("uF", i, U.at[2, i, top], U.at[3, i, top], to_p) for i in range(2)]
    gP = [rc("gP", i, G.at[0, i, top], G.at[1, i, top], to_p) for i in range(2)]
    gO = [rc("gO", i, G.at[0, i, top], G.at[2, i, top], to_o) for i in range(2)]
    gF = [rc("gF", i, G.at[2, i, top], G.at[3, i, top], to_p) for i in range(2)]
    sP = rc("sP", 0, SL.at[0], SL.at[1], to_p)
    sO = rc("sO", 0, SL.at[0], SL.at[2], to_o)
    sF = rc("sF", 0, SL.at[2], SL.at[3], to_p)
    loads[2].wait()
    sO.start()
    sP.start()
    for i in range(2):
        loads[i].wait()
        uO[i].start()
        uP[i].start()
    for i in range(2):
        loads[3 + i].wait()
        gO[i].start()
        gP[i].start()

    def onehot(s):
        want = sub((LP, LP)).astype(F32)
        parts = [(want == SL[s, i, pl.ds(ep, 1), :]).astype(BF) for i in range(2)]
        return jnp.concatenate(parts, axis=1)

    def gather(s):
        got = dot(onehot(s), U[s].reshape(2 * LP, width))
        X[s * LP:(s + 1) * LP, :] = got.astype(BF)

    tile = 512
    tiles = f // tile
    c0 = 0.7978845608028654
    c1 = c0 * 0.044715

    def expert_in(first):
        rs = slice(first, first + half_rows)

        def step(n, carry):
            cols = pl.ds(pl.multiple_of(n * tile, tile), tile)
            v = dot(X[rs, :], WI[:, cols])
            w = v * v
            t = jnp.tanh(v * (c0 + c1 * w))
            h = 0.5 + 0.5 * t
            M[rs, cols] = (v * h).astype(BF)
            D[rs, cols] = (h + h * (1.0 - t) * (v * (c0 + 3.0 * c1 * w))).astype(BF)
            return carry

        lax.fori_loop(0, tiles, step, 0)
        r = dot(X[rs, :], wr[...])
        r = jnp.where(lane(r.shape) < experts, r, NEG)
        r = jnp.exp(r - jnp.max(r, axis=-1, keepdims=True))
        r = r / jnp.sum(r, axis=-1, keepdims=True)
        GD[rs, 0:1] = jnp.sum(jnp.where(lane(r.shape) == ep, r, 0.0), axis=-1, keepdims=True)

    gather(0)
    sP.wait_recv()
    for i in range(2):
        uP[i].wait_recv()
    gather(1)
    loads[5].wait()
    expert_in(0)
    sO.wait_recv()
    sF.start()
    for i in range(2):
        uO[i].wait_recv()
        uF[i].start()
    gather(2)
    sF.wait_recv()
    for i in range(2):
        uF[i].wait_recv()
    gather(3)
    for i in range(2):
        gP[i].wait_recv()
    for i in range(2):
        gO[i].wait_recv()
        gF[i].start()
    expert_in(half_rows)

    def gather_grads(s):
        rs = slice(s * LP, (s + 1) * LP)
        got = dot(onehot(s), G[s].reshape(2 * LP, width))
        GE[rs, :] = got.astype(BF)
        DT[:, rs] = jnp.transpose(GD[rs, 0:1] * got).astype(BF)

    gather_grads(0)
    gather_grads(1)
    gather_grads(2)
    for i in range(2):
        gF[i].wait_recv()
    gather_grads(3)

    def ox(t):
        return rc("ox", t, GOs.at[t], GOx.at[t], to_x)

    def oz(k):
        return rc("oz", k - 1, GOk.at[k - 1], GOz.at[k - 1], to_z[k])

    def ix(j):
        return rc("ix", j, GIs.at[j], GIx.at[j], to_x)

    def iz(j, k):
        return rc("iz", j * 3 + k - 1, GIk.at[j, zs[k]], GIz.at[k - 1, j], to_z[k])

    def w_out_tile(t, carry):
        zp = lax.rem(z + 1 + t, 4)
        r = dot(DT[...], M[:, pl.ds(pl.multiple_of(zp * width, width), width)])
        lo, hi = r[:, :width // 2], r[:, width // 2:]
        GOs[t] = jnp.where(x == 0, hi, lo).astype(BF)
        GOk[t] = jnp.where(x == 0, lo, hi).astype(BF)
        ox(t).start()
        return carry

    lax.fori_loop(0, 4, w_out_tile, 0)

    def take_o(t):
        ox(t).wait_recv()
        GOk[t] = (GOk[t].astype(F32) + GOx[t].astype(F32)).astype(BF)
        if t < 3:
            oz(t + 1).start()

    def take_i(j):
        ix(j).wait_recv()
        GIk[j] = (GIk[j].astype(F32) + GIx[j].astype(F32)).astype(BF)
        for k in range(1, 4):
            iz(j, k).start()

    loads[6].wait()
    GD[:, 1:2] = jnp.zeros((GD.shape[0], 1), F32)

    def expert_back(n, carry):
        cols = pl.ds(pl.multiple_of(n * tile, tile), tile)
        for first in (0, half_rows):
            rs = slice(first, first + half_rows)
            back = dot_nt(GE[rs, :], WO[cols, :])
            GD[rs, 1:2] += jnp.sum(back * M[rs, cols].astype(F32), axis=-1, keepdims=True)
            D[rs, cols] = (D[rs, cols].astype(F32) * (GD[rs, 0:1] * back)).astype(BF)
        return carry

    lax.fori_loop(0, tiles, expert_back, 0)

    dP = [rc("dP", i, U.at[1, i, top], RP.at[i], to_p) for i in range(2)]
    dD = [rc("dD", i, U.at[3, i, top], RD.at[i], to_p) for i in range(2)]
    dO = [rc("dO", i, U.at[2, i, top], RO.at[i], to_o) for i in range(2)]
    eP = rc("eP", 0, ES.at[1], EP, to_p)
    eD = rc("eD", 0, ES.at[3], ED, to_p)
    eO = rc("eO", 0, ES.at[2], EO, to_o)
    yP = [rc("yP", i, G.at[1, i, top], YP.at[i], to_p) for i in range(2)]
    yD = [rc("yD", i, G.at[3, i, top], YD.at[i], to_p) for i in range(2)]
    yO = [rc("yO", i, G.at[2, i, top], YO.at[i], to_o) for i in range(2)]

    for cp in uP + uO + uF:
        cp.wait_send()

    def scatter(s, values):
        return dot_tn(onehot(s), values)

    for s in (3, 2, 1, 0):
        rs = slice(s * LP, (s + 1) * LP)
        back = dot_nt(D[rs, :], WI[...]).astype(BF)
        out = scatter(s, back).astype(BF)
        if s == 0:
            for i in range(2):
                DH[i] = out[i * LP:i * LP + sp].astype(F32)
        else:
            U[s] = out.reshape(2, LP, width)
        dg = GD[rs, 1:2]
        hi = dg.astype(BF)
        low = (dg - hi.astype(F32)).astype(BF)
        at = lane((LP, 128))
        zero = jnp.zeros((LP, 128), BF)
        two = jnp.where(at == ep, hi, zero) + jnp.where(at == ep + 64, low, zero)
        ES[s] = scatter(s, two).astype(BF).reshape(2, LP, 128)
        if s == 3:
            for cp in dD + [eD]:
                cp.start()
        if s == 1:
            for cp in dP + [eP]:
                cp.start()
    for i in range(2):
        dD[i].wait_recv()
        U[2, i, :sp, :] = (U[2, i, :sp, :].astype(F32) + RD[i].astype(F32)).astype(BF)
        dO[i].start()
    eD.wait_recv()
    ES[2] = ES[2] + ED[...]
    eO.start()

    def w_in_tile(j, carry):
        r = dot_tn(X[...], D[:, pl.ds(pl.multiple_of(j * width, width), width)]).reshape(4, 2, width // 8, width)
        first, second = r[:, 0], r[:, 1]
        GIs[j] = jnp.where(x == 0, second, first).astype(BF)
        GIk[j] = jnp.where(x == 0, first, second).astype(BF)
        ix(j).start()
        return carry

    lax.fori_loop(0, 4, w_in_tile, 0)
    take_o(0)

    for cp in gP + gO + gF:
        cp.wait_send()
    for s in (3, 2, 1):
        rs = slice(s * LP, (s + 1) * LP)
        o = dot(M[rs, :], WO[...]).astype(BF).astype(F32)
        G[s] = scatter(s, (GD[rs, 0:1] * o).astype(BF)).astype(BF).reshape(2, LP, width)
        if s == 3:
            for cp in yD:
                cp.start()
        if s == 1:
            for cp in yP:
                cp.start()
    o = dot(M[0:LP, :], WO[...]).astype(BF).astype(F32)
    X[0:half_rows, :] = scatter(0, (GD[0:LP, 0:1] * o).astype(BF)).astype(BF)
    for i in range(2):
        yD[i].wait_recv()
        G[2, i, :sp, :] = (G[2, i, :sp, :].astype(F32) + YD[i].astype(F32)).astype(BF)
        yO[i].start()
    take_o(1)

    late = [lc(8 + n, wqkv.at[:, pl.ds(n * width, width)], WO.at[pl.ds(n * width, width)]) for n in range(3)]
    late.append(lc(11, wo, WO.at[pl.ds(3 * width, width)]))
    at = 12
    for i in range(2):
        r0 = pl.ds(i * sp, sp)
        for n in range(3):
            late.append(lc(at + n, qkv.at[n, i], M.at[r0, pl.ds(n * width, width)]))
        late.append(lc(at + 3, a.at[i], M.at[r0, pl.ds(3 * width, width)]))
        late.append(lc(at + 4, c.at[i], M.at[pl.ds(rows + i * sp, sp), pl.ds(0, width)]))
        late.append(lc(at + 5, xb.at[i], GE.at[pl.ds(rows + i * sp, sp)]))
        at += 6
    for cp in late:
        cp.start()
    loads[7].wait()
    loads[8].wait()

    for i in range(2):
        dP[i].wait_recv()
        dO[i].wait_recv()
    eP.wait_recv()
    eO.wait_recv()
    router = jnp.zeros((width, 128), F32)
    gain2 = jnp.zeros((1, width), F32)
    bias2 = jnp.zeros((1, width), F32)
    for i in range(2):
        du = DH[i] + RP[i].astype(F32) + RO[i].astype(F32)
        back = ES[0, i, :sp, :].astype(F32) + EP[i, :sp, :].astype(F32) + EO[i, :sp, :].astype(F32)
        back = back + pltpu.roll(back, 64, axis=1)
        own = U[0, i, :sp, :]
        r = dot(own, wr[...])
        r = jnp.where(lane(r.shape) < experts, r, NEG)
        r = jnp.exp(r - jnp.max(r, axis=-1, keepdims=True))
        r = r / jnp.sum(r, axis=-1, keepdims=True)
        dl = (r * (back - jnp.sum(r * back, axis=-1, keepdims=True))).astype(BF)
        router = router + dot_tn(own, dl)
        du = du + dot_nt(dl, wr[...])
        n2, inv2 = norm_parts(H[i])
        gain2 = gain2 + jnp.sum(du * n2, axis=0, keepdims=True)
        bias2 = bias2 + jnp.sum(du, axis=0, keepdims=True)
        dh = G[0, i, :sp, :].astype(F32) + norm_backward(du * g2[...], n2, inv2)
        DH[i] = dh
        GE[i * sp:(i + 1) * sp, :] = dh.astype(BF)

    for cp in late:
        cp.wait()
    X[half_rows:half_rows + rows, :] = dot_nt(GE[0:rows, :], WO[3 * width:, :]).astype(BF)
    WI[:, 3 * width:] = dot_tn(M[rows:2 * rows, 0:width], GE[0:rows, :]).astype(BF)
    take_o(2)

    low = lane((sp, 128)) < HEAD_DIM
    keys = lane((sp, sp)) < seq
    scaling = HEAD_DIM ** -0.5

    def pair(h, carry):
        def cols(n):
            return pl.ds(pl.multiple_of(h * 128 + n * width, 128), 128)

        for i in range(2):
            r0 = slice(i * sp, (i + 1) * sp)
            q, k, v = M[r0, cols(0)], M[r0, cols(1)], M[r0, cols(2)]
            dc = X[half_rows + i * sp:half_rows + (i + 1) * sp, cols(0)]
            parts = []
            for side in range(2):
                mine = low if side == 0 else ~low
                zero = jnp.zeros_like(q)
                lse_col = jnp.sum(jnp.where(lane((sp, 128)) == 2 * h + side, LS[i], 0.0), axis=-1, keepdims=True)
                s = dot_nt(jnp.where(mine, q, zero), k) * scaling
                p = jnp.exp(jnp.where(keys, s, NEG) - lse_col)
                dv = dot_tn(p.astype(BF), dc)
                dp_ = dot_nt(jnp.where(mine, dc, zero), v)
                ds = (p * (dp_ - jnp.sum(p * dp_, axis=-1, keepdims=True))).astype(BF)
                dq = dot(ds, k) * scaling
                dk = dot_tn(ds, q) * scaling
                parts.append((dq, dk, dv))
            r1 = slice(rows + i * sp, rows + (i + 1) * sp)
            for n in range(3):
                M[r1, cols(n + 1)] = jnp.where(low, parts[0][n], parts[1][n]).astype(BF)
        return carry

    lax.fori_loop(0, width // 128, pair, 0)
    take_o(3)
    take_i(0)

    da = jnp.zeros((rows, width), F32)
    for n in range(3):
        grads = M[rows:2 * rows, (n + 1) * width:(n + 2) * width]
        WI[:, n * width:(n + 1) * width] = dot_tn(M[0:rows, 3 * width:], grads).astype(BF)
        da = da + dot_nt(grads, WO[n * width:(n + 1) * width, :])
    out_sg = lc(at, WI, sg_o)
    out_sg.start()
    gain1 = jnp.zeros((1, width), F32)
    bias1 = jnp.zeros((1, width), F32)
    for i in range(2):
        grad = da[i * sp:(i + 1) * sp]
        n1, inv1 = norm_parts(GE[rows + i * sp:rows + (i + 1) * sp, :].astype(F32))
        gain1 = gain1 + jnp.sum(grad * n1, axis=0, keepdims=True)
        bias1 = bias1 + jnp.sum(grad, axis=0, keepdims=True)
        DH[i] = DH[i] + norm_backward(grad * g1[...], n1, inv1)
    vectors = jnp.concatenate([jnp.zeros((4, width), F32), gain1, bias1, gain2, bias2], axis=0)
    vectors = jnp.concatenate([vectors, jnp.zeros((120, width), F32)], axis=0)
    sm_o[...] = (router + jnp.transpose(vectors)).astype(BF)

    for i in range(2):
        yP[i].wait_recv()
        yO[i].wait_recv()
        on = (live[0] > i).astype(F32)
        mix = X[i * LP:i * LP + sp, :].astype(F32) + YP[i].astype(F32) + YO[i].astype(F32)
        bo_o[i] = ((H[i] + mix) * on).astype(BF)

    for j in range(1, 4):
        take_i(j)
    for k in range(1, 4):
        oz(k).wait_recv()
    total = GOk[3].astype(F32)
    for k in range(3):
        total = total + GOz[k].astype(F32)
    GOk[3] = total.astype(BF)
    out_wo = lc(0, GOk.at[3], wo_o)
    out_wo.start()
    outs = [out_wo, out_sg]
    for j in range(4):
        for k in range(1, 4):
            iz(j, k).wait_recv()
        total = GIk[j, z].astype(F32)
        for k in range(3):
            total = total + GIz[k, j].astype(F32)
        GIx[j, 0] = total.astype(BF)
        out_wi = lc(1 + j, GIx.at[j, 0], wi_o.at[:, pl.ds(j * width, width)])
        out_wi.start()
        outs.append(out_wi)
    for cp in gP[:0] + dP + dD + dO + yP + yD + yO + [sP, sO, sF, eP, eD, eO]:
        cp.wait_send()
    for t in range(4):
        ox(t).wait_send()
        ix(t).wait_send()
        for k in range(1, 4):
            iz(t, k).wait_send()
    for k in range(1, 4):
        oz(k).wait_send()
    for cp in outs:
        cp.wait()


def run_experts(n_ep, seq, saved, live, w_in, w_out, wqkv, wo, g1, g2):
    xb, a, qkv, c, h1, u, gl, lse, slot, wr = saved
    slots, sp, width = u.shape
    f = w_in.shape[2]
    sds = jax.ShapeDtypeStruct
    vm = pl.BlockSpec(memory_space=pltpu.VMEM)
    anys = pl.BlockSpec(memory_space=pl.ANY)
    b = lambda *shape: pltpu.VMEM(shape, BF)
    g = lambda *shape: pltpu.VMEM(shape, F32)
    cap = n_ep * LP
    return pl.pallas_call(
        functools.partial(expert_kernel, n_ep, seq),
        name="experts",
        out_shape=(
            sds((slots, sp, width), BF), sds((slots, sp, width), F32), sds((width, 128), BF),
            sds((width, f // 8), BF), sds((width // 8, f), BF), sds((width, 4 * width), BF),
        ),
        in_specs=[pl.BlockSpec(memory_space=pltpu.SMEM)] + [vm] * 3 + [anys] * 13,
        out_specs=[vm] * 3 + [anys] * 3,
        scratch_shapes=[
            b(4, 2, LP, width), b(4, 2, LP, width), g(4, 2, 8, LP), b(width, f), b(f, width),
            b(cap, f), b(cap, f), b(cap, width), b(cap, width), b(width, cap),
            b(4, width, f // 8), b(4, width, f // 8), b(4, width, f // 8), b(3, width, f // 8),
            b(4, 4, width // 8, width), b(4, 4, width // 8, width), b(4, 4, width // 8, width),
            b(3, 4, width // 8, width),
            g(slots, sp, width), g(slots, sp, 128), g(cap, 2),
            b(2, sp, width), b(2, sp, width), b(2, sp, width),
            b(2, LP, 128), b(2, LP, 128), b(2, LP, 128), b(4, 2, LP, 128),
            b(2, sp, width), b(2, sp, width), b(2, sp, width),
            pltpu.SemaphoreType.DMA((N_COPIES,)), pltpu.SemaphoreType.DMA((N_COPIES,)),
            pltpu.SemaphoreType.DMA((26,)),
        ],
        compiler_params=pltpu.CompilerParams(
            collective_id=0, has_side_effects=True, vmem_limit_bytes=67043328),
    )(live, wr, g1.reshape(1, width), g2.reshape(1, width), u, gl, slot, w_in, w_out, xb, a, qkv, c, h1, lse, wqkv, wo)


def fast_body(n_ep, tokens, live, routes, g1, b1, wqkv, wo, g2, b2, wr, w_in, w_out, cot):
    slots, seq, width = tokens.shape
    saved = run_forward(tokens, live, routes, g1, b1, wqkv, wo, g2, b2, wr, cot)
    bo, gt, sm, wo_t, wi, sg = run_experts(n_ep, seq, saved, live, w_in, w_out, wqkv, wo, g1, g2)
    sg = lax.psum_scatter(sg, "ep", scatter_dimension=0, tiled=True)
    sm = lax.psum_scatter(sm, "ep", scatter_dimension=0, tiled=True)
    sg = lax.psum(sg, "dp").astype(F32)
    sm = lax.psum(sm, "dp").astype(F32)
    return (
        bo[:, :seq], gt[:, :seq], sm[:, 4], sm[:, 5], sg[:, :3 * width], sg[:, 3 * width:],
        sm[:, 6], sm[:, 7], sm[:, :n_ep], wi.astype(F32)[None], jnp.transpose(wo_t).astype(F32)[None],
    )


def general_body(
    tokens,
    live_images,
    routes,
    ln1_gain,
    ln1_bias,
    query_key_value_weight,
    attention_output_weight,
    ln2_gain,
    ln2_bias,
    w_router,
    w_in,
    w_out,
    cotangent,
):
    slot_count, seq_len, model_width = tokens.shape
    row_count = slot_count * seq_len
    expert_count = w_router.shape[1]
    hidden_width = w_in.shape[2]
    capacity = ((2 * row_count + expert_count - 1) // expert_count * 5 // 4 + 7) // 8 * 8
    scaling = HEAD_DIM ** (-0.5)
    inputs = tokens.astype(jnp.float32).reshape(row_count, model_width)
    normed1, inverse1 = norm_parts(inputs)
    attn_in = (normed1 * ln1_gain + ln1_bias).astype(jnp.bfloat16)
    qkv_rows = jnp.dot(attn_in, query_key_value_weight, preferred_element_type=jnp.float32).astype(
        jnp.bfloat16
    )
    qkv_heads = qkv_rows.reshape(slot_count, seq_len, 3, HEADS, HEAD_DIM)
    queries = qkv_heads[:, :, 0]
    keys_all = qkv_heads[:, :, 1]
    values_all = qkv_heads[:, :, 2]
    scores = (
        jnp.einsum("sqhc,skhc->shqk", queries, keys_all, preferred_element_type=jnp.float32)
        * scaling
    )
    row_peak = jnp.max(scores, axis=-1, keepdims=True)
    raised = jnp.exp(scores - row_peak)
    totals = jnp.sum(raised, axis=-1, keepdims=True)
    log_total = row_peak + jnp.log(totals)
    weights = (raised / totals).astype(jnp.bfloat16)
    attended_context = jnp.einsum(
        "shqk,skhc->sqhc", weights, values_all, preferred_element_type=jnp.float32
    )
    attended_context = attended_context.astype(jnp.bfloat16).reshape(row_count, model_width)
    hidden1 = inputs + jnp.dot(
        attended_context, attention_output_weight, preferred_element_type=jnp.float32
    )
    normed2, inverse2 = norm_parts(hidden1)
    moe_in = (normed2 * ln2_gain + ln2_bias).astype(jnp.bfloat16)
    router = jax.nn.softmax(jnp.dot(moe_in, w_router, preferred_element_type=jnp.float32), axis=-1)
    chosen = routes.reshape(row_count, 2)
    expert_ids = jnp.arange(expert_count, dtype=jnp.int32)
    picked = (chosen[:, :, None] == expert_ids[None, None, :]).astype(jnp.float32)
    gates = jnp.sum(picked * router[:, None, :], axis=-1)
    token_live = (jnp.arange(row_count, dtype=jnp.int32) // seq_len < live_images[0]).astype(
        jnp.float32
    )
    pair_ids = chosen.reshape(2 * row_count)
    pair_live = jnp.repeat(token_live, 2) > 0.5
    member = ((pair_ids[:, None] == expert_ids[None, :]) & pair_live[:, None]).astype(jnp.int32)
    position = jnp.sum((jnp.cumsum(member, axis=0) - 1) * member, axis=-1)
    slot_ids = jnp.where(pair_live, pair_ids * capacity + position, -1).reshape(row_count, 2)
    lanes = jnp.arange(expert_count * capacity, dtype=jnp.int32)
    placing = (jnp.transpose(slot_ids)[:, None, :] == lanes[None, :, None]).astype(jnp.bfloat16)
    outbox = jnp.einsum("jsr,rd->sd", placing, moe_in, preferred_element_type=jnp.float32)
    outbox = outbox.astype(jnp.bfloat16).reshape(expert_count, capacity, model_width)
    inbox = lax.all_to_all(outbox, "ep", split_axis=0, concat_axis=0, tiled=True)
    flat_in = inbox.reshape(-1, model_width)
    pre_act = jnp.dot(flat_in, w_in[0], preferred_element_type=jnp.float32)
    activated = jax.nn.gelu(pre_act).astype(jnp.bfloat16)
    produced = jnp.dot(activated, w_out[0], preferred_element_type=jnp.float32).astype(jnp.bfloat16)
    coming_back = lax.all_to_all(
        produced.reshape(inbox.shape), "ep", split_axis=0, concat_axis=0, tiled=True
    )
    coming_back, pre_act = (
        coming_back,
        pre_act.reshape(inbox.shape[0], inbox.shape[1], hidden_width),
    )
    arrived_rows = inbox.reshape(-1, model_width)
    pre_rows = pre_act.reshape(-1, hidden_width)
    returned_rows = coming_back.reshape(expert_count * capacity, model_width)
    taken = jnp.einsum("jsr,sd->rjd", placing, returned_rows, preferred_element_type=jnp.float32)
    mixture = jnp.sum(gates[:, :, None] * taken, axis=1)
    block_out = (
        ((hidden1 + mixture) * token_live[:, None]).astype(jnp.bfloat16).reshape(tokens.shape)
    )
    upstream = cotangent.astype(jnp.float32).reshape(row_count, model_width) * token_live[:, None]
    gate_grads = jnp.sum(taken * upstream[:, None, :], axis=-1)
    sent_grads = (gates[:, :, None] * upstream[:, None, :]).astype(jnp.bfloat16)
    grad_outbox = jnp.einsum("jsr,rjd->sd", placing, sent_grads, preferred_element_type=jnp.float32)
    grad_outbox = grad_outbox.astype(jnp.bfloat16).reshape(expert_count, capacity, model_width)
    grad_inbox = lax.all_to_all(grad_outbox, "ep", split_axis=0, concat_axis=0, tiled=True)
    grad_rows = grad_inbox.reshape(-1, model_width)
    activated_rows, gelu_pull = jax.vjp(jax.nn.gelu, pre_rows)
    activated_low = activated_rows.astype(jnp.bfloat16)
    grad_activated = jnp.einsum(
        "rd,fd->rf", grad_rows, w_out[0], preferred_element_type=jnp.float32
    )
    grad_pre = gelu_pull(grad_activated)[0].astype(jnp.bfloat16)
    columns = activated_low
    grad_w_out = lax.psum_scatter(
        jnp.einsum("rf,rd->fd", columns, grad_rows, preferred_element_type=jnp.float32).astype(
            jnp.bfloat16
        ),
        "dp",
        scatter_dimension=0,
        tiled=True,
    ).astype(jnp.float32)
    grad_back_rows = jnp.einsum(
        "rf,df->rd", grad_pre, w_in[0], preferred_element_type=jnp.float32
    ).astype(jnp.bfloat16)
    grad_back = lax.all_to_all(
        grad_back_rows.reshape(grad_inbox.shape), "ep", split_axis=0, concat_axis=0, tiled=True
    )
    columns = arrived_rows
    grad_w_in = lax.psum_scatter(
        jnp.einsum("rd,rf->df", columns, grad_pre, preferred_element_type=jnp.float32).astype(
            jnp.bfloat16
        ),
        "dp",
        scatter_dimension=0,
        tiled=True,
    ).astype(jnp.float32)
    grad_back_flat = grad_back.reshape(expert_count * capacity, model_width)
    expert_grad = jnp.einsum(
        "jsr,sd->rd", placing, grad_back_flat, preferred_element_type=jnp.float32
    )
    grad_router_probs = jnp.sum(gate_grads[:, :, None] * picked, axis=1)
    grad_logits = router * (
        grad_router_probs - jnp.sum(router * grad_router_probs, axis=-1, keepdims=True)
    )
    grad_logits = grad_logits.astype(jnp.bfloat16)
    grad_w_router = jnp.einsum("rd,re->de", moe_in, grad_logits, preferred_element_type=jnp.float32)
    grad_moe_in = expert_grad + jnp.einsum(
        "re,de->rd", grad_logits, w_router, preferred_element_type=jnp.float32
    )
    grad_ln2_gain = jnp.sum(grad_moe_in * normed2, axis=0)
    grad_ln2_bias = jnp.sum(grad_moe_in, axis=0)
    grad_hidden1 = upstream + norm_backward(grad_moe_in * ln2_gain, normed2, inverse2)
    grad_attn = grad_hidden1.astype(jnp.bfloat16)
    grad_w_attn_out = jnp.einsum(
        "rd,re->de", attended_context, grad_attn, preferred_element_type=jnp.float32
    )
    grad_context = jnp.einsum(
        "re,de->rd", grad_attn, attention_output_weight, preferred_element_type=jnp.float32
    )
    grad_context = grad_context.astype(jnp.bfloat16).reshape(slot_count, seq_len, HEADS, HEAD_DIM)
    again = (
        jnp.einsum("sqhc,skhc->shqk", queries, keys_all, preferred_element_type=jnp.float32)
        * scaling
    )
    probs_again = jnp.exp(again - log_total)
    probs_low = probs_again.astype(jnp.bfloat16)
    grad_values = jnp.einsum(
        "shqk,sqhc->skhc", probs_low, grad_context, preferred_element_type=jnp.float32
    )
    grad_probs = jnp.einsum(
        "sqhc,skhc->shqk", grad_context, values_all, preferred_element_type=jnp.float32
    )
    grad_scores = probs_again * (
        grad_probs - jnp.sum(probs_again * grad_probs, axis=-1, keepdims=True)
    )
    grad_scores = grad_scores.astype(jnp.bfloat16)
    grad_queries = (
        jnp.einsum("shqk,skhc->sqhc", grad_scores, keys_all, preferred_element_type=jnp.float32)
        * scaling
    )
    grad_keys = (
        jnp.einsum("shqk,sqhc->skhc", grad_scores, queries, preferred_element_type=jnp.float32)
        * scaling
    )
    grad_qkv = (
        jnp.stack([grad_queries, grad_keys, grad_values], axis=2)
        .astype(jnp.bfloat16)
        .reshape(row_count, 3 * model_width)
    )
    grad_w_qkv = jnp.einsum("rd,re->de", attn_in, grad_qkv, preferred_element_type=jnp.float32)
    grad_attn_in = jnp.einsum(
        "re,de->rd", grad_qkv, query_key_value_weight, preferred_element_type=jnp.float32
    )
    grad_ln1_gain = jnp.sum(grad_attn_in * normed1, axis=0)
    grad_ln1_bias = jnp.sum(grad_attn_in, axis=0)
    grad_inputs = grad_hidden1 + norm_backward(grad_attn_in * ln1_gain, normed1, inverse1)
    shared = (
        grad_w_qkv,
        grad_w_attn_out,
        grad_w_router,
        grad_ln1_gain,
        grad_ln1_bias,
        grad_ln2_gain,
        grad_ln2_bias,
    )
    partial_sums = (
        lax.psum_scatter(
            shared[0].astype(jnp.bfloat16), "ep", scatter_dimension=0, tiled=True
        ).astype(jnp.float32),
        lax.psum_scatter(
            shared[1].astype(jnp.bfloat16), "ep", scatter_dimension=0, tiled=True
        ).astype(jnp.float32),
        lax.psum_scatter(
            shared[2].astype(jnp.bfloat16), "ep", scatter_dimension=0, tiled=True
        ).astype(jnp.float32),
        lax.psum_scatter(
            shared[3].astype(jnp.bfloat16), "ep", scatter_dimension=0, tiled=True
        ).astype(jnp.float32),
        lax.psum_scatter(
            shared[4].astype(jnp.bfloat16), "ep", scatter_dimension=0, tiled=True
        ).astype(jnp.float32),
        lax.psum_scatter(
            shared[5].astype(jnp.bfloat16), "ep", scatter_dimension=0, tiled=True
        ).astype(jnp.float32),
        lax.psum_scatter(
            shared[6].astype(jnp.bfloat16), "ep", scatter_dimension=0, tiled=True
        ).astype(jnp.float32),
    )
    shares = (
        lax.psum(partial_sums[0].astype(jnp.bfloat16), "dp").astype(jnp.float32),
        lax.psum(partial_sums[1].astype(jnp.bfloat16), "dp").astype(jnp.float32),
        lax.psum(partial_sums[2].astype(jnp.bfloat16), "dp").astype(jnp.float32),
        lax.psum(partial_sums[3].astype(jnp.bfloat16), "dp").astype(jnp.float32),
        lax.psum(partial_sums[4].astype(jnp.bfloat16), "dp").astype(jnp.float32),
        lax.psum(partial_sums[5].astype(jnp.bfloat16), "dp").astype(jnp.float32),
        lax.psum(partial_sums[6].astype(jnp.bfloat16), "dp").astype(jnp.float32),
    )
    return (
        block_out,
        grad_inputs.reshape(tokens.shape),
        shares[3],
        shares[4],
        shares[0],
        shares[1],
        shares[5],
        shares[6],
        shares[2],
        grad_w_in[None],
        grad_w_out[None],
    )


def solution(mesh):
    in_specs = (
        P(("dp", "ep"), None, None),
        P(("dp", "ep")),
        P(("dp", "ep"), None, None),
        P(),
        P(),
        P(),
        P(),
        P(),
        P(),
        P(),
        P("ep", None, None),
        P("ep", None, None),
        P(("dp", "ep"), None, None),
    )
    out_specs = (
        P(("dp", "ep"), None, None),
        P(("dp", "ep"), None, None),
        P("ep"),
        P("ep"),
        P("ep", None),
        P("ep", None),
        P("ep"),
        P("ep"),
        P("ep", None),
        P("ep", "dp", None),
        P("ep", "dp", None),
    )
    n_dp, n_ep = mesh.shape["dp"], mesh.shape["ep"]
    body = functools.partial(fast_body, n_ep) if (n_dp, n_ep) == (8, 4) else general_body
    return jax.shard_map(body, mesh=mesh, in_specs=in_specs, out_specs=out_specs, check_vma=False)
```

```python
import contextlib
import functools

import jax
import jax.numpy as jnp
from jax import lax
from jax.experimental import pallas as pl
from jax.experimental.pallas import tpu as pltpu
from jax.sharding import PartitionSpec as P

HEADS = 12
HEAD_DIM = 64
MESH = pl.DeviceIdType.MESH
BF = jnp.bfloat16
F32 = jnp.float32
eps = 1e-06
NEG = -1e30
LP = 256


def dot(a, b):
    return jnp.dot(a, b, preferred_element_type=F32)


def dot_nt(a, b):
    return lax.dot_general(a, b, (((1,), (1,)), ((), ())), preferred_element_type=F32)


def dot_tn(a, b):
    return lax.dot_general(a, b, (((0,), (0,)), ((), ())), preferred_element_type=F32)


def lane(shape):
    return lax.broadcasted_iota(jnp.int32, shape, len(shape) - 1)


def sub(shape):
    return lax.broadcasted_iota(jnp.int32, shape, len(shape) - 2)


def norm_parts(v):
    centre = jnp.mean(v, axis=-1, keepdims=True)
    shifted = v - centre
    inverse = lax.rsqrt(jnp.mean(shifted * shifted, axis=-1, keepdims=True) + eps)
    return shifted * inverse, inverse


def norm_backward(y, n, inverse):
    middle = jnp.mean(y, axis=-1, keepdims=True)
    along = jnp.mean(y * n, axis=-1, keepdims=True)
    return (y - middle - n * along) * inverse


def sc(name):
    return contextlib.nullcontext()


COPIES = {}
for _name, _count in (
    ("uP", 2), ("uO", 2), ("uF", 2), ("sP", 1), ("sO", 1), ("sF", 1), ("gP", 2), ("gO", 2), ("gF", 2),
    ("ox", 4), ("oz", 3), ("ix", 4), ("iz", 12),
    ("dP", 2), ("dD", 2), ("dO", 2), ("eP", 1), ("eD", 1), ("eO", 1), ("yP", 2), ("yD", 2), ("yO", 2),
    ("C", 8), ("Y", 4), ("X", 4), ("Z", 12), ("AZ", 12), ("AX", 4), ("mC", 2), ("mY", 1), ("mX", 1), ("mZ", 3),
):
    COPIES[_name] = sum(n for _, n in COPIES.values()), _count
N_COPIES = sum(n for _, n in COPIES.values())


def layer_kernel(
    experts, seq, live, routes, gains, wrt, xb, gl, w_in, w_out, wqkv, wo,
    bo_o, DH, sm_o, wo_o, wi_o, sg_o, qa_h, c_h,
    U, G, SL, WR, WI, WO, M, D, X, GE, DT,
    GOs, GOk, GOx, GOz, GIs, GIk, GIx, GIz,
    H, LS, GD, RP, RD, RO, EP, ED, EO, ES, YP, YD, YO, SM, SMx,
    ssem, rsem, lsem, free,
):
    f, width = WO.shape
    sp, rows, half_rows = 208, 416, 512
    shard, block = width // 4, width // 16
    dp, ep = lax.axis_index("dp"), lax.axis_index("ep")
    z, x = dp // 2, dp % 2
    y, core = ep // 2, ep % 2
    to_p = {"ep": y * 2 + 1 - core}
    to_o = {"ep": (1 - y) * 2 + core}
    to_x = {"dp": z * 2 + 1 - x}
    zs = [lax.rem(z + k, 4) for k in range(4)]
    to_z = [{"dp": zs[k] * 2 + x} for k in range(4)]
    friends = (to_p, to_o, to_x, to_z[1], to_z[2], to_z[3])
    g1, b1, g2, b2 = (gains[n:n + 1, :] for n in range(4))

    def rc(name, i, src, dst, dev):
        at = COPIES[name][0] + i
        return pltpu.make_async_remote_copy(
            src_ref=src, dst_ref=dst, send_sem=ssem.at[at], recv_sem=rsem.at[at], device_id=dev, device_id_type=MESH)

    def lc(i, src, dst):
        return pltpu.make_async_copy(src, dst, lsem.at[i])

    top = pl.ds(0, sp)
    barrier = pltpu.get_barrier_semaphore()
    for dev in friends:
        pl.semaphore_signal(barrier, inc=1, device_id=dev, device_id_type=MESH)

    def attention_weights(first):
        cps = [lc(first + n, wqkv.at[:, pl.ds(n * width, width)], WO.at[pl.ds(n * width, width)]) for n in range(3)]
        return cps + [lc(first + 3, wo, WO.at[pl.ds(3 * width, width)])]

    load_x = [lc(i, xb.at[i], GE.at[pl.ds(i * sp, sp)]) for i in range(2)]
    load_w = attention_weights(2)
    load_g = [lc(6 + i, gl.at[i], G.at[0, i, top]) for i in range(2)]
    load_in = lc(8, w_in.at[0], WI)
    for cp in load_x + load_w + load_g + [load_in]:
        cp.start()

    shape = SL.shape[2:]
    before = (sub((LP, LP)) < lane((LP, LP))).astype(BF)
    base = jnp.zeros((shape[0], 1), F32)
    for i in range(2):
        r = jnp.concatenate([routes[i], jnp.full((2, LP - seq), -1, jnp.int32)], axis=1)
        member = (r[0:1, :] == sub(shape)) | (r[1:2, :] == sub(shape))
        member = member & (live[0] > i)
        m = member.astype(F32)
        place = dot(m.astype(BF), before) + base
        SL[0, i] = jnp.where(member, place, -1.0)
        base = base + jnp.sum(m, axis=1, keepdims=True)
    WR[...] = jnp.zeros(WR.shape, BF)
    WR[0:experts, :] = wrt[...]
    for s in range(4):
        for i in range(2):
            U[s, i, sp:, :] = jnp.zeros((LP - sp, width), BF)
            G[s, i, sp:, :] = jnp.zeros((LP - sp, width), BF)

    uP = [rc("uP", i, U.at[0, i, top], U.at[1, i, top], to_p) for i in range(2)]
    uO = [rc("uO", i, U.at[0, i, top], U.at[2, i, top], to_o) for i in range(2)]
    uF = [rc("uF", i, U.at[2, i, top], U.at[3, i, top], to_p) for i in range(2)]
    gP = [rc("gP", i, G.at[0, i, top], G.at[1, i, top], to_p) for i in range(2)]
    gO = [rc("gO", i, G.at[0, i, top], G.at[2, i, top], to_o) for i in range(2)]
    gF = [rc("gF", i, G.at[2, i, top], G.at[3, i, top], to_p) for i in range(2)]
    sP = rc("sP", 0, SL.at[0], SL.at[1], to_p)
    sO = rc("sO", 0, SL.at[0], SL.at[2], to_o)
    sF = rc("sF", 0, SL.at[2], SL.at[3], to_p)

    low = lane((sp, 128)) < HEAD_DIM
    keys = lane((sp, sp)) < seq
    scaling = HEAD_DIM ** -0.5
    with sc("ln1"):
        for i in range(2):
            load_x[i].wait()
            r0 = slice(i * sp, (i + 1) * sp)
            n1, _ = norm_parts(GE[r0, :].astype(F32))
            D[r0, 3 * width:] = (n1 * g1 + b1).astype(BF)
    with sc("qkv"):
        for n in range(3):
            load_w[n].wait()
            D[0:rows, n * width:(n + 1) * width] = dot(
                D[0:rows, 3 * width:], WO[n * width:(n + 1) * width, :]).astype(BF)
    with sc("barrier"):
        pl.semaphore_wait(barrier, 6)
    sO.start()
    sP.start()
    load_g[0].wait()
    gO[0].start()
    gP[0].start()
    LS[...] = jnp.zeros(LS.shape, F32)

    def attend(i, per):
        r0 = slice(i * sp, (i + 1) * sp)

        def pair(step, carry):
            lse = LS[i]
            for inner in range(per):
                h = step * per + inner

                def cols(n):
                    return pl.ds(pl.multiple_of(h * 128 + n * width, 128), 128)

                q, k, v = D[r0, cols(0)], D[r0, cols(1)], D[r0, cols(2)]
                outs = []
                for side in range(2):
                    mine = low if side == 0 else ~low
                    s = dot_nt(jnp.where(mine, q, jnp.zeros_like(q)), k) * scaling
                    s = jnp.where(keys, s, NEG)
                    peak = jnp.max(s, axis=-1, keepdims=True)
                    e = jnp.exp(s - peak)
                    total = jnp.sum(e, axis=-1, keepdims=True)
                    lse = jnp.where(lane((sp, 128)) == 2 * h + side, peak + jnp.log(total), lse)
                    outs.append(dot((e / total).astype(BF), v))
                D[rows + i * sp:rows + (i + 1) * sp, cols(0)] = jnp.where(low, outs[0], outs[1]).astype(BF)
            LS[i] = lse
            return carry

        lax.fori_loop(0, width // 128 // per, pair, 0)

    for i in range(2):
        with sc("attend"):
            attend(i, 2)
        with sc("proj_ln2"):
            if i == 0:
                load_w[3].wait()
            r1 = slice(rows + i * sp, rows + (i + 1) * sp)
            h1 = GE[i * sp:(i + 1) * sp, :].astype(F32) + dot(D[r1, 0:width], WO[3 * width:, :])
            H[i] = h1
            n2, _ = norm_parts(h1)
            U[0, i, :sp, :] = (n2 * g2 + b2).astype(BF)
        uO[i].start()
        uP[i].start()
    load_g[1].wait()
    gO[1].start()
    gP[1].start()
    keep = [lc(0, D.at[pl.ds(0, rows)], qa_h), lc(1, D.at[pl.ds(rows, rows), pl.ds(0, width)], c_h)]
    load_out = lc(2, w_out.at[0], WO)
    for cp in keep + [load_out]:
        cp.start()

    def onehot(s):
        want = sub((LP, LP)).astype(F32)
        parts = [(want == SL[s, i, pl.ds(ep, 1), :]).astype(BF) for i in range(2)]
        return jnp.concatenate(parts, axis=1)

    def gather(s):
        X[s * LP:(s + 1) * LP, :] = dot(onehot(s), U[s].reshape(2 * LP, width)).astype(BF)

    tile = 512
    tiles = f // tile
    c0 = 0.7978845608028654
    c1 = c0 * 0.044715

    def expert_in(first):
        rs = slice(first, first + half_rows)

        def step(n, carry):
            cols = pl.ds(pl.multiple_of(n * tile, tile), tile)
            v = dot(X[rs, :], WI[:, cols])
            w = v * v
            t = jnp.tanh(v * (c0 + c1 * w))
            h = 0.5 + 0.5 * t
            M[rs, cols] = (v * h).astype(BF)
            D[rs, cols] = (h + h * (1.0 - t) * (v * (c0 + 3.0 * c1 * w))).astype(BF)
            return carry

        lax.fori_loop(0, tiles, step, 0)
        r = dot_nt(X[rs, :], WR[...])
        r = jnp.where(lane(r.shape) < experts, r, NEG)
        r = jnp.exp(r - jnp.max(r, axis=-1, keepdims=True))
        r = r / jnp.sum(r, axis=-1, keepdims=True)
        GD[rs, 0:1] = jnp.sum(jnp.where(lane(r.shape) == ep, r, 0.0), axis=-1, keepdims=True)

    def gather_grads(s):
        rs = slice(s * LP, (s + 1) * LP)
        got = dot(onehot(s), G[s].reshape(2 * LP, width))
        GE[rs, :] = got.astype(BF)
        DT[:, rs] = jnp.transpose(GD[rs, 0:1] * got).astype(BF)

    with sc("wait_uP"):
        gather(0)
        sP.wait_recv()
        for i in range(2):
            uP[i].wait_recv()
        gather(1)
        load_in.wait()
        for cp in keep:
            cp.wait()
    with sc("expert_in_0"):
        expert_in(0)
    with sc("wait_g0"):
        sO.wait_recv()
        sF.start()
        gO[0].wait_recv()
        gF[0].start()
    with sc("wait_uO"):
        for i in range(2):
            uO[i].wait_recv()
            uF[i].start()
        gather(2)
    with sc("wait_uF"):
        sF.wait_recv()
        for i in range(2):
            uF[i].wait_recv()
        gather(3)
    with sc("expert_in_1"):
        expert_in(half_rows)
    with sc("wait_gP"):
        for i in range(2):
            gP[i].wait_recv()
        gather_grads(0)
        gather_grads(1)
    with sc("wait_gO"):
        gO[1].wait_recv()
        gF[1].start()
        gather_grads(2)
    with sc("wait_gF"):
        for i in range(2):
            gF[i].wait_recv()
        gather_grads(3)

    def ox(t):
        return rc("ox", t, GOs.at[t], GOx.at[t], to_x)

    def oz(k):
        return rc("oz", k - 1, GOk.at[k - 1], GOz.at[k - 1], to_z[k])

    def ix(j):
        return rc("ix", j, GIs.at[j], GIx.at[j], to_x)

    def iz(j, k):
        return rc("iz", j * 3 + k - 1, GIk.at[j, zs[k]], GIz.at[k - 1, j], to_z[k])

    def w_out_tile(t, carry):
        zp = lax.rem(z + 1 + t, 4)
        r = dot(DT[...], M[:, pl.ds(pl.multiple_of(zp * width, width), width)])
        lo, hi = r[:, :width // 2], r[:, width // 2:]
        GOs[t] = jnp.where(x == 0, hi, lo).astype(BF)
        GOk[t] = jnp.where(x == 0, lo, hi).astype(BF)
        ox(t).start()
        return carry

    with sc("w_out_tiles"):
        lax.fori_loop(0, 4, w_out_tile, 0)

    def take_o(t):
        with sc("take_o%d" % t):
            ox(t).wait_recv()
            GOk[t] = (GOk[t].astype(F32) + GOx[t].astype(F32)).astype(BF)
            if t < 3:
                oz(t + 1).start()

    def take_i(j):
        with sc("take_i%d" % j):
            ix(j).wait_recv()
            GIk[j] = (GIk[j].astype(F32) + GIx[j].astype(F32)).astype(BF)
            for k in range(1, 4):
                iz(j, k).start()

    load_out.wait()
    GD[:, 1:2] = jnp.zeros((GD.shape[0], 1), F32)

    def expert_back(n, carry):
        cols = pl.ds(pl.multiple_of(n * tile, tile), tile)
        for first in (0, half_rows):
            rs = slice(first, first + half_rows)
            back = dot_nt(GE[rs, :], WO[cols, :])
            GD[rs, 1:2] += jnp.sum(back * M[rs, cols].astype(F32), axis=-1, keepdims=True)
            D[rs, cols] = (D[rs, cols].astype(F32) * (GD[rs, 0:1] * back)).astype(BF)
        return carry

    with sc("expert_back"):
        lax.fori_loop(0, tiles, expert_back, 0)
    take_o(0)

    dP = [rc("dP", i, U.at[1, i, top], RP.at[i], to_p) for i in range(2)]
    dD = [rc("dD", i, U.at[3, i, top], RD.at[i], to_p) for i in range(2)]
    dO = [rc("dO", i, U.at[2, i, top], RO.at[i], to_o) for i in range(2)]
    eP = rc("eP", 0, ES.at[1], EP, to_p)
    eD = rc("eD", 0, ES.at[3], ED, to_p)
    eO = rc("eO", 0, ES.at[2], EO, to_o)
    yP = [rc("yP", i, G.at[1, i, top], YP.at[i], to_p) for i in range(2)]
    yD = [rc("yD", i, G.at[3, i, top], YD.at[i], to_p) for i in range(2)]
    yO = [rc("yO", i, G.at[2, i, top], YO.at[i], to_o) for i in range(2)]

    for cp in uP + uO + uF:
        cp.wait_send()

    def scatter(s, values):
        return dot_tn(onehot(s), values)

    for s in (3, 2, 1, 0):
        with sc("du%d" % s):
            rs = slice(s * LP, (s + 1) * LP)
            out = scatter(s, dot_nt(D[rs, :], WI[...]).astype(BF))
            if s == 0:
                for i in range(2):
                    DH[i] = out[i * LP:i * LP + sp]
            else:
                U[s] = out.astype(BF).reshape(2, LP, width)
            dg = GD[rs, 1:2]
            hi = dg.astype(BF)
            rest = (dg - hi.astype(F32)).astype(BF)
            at = lane((LP, 128))
            zero = jnp.zeros((LP, 128), BF)
            two = jnp.where(at == ep, hi, zero) + jnp.where(at == ep + 64, rest, zero)
            ES[s] = scatter(s, two).astype(BF).reshape(2, LP, 128)
            if s == 3:
                for cp in dD + [eD]:
                    cp.start()
            if s == 1:
                for cp in dP + [eP]:
                    cp.start()
    with sc("combine_du"):
        for i in range(2):
            dD[i].wait_recv()
            U[2, i, :sp, :] = (U[2, i, :sp, :].astype(F32) + RD[i].astype(F32)).astype(BF)
            dO[i].start()
        eD.wait_recv()
        ES[2] = ES[2] + ED[...]
        eO.start()
    take_o(1)

    def w_in_tile(j, carry):
        r = dot_tn(X[...], D[:, pl.ds(pl.multiple_of(j * width, width), width)]).reshape(4, 2, width // 8, width)
        first, second = r[:, 0], r[:, 1]
        GIs[j] = jnp.where(x == 0, second, first).astype(BF)
        GIk[j] = jnp.where(x == 0, first, second).astype(BF)
        ix(j).start()
        return carry

    with sc("w_in_tiles"):
        lax.fori_loop(0, 4, w_in_tile, 0)
    for dev in friends:
        pl.semaphore_signal(free, inc=1, device_id=dev, device_id_type=MESH)

    for cp in gP + gO + gF:
        cp.wait_send()
    for s in (3, 2, 1, 0):
        with sc("o%d" % s):
            rs = slice(s * LP, (s + 1) * LP)
            o = dot(M[rs, :], WO[...]).astype(BF).astype(F32)
            out = scatter(s, (GD[rs, 0:1] * o).astype(BF)).astype(BF)
            if s == 0:
                X[0:half_rows, :] = out
            else:
                G[s] = out.reshape(2, LP, width)
            if s == 3:
                for cp in yD:
                    cp.start()
            if s == 1:
                for cp in yP:
                    cp.start()
    late = attention_weights(3) + [
        lc(7, qa_h, M.at[pl.ds(0, rows)]), lc(8, c_h, M.at[pl.ds(rows, rows), pl.ds(0, width)])
    ] + [lc(9 + i, xb.at[i], GE.at[pl.ds(rows + i * sp, sp)]) for i in range(2)]
    for cp in late:
        cp.start()
    with sc("combine_y"):
        for i in range(2):
            yD[i].wait_recv()
            G[2, i, :sp, :] = (G[2, i, :sp, :].astype(F32) + YD[i].astype(F32)).astype(BF)
            yO[i].start()
    take_o(2)

    with sc("wait_du"):
        for i in range(2):
            dP[i].wait_recv()
            dO[i].wait_recv()
        eP.wait_recv()
        eO.wait_recv()
    with sc("ln2_back"):
        router = jnp.zeros((width, 128), F32)
        gain2 = jnp.zeros((1, width), F32)
        bias2 = jnp.zeros((1, width), F32)
        for i in range(2):
            du = DH[i] + RP[i].astype(F32) + RO[i].astype(F32)
            back = ES[0, i, :sp, :].astype(F32) + EP[i, :sp, :].astype(F32) + EO[i, :sp, :].astype(F32)
            back = back + pltpu.roll(back, 64, axis=1)
            own = U[0, i, :sp, :]
            r = dot_nt(own, WR[...])
            r = jnp.where(lane(r.shape) < experts, r, NEG)
            r = jnp.exp(r - jnp.max(r, axis=-1, keepdims=True))
            r = r / jnp.sum(r, axis=-1, keepdims=True)
            dl = (r * (back - jnp.sum(r * back, axis=-1, keepdims=True))).astype(BF)
            router = router + dot_tn(own, dl)
            du = du + dot(dl, WR[...])
            n2, inv2 = norm_parts(H[i])
            gain2 = gain2 + jnp.sum(du * n2, axis=0, keepdims=True)
            bias2 = bias2 + jnp.sum(du, axis=0, keepdims=True)
            dh = G[0, i, :sp, :].astype(F32) + norm_backward(du * g2, n2, inv2)
            DH[i] = dh
            GE[i * sp:(i + 1) * sp, :] = dh.astype(BF)
        SM[...] = router.astype(BF)
    for cp in late:
        cp.wait()

    def part(e, b):
        return pl.ds(pl.multiple_of(e * shard, shard), shard), pl.ds(b * width, width)

    def mine(b, h):
        return pl.ds(pl.multiple_of(b * width + h * (width // 2), 128), width // 2)

    def rest(r0, n, b, second):
        return D.at[r0:r0 + n, pl.ds(b * width + second * (width // 2), width // 2)]

    def cp_c(b, i):
        return rc("C", b * 2 + i, WI.at[part(i * 2 + 1 - core, b)], D.at[pl.ds(i * shard, shard), pl.ds(b * width, width)], to_p)

    def cp_y(b):
        return rc("Y", b, WI.at[part((1 - y) * 2 + core, b)], D.at[pl.ds(2 * shard, shard), pl.ds(b * width, width)], to_o)

    def own_rows(k=0, n=shard):
        return pl.ds(pl.multiple_of(ep * shard + k * block, block), n)

    def cp_x(b):
        return rc("X", b, WI.at[own_rows(), mine(b, 1 - x)], rest(3 * shard, shard, b, 0), to_x)

    def cp_z(b, k):
        return rc("Z", b * 3 + k - 1, WI.at[own_rows(zs[k], block), mine(b, x)],
                  rest(4 * shard + (k - 1) * block, block, b, 0), to_z[k])

    def result(k, b):
        return D.at[pl.ds(pl.multiple_of(4 * shard + k * block, block), block),
                    pl.ds(b * width + width // 2, width // 2)]

    def cp_az(b, k):
        return rc("AZ", b * 3 + k - 1, result(z, b), result(z, b), to_z[k])

    def cp_ax(b):
        return rc("AX", b, rest(4 * shard, shard, b, 1), rest(3 * shard, shard, b, 1), to_x)

    def stage_c(b):
        for i in range(2):
            cp_c(b, i).start()

    def stage_y(b):
        with sc("stage_y%d" % b):
            for i in range(2):
                cp_c(b, i).wait_recv()
            for i in range(2):
                at = part(i * 2 + core, b)
                WI[at] = (WI[at].astype(F32) + D[i * shard:(i + 1) * shard, b * width:(b + 1) * width].astype(F32)).astype(BF)
            cp_y(b).start()

    def stage_x(b):
        with sc("stage_x%d" % b):
            cp_y(b).wait_recv()
            at = part(ep, b)
            WI[at] = (WI[at].astype(F32) + D[2 * shard:3 * shard, b * width:(b + 1) * width].astype(F32)).astype(BF)
            cp_x(b).start()

    def stage_z(b):
        with sc("stage_z%d" % b):
            cp_x(b).wait_recv()
            at = own_rows(), mine(b, x)
            WI[at] = (WI[at].astype(F32) + rest(3 * shard, shard, b, 0)[...].astype(F32)).astype(BF)
            for k in range(1, 4):
                cp_z(b, k).start()

    def stage_az(b):
        with sc("stage_az%d" % b):
            for k in range(1, 4):
                cp_z(b, k).wait_recv()
            total = WI[own_rows(z, block), mine(b, x)].astype(F32)
            for k in range(3):
                total = total + rest(4 * shard + k * block, block, b, 0)[...].astype(F32)
            result(z, b)[...] = total.astype(BF)
            for k in range(1, 4):
                cp_az(b, k).start()

    def stage_ax(b):
        with sc("stage_ax%d" % b):
            for k in range(1, 4):
                rc("AZ", b * 3 + k - 1, result(zs[4 - k], b), result(zs[4 - k], b), to_z[k]).wait_recv()
            cp_ax(b).start()

    with sc("attn_out_grads"):
        X[half_rows:half_rows + rows, :] = dot_nt(GE[0:rows, :], WO[3 * width:, :]).astype(BF)
        WI[:, 3 * width:] = dot_tn(M[rows:2 * rows, 0:width], GE[0:rows, :]).astype(BF)
    with sc("wait_free"):
        pl.semaphore_wait(free, 6)
    stage_c(3)
    take_o(3)

    def pair_back(h, carry):
        def cols(n):
            return pl.ds(pl.multiple_of(h * 128 + n * width, 128), 128)

        for i in range(2):
            r0 = slice(i * sp, (i + 1) * sp)
            q, k, v = M[r0, cols(0)], M[r0, cols(1)], M[r0, cols(2)]
            dc = X[half_rows + i * sp:half_rows + (i + 1) * sp, cols(0)]
            parts = []
            for side in range(2):
                here = low if side == 0 else ~low
                zero = jnp.zeros_like(q)
                lse = jnp.sum(jnp.where(lane((sp, 128)) == 2 * h + side, LS[i], 0.0), axis=-1, keepdims=True)
                s = dot_nt(jnp.where(here, q, zero), k) * scaling
                p = jnp.exp(jnp.where(keys, s, NEG) - lse)
                dv = dot_tn(p.astype(BF), dc)
                dp_ = dot_nt(jnp.where(here, dc, zero), v)
                ds = (p * (dp_ - jnp.sum(p * dp_, axis=-1, keepdims=True))).astype(BF)
                parts.append((dot(ds, k) * scaling, dot_tn(ds, q) * scaling, dv))
            r1 = slice(rows + i * sp, rows + (i + 1) * sp)
            for n in range(3):
                M[r1, cols(n + 1)] = jnp.where(low, parts[0][n], parts[1][n]).astype(BF)
        return carry

    with sc("attention_back_a"):
        lax.fori_loop(0, width // 256, pair_back, 0)
    stage_y(3)
    take_i(0)
    with sc("attention_back_b"):
        lax.fori_loop(width // 256, width // 128, pair_back, 0)
    for n in range(3):
        with sc("qkv_grads"):
            grads = M[rows:2 * rows, (n + 1) * width:(n + 2) * width]
            WI[:, n * width:(n + 1) * width] = dot_tn(M[0:rows, 3 * width:], grads).astype(BF)
        stage_c(n)
    stage_x(3)
    with sc("ln1_back"):
        gain1 = jnp.zeros((1, width), F32)
        bias1 = jnp.zeros((1, width), F32)
        for i in range(2):
            r1 = slice(rows + i * sp, rows + (i + 1) * sp)
            grad = dot_nt(M[r1, width:2 * width], WO[0:width, :])
            for n in range(1, 3):
                grad = grad + dot_nt(M[r1, (n + 1) * width:(n + 2) * width], WO[n * width:(n + 1) * width, :])
            n1, inv1 = norm_parts(GE[r1, :].astype(F32))
            gain1 = gain1 + jnp.sum(grad * n1, axis=0, keepdims=True)
            bias1 = bias1 + jnp.sum(grad, axis=0, keepdims=True)
            DH[i] = DH[i] + norm_backward(grad * g1, n1, inv1)
        vectors = jnp.concatenate([jnp.zeros((4, width), F32), gain1, bias1, gain2, bias2], axis=0)
        vectors = jnp.concatenate([vectors, jnp.zeros((120, width), F32)], axis=0)
        SM[...] = (SM[...].astype(F32) + jnp.transpose(vectors)).astype(BF)

    def small(e):
        return pl.ds(pl.multiple_of(e * shard, shard), shard)

    mC = [rc("mC", i, SM.at[small(i * 2 + 1 - core)], SMx.at[i], to_p) for i in range(2)]
    mY = rc("mY", 0, SM.at[small((1 - y) * 2 + core)], SMx.at[2], to_o)
    mX = rc("mX", 0, SM.at[small(ep)], SMx.at[3], to_x)
    mZ = [rc("mZ", k - 1, SMx.at[3], SMx.at[3 + k], to_z[k]) for k in range(1, 4)]
    for cp in mC:
        cp.start()
    for b in range(3):
        stage_y(b)
    with sc("small_y"):
        for i in range(2):
            mC[i].wait_recv()
            at = small(i * 2 + core)
            SM[at, :] = (SM[at, :].astype(F32) + SMx[i].astype(F32)).astype(BF)
        mY.start()
    with sc("block_out"):
        for i in range(2):
            yP[i].wait_recv()
            yO[i].wait_recv()
            on = (live[0] > i).astype(F32)
            mix = X[i * LP:i * LP + sp, :].astype(F32) + YP[i].astype(F32) + YO[i].astype(F32)
            bo_o[i] = ((H[i] + mix) * on).astype(BF)
    take_i(1)
    stage_x(0)
    take_i(2)
    stage_x(1)
    stage_z(3)
    stage_x(2)
    with sc("small_x"):
        mY.wait_recv()
        at = small(ep)
        SM[at, :] = (SM[at, :].astype(F32) + SMx[2].astype(F32)).astype(BF)
        mX.start()
    take_i(3)
    with sc("small_z"):
        mX.wait_recv()
        SMx[3] = (SM[small(ep), :].astype(F32) + SMx[3].astype(F32)).astype(BF)
        for cp in mZ:
            cp.start()
    stage_az(3)
    for b in range(3):
        stage_z(b)
    stage_ax(3)
    for b in range(3):
        stage_az(b)
    with sc("o_sum"):
        for k in range(1, 4):
            oz(k).wait_recv()
        total = GOk[3].astype(F32)
        for k in range(3):
            total = total + GOz[k].astype(F32)
        GOk[3] = total.astype(BF)
        outs = [lc(0, GOk.at[3], wo_o)]
        outs[0].start()
    for j in range(4):
        with sc("i_sum"):
            for k in range(1, 4):
                iz(j, k).wait_recv()
            total = GIk[j, z].astype(F32)
            for k in range(3):
                total = total + GIz[k, j].astype(F32)
            GIx[j, 0] = total.astype(BF)
            outs.append(lc(1 + j, GIx.at[j, 0], wi_o.at[:, pl.ds(j * width, width)]))
            outs[-1].start()
    with sc("small_sum"):
        for cp in mZ:
            cp.wait_recv()
        total = SMx[3].astype(F32) + SMx[4].astype(F32) + SMx[5].astype(F32) + SMx[6].astype(F32)
        sm_o[...] = jnp.transpose(total)[0:8, :]
    for b in range(3):
        stage_ax(b)
    for b in (3, 0, 1, 2):
        outs.append(lc(5 + b, rest(4 * shard, shard, b, 1), sg_o.at[:, mine(b, x)]))
        outs[-1].start()
    with sc("wait_ax"):
        for b in (3, 0, 1, 2):
            cp_ax(b).wait_recv()
            outs.append(lc(9 + b, rest(3 * shard, shard, b, 1), sg_o.at[:, mine(b, 1 - x)]))
            outs[-1].start()
    with sc("drain"):
        for cp in dP + dD + dO + yP + yD + yO + [sP, sO, sF, eP, eD, eO, mY, mX] + mC + mZ:
            cp.wait_send()
        for t in range(4):
            ox(t).wait_send()
            ix(t).wait_send()
            cp_y(t).wait_send()
            cp_x(t).wait_send()
            cp_ax(t).wait_send()
            for i in range(2):
                cp_c(t, i).wait_send()
            for k in range(1, 4):
                iz(t, k).wait_send()
                cp_z(t, k).wait_send()
                cp_az(t, k).wait_send()
        for k in range(1, 4):
            oz(k).wait_send()
        for cp in outs:
            cp.wait()


def fast_body(n_ep, tokens, live, routes, g1, b1, wqkv, wo, g2, b2, wr, w_in, w_out, cot):
    slots, seq, width = tokens.shape
    sp = (seq + 15) // 16 * 16
    f = w_in.shape[2]
    cap = n_ep * LP
    pads = ((0, 0), (0, sp - seq), (0, 0))
    on = (jnp.arange(slots, dtype=jnp.int32) < live[0])[:, None, None]
    gl = jnp.pad(jnp.where(on, cot, jnp.zeros_like(cot)), pads)
    xb = jnp.pad(tokens, pads)
    gains = jnp.stack([g1, b1, g2, b2])
    sds = jax.ShapeDtypeStruct
    vm = pl.BlockSpec(memory_space=pltpu.VMEM)
    anys = pl.BlockSpec(memory_space=pl.ANY)
    b = lambda *shape: pltpu.VMEM(shape, BF)
    g = lambda *shape: pltpu.VMEM(shape, F32)
    shard = width // n_ep
    bo, gt, sm, wo_t, wi, sg, _, _ = pl.pallas_call(
        functools.partial(layer_kernel, n_ep, seq),
        name="layer",
        out_shape=(
            sds((slots, sp, width), BF), sds((slots, sp, width), F32), sds((8, shard), F32),
            sds((width, f // 8), BF), sds((width // 8, f), BF), sds((shard, 4 * width), BF),
            sds((2 * sp, 4 * width), BF), sds((2 * sp, width), BF),
        ),
        in_specs=[pl.BlockSpec(memory_space=pltpu.SMEM)] + [vm] * 3 + [anys] * 6,
        out_specs=[vm] * 3 + [anys] * 5,
        scratch_shapes=[
            b(4, 2, LP, width), b(4, 2, LP, width), g(4, 2, 8, LP), b(128, width), b(width, f), b(f, width),
            b(cap, f), b(cap, f), b(cap, width), b(cap, width), b(width, cap),
            b(4, width, f // 8), b(4, width, f // 8), b(4, width, f // 8), b(3, width, f // 8),
            b(4, 4, width // 8, width), b(4, 4, width // 8, width), b(4, 4, width // 8, width),
            b(3, 4, width // 8, width),
            g(slots, sp, width), g(slots, sp, 128), g(cap, 2),
            b(2, sp, width), b(2, sp, width), b(2, sp, width),
            b(2, LP, 128), b(2, LP, 128), b(2, LP, 128), b(4, 2, LP, 128),
            b(2, sp, width), b(2, sp, width), b(2, sp, width), b(width, 128), b(7, shard, 128),
            pltpu.SemaphoreType.DMA((N_COPIES,)), pltpu.SemaphoreType.DMA((N_COPIES,)),
            pltpu.SemaphoreType.DMA((14,)), pltpu.SemaphoreType.REGULAR,
        ],
        compiler_params=pltpu.CompilerParams(
            collective_id=0, has_side_effects=True, vmem_limit_bytes=67043328),
    )(live, jnp.transpose(routes, (0, 2, 1)), gains, jnp.transpose(wr), xb, gl, w_in, w_out, wqkv, wo)
    return (
        bo[:, :seq], gt[:, :seq], sm[4], sm[5], sg[:, :3 * width].astype(F32), sg[:, 3 * width:].astype(F32),
        sm[6], sm[7], jnp.transpose(sm[:n_ep]), wi.astype(F32)[None], jnp.transpose(wo_t).astype(F32)[None],
    )


def general_body(
    tokens,
    live_images,
    routes,
    ln1_gain,
    ln1_bias,
    query_key_value_weight,
    attention_output_weight,
    ln2_gain,
    ln2_bias,
    w_router,
    w_in,
    w_out,
    cotangent,
):
    slot_count, seq_len, model_width = tokens.shape
    row_count = slot_count * seq_len
    expert_count = w_router.shape[1]
    hidden_width = w_in.shape[2]
    capacity = ((2 * row_count + expert_count - 1) // expert_count * 5 // 4 + 7) // 8 * 8
    scaling = HEAD_DIM ** (-0.5)
    inputs = tokens.astype(jnp.float32).reshape(row_count, model_width)
    normed1, inverse1 = norm_parts(inputs)
    attn_in = (normed1 * ln1_gain + ln1_bias).astype(jnp.bfloat16)
    qkv_rows = jnp.dot(attn_in, query_key_value_weight, preferred_element_type=jnp.float32).astype(
        jnp.bfloat16
    )
    qkv_heads = qkv_rows.reshape(slot_count, seq_len, 3, HEADS, HEAD_DIM)
    queries = qkv_heads[:, :, 0]
    keys_all = qkv_heads[:, :, 1]
    values_all = qkv_heads[:, :, 2]
    scores = (
        jnp.einsum("sqhc,skhc->shqk", queries, keys_all, preferred_element_type=jnp.float32)
        * scaling
    )
    row_peak = jnp.max(scores, axis=-1, keepdims=True)
    raised = jnp.exp(scores - row_peak)
    totals = jnp.sum(raised, axis=-1, keepdims=True)
    log_total = row_peak + jnp.log(totals)
    weights = (raised / totals).astype(jnp.bfloat16)
    attended_context = jnp.einsum(
        "shqk,skhc->sqhc", weights, values_all, preferred_element_type=jnp.float32
    )
    attended_context = attended_context.astype(jnp.bfloat16).reshape(row_count, model_width)
    hidden1 = inputs + jnp.dot(
        attended_context, attention_output_weight, preferred_element_type=jnp.float32
    )
    normed2, inverse2 = norm_parts(hidden1)
    moe_in = (normed2 * ln2_gain + ln2_bias).astype(jnp.bfloat16)
    router = jax.nn.softmax(jnp.dot(moe_in, w_router, preferred_element_type=jnp.float32), axis=-1)
    chosen = routes.reshape(row_count, 2)
    expert_ids = jnp.arange(expert_count, dtype=jnp.int32)
    picked = (chosen[:, :, None] == expert_ids[None, None, :]).astype(jnp.float32)
    gates = jnp.sum(picked * router[:, None, :], axis=-1)
    token_live = (jnp.arange(row_count, dtype=jnp.int32) // seq_len < live_images[0]).astype(
        jnp.float32
    )
    pair_ids = chosen.reshape(2 * row_count)
    pair_live = jnp.repeat(token_live, 2) > 0.5
    member = ((pair_ids[:, None] == expert_ids[None, :]) & pair_live[:, None]).astype(jnp.int32)
    position = jnp.sum((jnp.cumsum(member, axis=0) - 1) * member, axis=-1)
    slot_ids = jnp.where(pair_live, pair_ids * capacity + position, -1).reshape(row_count, 2)
    lanes = jnp.arange(expert_count * capacity, dtype=jnp.int32)
    placing = (jnp.transpose(slot_ids)[:, None, :] == lanes[None, :, None]).astype(jnp.bfloat16)
    outbox = jnp.einsum("jsr,rd->sd", placing, moe_in, preferred_element_type=jnp.float32)
    outbox = outbox.astype(jnp.bfloat16).reshape(expert_count, capacity, model_width)
    inbox = lax.all_to_all(outbox, "ep", split_axis=0, concat_axis=0, tiled=True)
    flat_in = inbox.reshape(-1, model_width)
    pre_act = jnp.dot(flat_in, w_in[0], preferred_element_type=jnp.float32)
    activated = jax.nn.gelu(pre_act).astype(jnp.bfloat16)
    produced = jnp.dot(activated, w_out[0], preferred_element_type=jnp.float32).astype(jnp.bfloat16)
    coming_back = lax.all_to_all(
        produced.reshape(inbox.shape), "ep", split_axis=0, concat_axis=0, tiled=True
    )
    coming_back, pre_act = (
        coming_back,
        pre_act.reshape(inbox.shape[0], inbox.shape[1], hidden_width),
    )
    arrived_rows = inbox.reshape(-1, model_width)
    pre_rows = pre_act.reshape(-1, hidden_width)
    returned_rows = coming_back.reshape(expert_count * capacity, model_width)
    taken = jnp.einsum("jsr,sd->rjd", placing, returned_rows, preferred_element_type=jnp.float32)
    mixture = jnp.sum(gates[:, :, None] * taken, axis=1)
    block_out = (
        ((hidden1 + mixture) * token_live[:, None]).astype(jnp.bfloat16).reshape(tokens.shape)
    )
    upstream = cotangent.astype(jnp.float32).reshape(row_count, model_width) * token_live[:, None]
    gate_grads = jnp.sum(taken * upstream[:, None, :], axis=-1)
    sent_grads = (gates[:, :, None] * upstream[:, None, :]).astype(jnp.bfloat16)
    grad_outbox = jnp.einsum("jsr,rjd->sd", placing, sent_grads, preferred_element_type=jnp.float32)
    grad_outbox = grad_outbox.astype(jnp.bfloat16).reshape(expert_count, capacity, model_width)
    grad_inbox = lax.all_to_all(grad_outbox, "ep", split_axis=0, concat_axis=0, tiled=True)
    grad_rows = grad_inbox.reshape(-1, model_width)
    activated_rows, gelu_pull = jax.vjp(jax.nn.gelu, pre_rows)
    activated_low = activated_rows.astype(jnp.bfloat16)
    grad_activated = jnp.einsum(
        "rd,fd->rf", grad_rows, w_out[0], preferred_element_type=jnp.float32
    )
    grad_pre = gelu_pull(grad_activated)[0].astype(jnp.bfloat16)
    columns = activated_low
    grad_w_out = lax.psum_scatter(
        jnp.einsum("rf,rd->fd", columns, grad_rows, preferred_element_type=jnp.float32).astype(
            jnp.bfloat16
        ),
        "dp",
        scatter_dimension=0,
        tiled=True,
    ).astype(jnp.float32)
    grad_back_rows = jnp.einsum(
        "rf,df->rd", grad_pre, w_in[0], preferred_element_type=jnp.float32
    ).astype(jnp.bfloat16)
    grad_back = lax.all_to_all(
        grad_back_rows.reshape(grad_inbox.shape), "ep", split_axis=0, concat_axis=0, tiled=True
    )
    columns = arrived_rows
    grad_w_in = lax.psum_scatter(
        jnp.einsum("rd,rf->df", columns, grad_pre, preferred_element_type=jnp.float32).astype(
            jnp.bfloat16
        ),
        "dp",
        scatter_dimension=0,
        tiled=True,
    ).astype(jnp.float32)
    grad_back_flat = grad_back.reshape(expert_count * capacity, model_width)
    expert_grad = jnp.einsum(
        "jsr,sd->rd", placing, grad_back_flat, preferred_element_type=jnp.float32
    )
    grad_router_probs = jnp.sum(gate_grads[:, :, None] * picked, axis=1)
    grad_logits = router * (
        grad_router_probs - jnp.sum(router * grad_router_probs, axis=-1, keepdims=True)
    )
    grad_logits = grad_logits.astype(jnp.bfloat16)
    grad_w_router = jnp.einsum("rd,re->de", moe_in, grad_logits, preferred_element_type=jnp.float32)
    grad_moe_in = expert_grad + jnp.einsum(
        "re,de->rd", grad_logits, w_router, preferred_element_type=jnp.float32
    )
    grad_ln2_gain = jnp.sum(grad_moe_in * normed2, axis=0)
    grad_ln2_bias = jnp.sum(grad_moe_in, axis=0)
    grad_hidden1 = upstream + norm_backward(grad_moe_in * ln2_gain, normed2, inverse2)
    grad_attn = grad_hidden1.astype(jnp.bfloat16)
    grad_w_attn_out = jnp.einsum(
        "rd,re->de", attended_context, grad_attn, preferred_element_type=jnp.float32
    )
    grad_context = jnp.einsum(
        "re,de->rd", grad_attn, attention_output_weight, preferred_element_type=jnp.float32
    )
    grad_context = grad_context.astype(jnp.bfloat16).reshape(slot_count, seq_len, HEADS, HEAD_DIM)
    again = (
        jnp.einsum("sqhc,skhc->shqk", queries, keys_all, preferred_element_type=jnp.float32)
        * scaling
    )
    probs_again = jnp.exp(again - log_total)
    probs_low = probs_again.astype(jnp.bfloat16)
    grad_values = jnp.einsum(
        "shqk,sqhc->skhc", probs_low, grad_context, preferred_element_type=jnp.float32
    )
    grad_probs = jnp.einsum(
        "sqhc,skhc->shqk", grad_context, values_all, preferred_element_type=jnp.float32
    )
    grad_scores = probs_again * (
        grad_probs - jnp.sum(probs_again * grad_probs, axis=-1, keepdims=True)
    )
    grad_scores = grad_scores.astype(jnp.bfloat16)
    grad_queries = (
        jnp.einsum("shqk,skhc->sqhc", grad_scores, keys_all, preferred_element_type=jnp.float32)
        * scaling
    )
    grad_keys = (
        jnp.einsum("shqk,sqhc->skhc", grad_scores, queries, preferred_element_type=jnp.float32)
        * scaling
    )
    grad_qkv = (
        jnp.stack([grad_queries, grad_keys, grad_values], axis=2)
        .astype(jnp.bfloat16)
        .reshape(row_count, 3 * model_width)
    )
    grad_w_qkv = jnp.einsum("rd,re->de", attn_in, grad_qkv, preferred_element_type=jnp.float32)
    grad_attn_in = jnp.einsum(
        "re,de->rd", grad_qkv, query_key_value_weight, preferred_element_type=jnp.float32
    )
    grad_ln1_gain = jnp.sum(grad_attn_in * normed1, axis=0)
    grad_ln1_bias = jnp.sum(grad_attn_in, axis=0)
    grad_inputs = grad_hidden1 + norm_backward(grad_attn_in * ln1_gain, normed1, inverse1)
    shared = (
        grad_w_qkv,
        grad_w_attn_out,
        grad_w_router,
        grad_ln1_gain,
        grad_ln1_bias,
        grad_ln2_gain,
        grad_ln2_bias,
    )
    partial_sums = (
        lax.psum_scatter(
            shared[0].astype(jnp.bfloat16), "ep", scatter_dimension=0, tiled=True
        ).astype(jnp.float32),
        lax.psum_scatter(
            shared[1].astype(jnp.bfloat16), "ep", scatter_dimension=0, tiled=True
        ).astype(jnp.float32),
        lax.psum_scatter(
            shared[2].astype(jnp.bfloat16), "ep", scatter_dimension=0, tiled=True
        ).astype(jnp.float32),
        lax.psum_scatter(
            shared[3].astype(jnp.bfloat16), "ep", scatter_dimension=0, tiled=True
        ).astype(jnp.float32),
        lax.psum_scatter(
            shared[4].astype(jnp.bfloat16), "ep", scatter_dimension=0, tiled=True
        ).astype(jnp.float32),
        lax.psum_scatter(
            shared[5].astype(jnp.bfloat16), "ep", scatter_dimension=0, tiled=True
        ).astype(jnp.float32),
        lax.psum_scatter(
            shared[6].astype(jnp.bfloat16), "ep", scatter_dimension=0, tiled=True
        ).astype(jnp.float32),
    )
    shares = (
        lax.psum(partial_sums[0].astype(jnp.bfloat16), "dp").astype(jnp.float32),
        lax.psum(partial_sums[1].astype(jnp.bfloat16), "dp").astype(jnp.float32),
        lax.psum(partial_sums[2].astype(jnp.bfloat16), "dp").astype(jnp.float32),
        lax.psum(partial_sums[3].astype(jnp.bfloat16), "dp").astype(jnp.float32),
        lax.psum(partial_sums[4].astype(jnp.bfloat16), "dp").astype(jnp.float32),
        lax.psum(partial_sums[5].astype(jnp.bfloat16), "dp").astype(jnp.float32),
        lax.psum(partial_sums[6].astype(jnp.bfloat16), "dp").astype(jnp.float32),
    )
    return (
        block_out,
        grad_inputs.reshape(tokens.shape),
        shares[3],
        shares[4],
        shares[0],
        shares[1],
        shares[5],
        shares[6],
        shares[2],
        grad_w_in[None],
        grad_w_out[None],
    )


def solution(mesh):
    in_specs = (
        P(("dp", "ep"), None, None),
        P(("dp", "ep")),
        P(("dp", "ep"), None, None),
        P(),
        P(),
        P(),
        P(),
        P(),
        P(),
        P(),
        P("ep", None, None),
        P("ep", None, None),
        P(("dp", "ep"), None, None),
    )
    out_specs = (
        P(("dp", "ep"), None, None),
        P(("dp", "ep"), None, None),
        P("ep"),
        P("ep"),
        P("ep", None),
        P("ep", None),
        P("ep"),
        P("ep"),
        P("ep", None),
        P("ep", "dp", None),
        P("ep", "dp", None),
    )
    n_dp, n_ep = mesh.shape["dp"], mesh.shape["ep"]
    body = functools.partial(fast_body, n_ep) if (n_dp, n_ep) == (8, 4) else general_body
    return jax.shard_map(body, mesh=mesh, in_specs=in_specs, out_specs=out_specs, check_vma=False)
```

```python
import contextlib
import functools

import jax
import jax.numpy as jnp
from jax import lax
from jax.experimental import pallas as pl
from jax.experimental.pallas import tpu as pltpu
from jax.sharding import PartitionSpec as P

HEADS = 12
HEAD_DIM = 64
MESH = pl.DeviceIdType.MESH
BF = jnp.bfloat16
F32 = jnp.float32
eps = 1e-06
NEG = -1e30
LP = 256


def dot(a, b):
    return jnp.dot(a, b, preferred_element_type=F32)


def dot_nt(a, b):
    return lax.dot_general(a, b, (((1,), (1,)), ((), ())), preferred_element_type=F32)


def dot_tn(a, b):
    return lax.dot_general(a, b, (((0,), (0,)), ((), ())), preferred_element_type=F32)


def lane(shape):
    return lax.broadcasted_iota(jnp.int32, shape, len(shape) - 1)


def sub(shape):
    return lax.broadcasted_iota(jnp.int32, shape, len(shape) - 2)


def norm_parts(v):
    centre = jnp.mean(v, axis=-1, keepdims=True)
    shifted = v - centre
    inverse = lax.rsqrt(jnp.mean(shifted * shifted, axis=-1, keepdims=True) + eps)
    return shifted * inverse, inverse


def norm_backward(y, n, inverse):
    middle = jnp.mean(y, axis=-1, keepdims=True)
    along = jnp.mean(y * n, axis=-1, keepdims=True)
    return (y - middle - n * along) * inverse


def sc(name):
    return contextlib.nullcontext()


COPIES = {}
for _name, _count in (
    ("uP", 2), ("uO", 2), ("uF", 2), ("sP", 1), ("sO", 1), ("sF", 1), ("gP", 2), ("gO", 2), ("gF", 2),
    ("ox", 4), ("oq", 2), ("oz", 1), ("oc", 2), ("ix", 4), ("iq", 8), ("iz", 4), ("ic", 8), ("jq", 2), ("jz", 1), ("jc", 2),
    ("dP", 2), ("dD", 2), ("dO", 2), ("eP", 1), ("eD", 1), ("eO", 1), ("yP", 2), ("yD", 2), ("yO", 2),
    ("C", 8), ("Y", 4), ("X", 4), ("R1", 4), ("R2", 4), ("R3", 4), ("AX", 4), ("mC", 2), ("mY", 1), ("mX", 1), ("mZ", 3),
):
    COPIES[_name] = sum(n for _, n in COPIES.values()), _count
N_COPIES = sum(n for _, n in COPIES.values())


def layer_kernel(
    experts, seq, live, routes, gains, wrt, xb, gl, w_in, w_out, wqkv, wo,
    bo_o, DH, sm_o, wo_o, wi_o, sg_o, qa_h, c_h, u_h,
    U, G, SL, WR, WI, WO, M, D, X, GE, DT,
    GOs, GOk, GOx, GOz, GIs, GIk, GIx, GIz, GJ,
    H, LS, GD, RP, RD, RO, EP, ED, EO, ES, YP, YD, YO, SM, SMx,
    ssem, rsem, lsem, free, credit,
):
    f, width = WO.shape
    sp, rows, half_rows = 208, 416, 512
    shard, block = width // 4, width // 16
    dp, ep = lax.axis_index("dp"), lax.axis_index("ep")
    z, x = dp // 2, dp % 2
    y, core = ep // 2, ep % 2
    to_p = {"ep": y * 2 + 1 - core}
    to_o = {"ep": (1 - y) * 2 + core}
    to_x = {"dp": z * 2 + 1 - x}
    zs = [lax.rem(z + k, 4) for k in range(4)]
    to_z = [{"dp": zs[k] * 2 + x} for k in range(4)]
    side = z // 2
    mate, near, far = z + 1 - 2 * (z % 2), 2 - side, 3 - 3 * side
    is_end = z % 2 == side
    is_mid = z % 2 != side
    to_mate, to_near, to_far = ({"dp": other * 2 + x} for other in (mate, near, far))
    friends = (to_p, to_o, to_x, to_z[1], to_z[2], to_z[3])
    g1, b1, g2, b2 = (gains[n:n + 1, :] for n in range(4))

    def rc(name, i, src, dst, dev, arrival=None):
        at = COPIES[name][0] + i
        to = at if arrival is None else COPIES[name][0] + arrival
        return pltpu.make_async_remote_copy(
            src_ref=src, dst_ref=dst, send_sem=ssem.at[at], recv_sem=rsem.at[to], device_id=dev, device_id_type=MESH)

    def lc(i, src, dst):
        return pltpu.make_async_copy(src, dst, lsem.at[i])

    top = pl.ds(0, sp)
    barrier = pltpu.get_barrier_semaphore()
    for dev in friends:
        pl.semaphore_signal(barrier, inc=1, device_id=dev, device_id_type=MESH)

    def attention_weights(first):
        cps = [lc(first + n, wqkv.at[:, pl.ds(n * width, width)], WO.at[pl.ds(n * width, width)]) for n in range(3)]
        return cps + [lc(first + 3, wo, WO.at[pl.ds(3 * width, width)])]

    load_x = [lc(i, xb.at[i], GE.at[pl.ds(i * sp, sp)]) for i in range(2)]
    load_w = attention_weights(2)
    load_g = [lc(6 + i, gl.at[i], G.at[0, i, top]) for i in range(2)]
    load_in = lc(8, w_in.at[0], WI)
    for cp in load_x + load_w + load_g + [load_in]:
        cp.start()

    shape = SL.shape[2:]
    before = (sub((LP, LP)) < lane((LP, LP))).astype(BF)
    base = jnp.zeros((shape[0], 1), F32)
    for i in range(2):
        r = jnp.concatenate([routes[i], jnp.full((2, LP - seq), -1, jnp.int32)], axis=1)
        member = (r[0:1, :] == sub(shape)) | (r[1:2, :] == sub(shape))
        member = member & (live[0] > i)
        m = member.astype(F32)
        place = dot(m.astype(BF), before) + base
        SL[0, i] = jnp.where(member, place, -1.0)
        base = base + jnp.sum(m, axis=1, keepdims=True)
    WR[...] = jnp.zeros(WR.shape, BF)
    WR[0:experts, :] = wrt[...]
    for s in range(4):
        for i in range(2):
            U[s, i, sp:, :] = jnp.zeros((LP - sp, width), BF)
            G[s, i, sp:, :] = jnp.zeros((LP - sp, width), BF)

    uP = [rc("uP", i, U.at[0, i, top], U.at[1, i, top], to_p) for i in range(2)]
    uO = [rc("uO", i, U.at[0, i, top], U.at[2, i, top], to_o) for i in range(2)]
    uF = [rc("uF", i, U.at[2, i, top], U.at[3, i, top], to_p) for i in range(2)]
    gP = [rc("gP", i, G.at[0, i, top], G.at[1, i, top], to_p) for i in range(2)]
    gO = [rc("gO", i, G.at[0, i, top], G.at[2, i, top], to_o) for i in range(2)]
    gF = [rc("gF", i, G.at[2, i, top], G.at[3, i, top], to_p) for i in range(2)]
    sP = rc("sP", 0, SL.at[0], SL.at[1], to_p)
    sO = rc("sO", 0, SL.at[0], SL.at[2], to_o)
    sF = rc("sF", 0, SL.at[2], SL.at[3], to_p)

    low = lane((sp, 128)) < HEAD_DIM
    keys = lane((sp, sp)) < seq
    scaling = HEAD_DIM ** -0.5
    with sc("ln1"):
        for i in range(2):
            load_x[i].wait()
            r0 = slice(i * sp, (i + 1) * sp)
            n1, _ = norm_parts(GE[r0, :].astype(F32))
            D[r0, 3 * width:] = (n1 * g1 + b1).astype(BF)
    with sc("barrier"):
        pl.semaphore_wait(barrier, 6)
    sO.start()
    sP.start()
    for i in range(2):
        load_g[i].wait()
        gO[i].start()
        gP[i].start()
    with sc("qkv"):
        for n in range(3):
            load_w[n].wait()
            D[0:rows, n * width:(n + 1) * width] = dot(
                D[0:rows, 3 * width:], WO[n * width:(n + 1) * width, :]).astype(BF)
    LS[...] = jnp.zeros(LS.shape, F32)

    def attend(i, per):
        r0 = slice(i * sp, (i + 1) * sp)

        def pair(step, carry):
            lse = LS[i]
            for inner in range(per):
                h = step * per + inner

                def cols(n):
                    return pl.ds(pl.multiple_of(h * 128 + n * width, 128), 128)

                q, k, v = D[r0, cols(0)], D[r0, cols(1)], D[r0, cols(2)]
                outs = []
                for side in range(2):
                    mine = low if side == 0 else ~low
                    s = dot_nt(jnp.where(mine, q, jnp.zeros_like(q)), k) * scaling
                    s = jnp.where(keys, s, NEG)
                    peak = jnp.max(s, axis=-1, keepdims=True)
                    e = jnp.exp(s - peak)
                    total = jnp.sum(e, axis=-1, keepdims=True)
                    lse = jnp.where(lane((sp, 128)) == 2 * h + side, peak + jnp.log(total), lse)
                    outs.append(dot((e / total).astype(BF), v))
                D[rows + i * sp:rows + (i + 1) * sp, cols(0)] = jnp.where(low, outs[0], outs[1]).astype(BF)
            LS[i] = lse
            return carry

        lax.fori_loop(0, width // 128 // per, pair, 0)

    for i in range(2):
        with sc("attend"):
            attend(i, 2)
        with sc("proj_ln2"):
            if i == 0:
                load_w[3].wait()
            r1 = slice(rows + i * sp, rows + (i + 1) * sp)
            h1 = GE[i * sp:(i + 1) * sp, :].astype(F32) + dot(D[r1, 0:width], WO[3 * width:, :])
            H[i] = h1
            n2, _ = norm_parts(h1)
            U[0, i, :sp, :] = (n2 * g2 + b2).astype(BF)
        uO[i].start()
        uP[i].start()
    keep = [lc(0, D.at[pl.ds(0, rows)], qa_h), lc(1, D.at[pl.ds(rows, rows), pl.ds(0, width)], c_h)]
    keep += [lc(3 + i, U.at[0, i, top], u_h.at[pl.ds(i * sp, sp)]) for i in range(2)]
    load_out = lc(2, w_out.at[0], WO)
    for cp in keep + [load_out]:
        cp.start()

    def onehot(s):
        want = sub((LP, LP)).astype(F32)
        parts = [(want == SL[s, i, pl.ds(ep, 1), :]).astype(BF) for i in range(2)]
        return jnp.concatenate(parts, axis=1)

    def gather(s):
        X[s * LP:(s + 1) * LP, :] = dot(onehot(s), U[s].reshape(2 * LP, width)).astype(BF)

    tile = 512
    tiles = f // tile
    c0 = 0.7978845608028654
    c1 = c0 * 0.044715

    def hidden(rs, cols):
        v = dot(X[rs, :], WI[:, cols])
        w = v * v
        t = jnp.tanh(v * (c0 + c1 * w))
        h = 0.5 + 0.5 * t
        M[rs, cols] = (v * h).astype(BF)
        D[rs, cols] = (h + h * (1.0 - t) * (v * (c0 + 3.0 * c1 * w))).astype(BF)

    def gate(rs):
        r = dot_nt(X[rs, :], WR[...])
        r = jnp.where(lane(r.shape) < experts, r, NEG)
        r = jnp.exp(r - jnp.max(r, axis=-1, keepdims=True))
        r = r / jnp.sum(r, axis=-1, keepdims=True)
        GD[rs, 0:1] = jnp.sum(jnp.where(lane(r.shape) == ep, r, 0.0), axis=-1, keepdims=True)

    first_half, second_half = slice(0, half_rows), slice(half_rows, 2 * half_rows)

    def first_in(n, carry):
        hidden(first_half, pl.ds(pl.multiple_of(n * tile, tile), tile))
        return carry

    def gather_grads(s):
        rs = slice(s * LP, (s + 1) * LP)
        got = dot(onehot(s), G[s].reshape(2 * LP, width))
        GE[rs, :] = got.astype(BF)
        DT[:, rs] = jnp.transpose(GD[rs, 0:1] * got).astype(BF)

    with sc("wait_uP"):
        gather(0)
        sP.wait_recv()
        for i in range(2):
            uP[i].wait_recv()
        gather(1)
        load_in.wait()
        for cp in keep:
            cp.wait()
    with sc("expert_in_0"):
        gate(first_half)
        lax.fori_loop(0, tiles, first_in, 0)
    with sc("wait_gO"):
        sO.wait_recv()
        sF.start()
        for i in range(2):
            gO[i].wait_recv()
            gF[i].start()
        for i in range(2):
            gP[i].wait_recv()
        gather_grads(0)
        gather_grads(1)
    with sc("wait_uO"):
        for i in range(2):
            uO[i].wait_recv()
            uF[i].start()
        gather(2)
    with sc("wait_uF"):
        sF.wait_recv()
        for i in range(2):
            uF[i].wait_recv()
        gather(3)
        gate(second_half)
    with sc("wait_gF"):
        gather_grads(2)
        for i in range(2):
            gF[i].wait_recv()
        gather_grads(3)

    def ox(t):
        return rc("ox", t, GOs.at[t], GOx.at[t], to_x)

    def ix(j):
        return rc("ix", j, GIs.at[j], GIx.at[j], to_x)

    def oq(t):
        return rc("oq", t, GOk.at[t], DT.at[:, pl.ds(t * (width // 2), width // 2)], to_mate)

    oz = rc("oz", 0, GOk.at[2], GOz.at[0], to_mate)
    oc = [rc("oc", t, GOk.at[t], GOz.at[1], dev, 0) for t, dev in enumerate((to_far, to_near))]

    def iq(j, t):
        return rc("iq", j * 2 + t, GIk.at[j, (far, near)[t]], GJ.at[t] if j == 0 else
                  DT.at[pl.ds((j * 2 + t) * (width // 8), width // 8), pl.ds(0, width)], to_mate)

    def jq(t):
        return rc("jq", t, GIs.at[0, (far, near)[t]], GJ.at[2 + t], to_mate)

    jz = rc("jz", 0, GIs.at[0, mate], GIx.at[0, 0], to_mate)

    def jc(t):
        return rc("jc", t, GIs.at[0, (far, near)[t]], GIx.at[0, 1], (to_far, to_near)[t], 0)

    ix0 = rc("ix", 0, GIs.at[0, z], GIx.at[0, 2], to_x)

    def iz(j):
        return rc("iz", j, GIk.at[j, mate], GIz.at[0, j], to_mate)

    def ic(j, t):
        return rc("ic", j * 2 + t, GIk.at[j, (far, near)[t]], GIz.at[1, j], (to_far, to_near)[t], j * 2)

    def w_out_tile(t, carry):
        is0, is3 = (3 - t) // 3, t // 3
        is2 = t // 2 - is3
        zp = is0 * far + (1 - is0 - is2 - is3) * near + is2 * mate + is3 * z
        cols = pl.ds(pl.multiple_of(zp * width, width), width)
        for piece in range(3):
            hidden(second_half, pl.ds(pl.multiple_of(zp * width + piece * 256, 256), 256))
        r = dot(DT[...], M[:, cols])
        lo, hi = r[:, :width // 2], r[:, width // 2:]
        GOs[t] = jnp.where(x == 0, hi, lo).astype(BF)
        GOk[t] = jnp.where(x == 0, lo, hi).astype(BF)
        ox(t).start()
        return carry

    with sc("w_out_tiles"):
        lax.fori_loop(0, 4, w_out_tile, 0)
    pl.semaphore_signal(credit.at[0], inc=1, device_id=to_mate, device_id_type=MESH)

    def take_o(t):
        with sc("take_o%d" % t):
            ox(t).wait_recv()
            GOk[t] = (GOk[t].astype(F32) + GOx[t].astype(F32)).astype(BF)
            if t == 0:
                pl.semaphore_wait(credit.at[0], 1)
            if t < 2:
                @pl.when(is_end)
                def _():
                    oq(t).start()
            if t == 2:
                oz.start()

    def pass_o(t):
        with sc("pass_o%d" % t):
            @pl.when(is_mid)
            def _():
                oq(t).wait_recv()
                GOk[t] = (GOk[t].astype(F32) + DT[:, t * (width // 2):(t + 1) * (width // 2)].astype(F32)).astype(BF)
                oc[t].start()
            if t == 1:
                pl.semaphore_signal(credit.at[1], inc=1, device_id=to_mate, device_id_type=MESH)

    def take_i(j):
        with sc("take_i%d" % j):
            if j > 0:
                ix(j).wait_recv()
                GIk[j] = (GIk[j].astype(F32) + GIx[j].astype(F32)).astype(BF)
            if j == 1:
                pl.semaphore_wait(credit.at[1], 1)

            @pl.when(is_end)
            def _():
                for t in range(2):
                    iq(j, t).start()
                    if j == 0:
                        jq(t).start()

            iz(j).start()
            if j == 0:
                jz.start()

    def pass_i(j):
        with sc("pass_i%d" % j):
            @pl.when(is_mid)
            def _():
                for t in range(2):
                    at = (far, near)[t]
                    iq(j, t).wait_recv()
                    if j == 0:
                        came = GJ[t]
                    else:
                        r0 = (j * 2 + t) * (width // 8)
                        came = DT[r0:r0 + width // 8, 0:width]
                    GIk[j, at] = (GIk[j, at].astype(F32) + came.astype(F32)).astype(BF)
                    ic(j, t).start()
                    if j == 0:
                        jq(t).wait_recv()
                        GIs[0, at] = (GIs[0, at].astype(F32) + GJ[2 + t].astype(F32)).astype(BF)
                        jc(t).start()

    def cross_first():
        with sc("cross_first"):
            jz.wait_recv()
            rc("jc", 0, GIs.at[0, far], GIx.at[0, 1], to_far, 0).wait_recv()
            total = GIs[0, z].astype(F32) + GIx[0, 0].astype(F32) + GIx[0, 1].astype(F32)
            GIs[0, z] = total.astype(BF)
            ix0.start()

    load_out.wait()
    GD[:, 1:2] = jnp.zeros((GD.shape[0], 1), F32)

    def expert_back(n, carry):
        cols = pl.ds(pl.multiple_of(n * tile, tile), tile)
        for first in (0, half_rows):
            rs = slice(first, first + half_rows)
            back = dot_nt(GE[rs, :], WO[cols, :])
            GD[rs, 1:2] += jnp.sum(back * M[rs, cols].astype(F32), axis=-1, keepdims=True)
            D[rs, cols] = (D[rs, cols].astype(F32) * (GD[rs, 0:1] * back)).astype(BF)
        return carry

    with sc("expert_back"):
        lax.fori_loop(0, tiles // 2, expert_back, 0)
    take_o(0)
    with sc("expert_back"):
        lax.fori_loop(tiles // 2, tiles, expert_back, 0)

    dP = [rc("dP", i, U.at[1, i, top], RP.at[i], to_p) for i in range(2)]
    dD = [rc("dD", i, U.at[3, i, top], RD.at[i], to_p) for i in range(2)]
    dO = [rc("dO", i, U.at[2, i, top], RO.at[i], to_o) for i in range(2)]
    eP = rc("eP", 0, ES.at[1], EP, to_p)
    eD = rc("eD", 0, ES.at[3], ED, to_p)
    eO = rc("eO", 0, ES.at[2], EO, to_o)
    yP = [rc("yP", i, G.at[1, i, top], YP.at[i], to_p) for i in range(2)]
    yD = [rc("yD", i, G.at[3, i, top], YD.at[i], to_p) for i in range(2)]
    yO = [rc("yO", i, G.at[2, i, top], YO.at[i], to_o) for i in range(2)]

    for cp in uP + uO + uF:
        cp.wait_send()

    def scatter(s, values):
        return dot_tn(onehot(s), values)

    def back_rows(step, carry):
        s = 3 - step
        rs = pl.ds(pl.multiple_of(s * LP, LP), LP)
        U[s] = scatter(s, dot_nt(D[rs, :], WI[...]).astype(BF)).astype(BF).reshape(2, LP, width)
        dg = GD[rs, 1:2]
        hi = dg.astype(BF)
        rest = (dg - hi.astype(F32)).astype(BF)
        at = lane((LP, 128))
        zero = jnp.zeros((LP, 128), BF)
        two = jnp.where(at == ep, hi, zero) + jnp.where(at == ep + 64, rest, zero)
        ES[s] = scatter(s, two).astype(BF).reshape(2, LP, 128)

        @pl.when(step == 0)
        def _():
            for cp in dD + [eD]:
                cp.start()

        @pl.when(step == 2)
        def _():
            for cp in dP + [eP]:
                cp.start()

        return carry

    with sc("du"):
        lax.fori_loop(0, 4, back_rows, 0)
    with sc("combine_du"):
        for i in range(2):
            dD[i].wait_recv()
            U[2, i, :sp, :] = (U[2, i, :sp, :].astype(F32) + RD[i].astype(F32)).astype(BF)
            dO[i].start()
        eD.wait_recv()
        ES[2] = ES[2] + ED[...]
        eO.start()
    pass_o(0)
    take_o(1)

    def w_in_tile(j, carry):
        r = dot_tn(X[...], D[:, pl.ds(pl.multiple_of(j * width, width), width)]).reshape(4, 2, width // 8, width)
        first, second = r[:, 0], r[:, 1]
        GIs[j] = jnp.where(x == 0, second, first).astype(BF)
        GIk[j] = jnp.where(x == 0, first, second).astype(BF)

        @pl.when(j > 0)
        def _():
            ix(j).start()

        return carry

    with sc("w_in_tiles"):
        lax.fori_loop(0, 4, w_in_tile, 0)
    take_i(0)
    for dev in friends:
        pl.semaphore_signal(free, inc=1, device_id=dev, device_id_type=MESH)

    for cp in gP + gO + gF:
        cp.wait_send()
    for i in range(2):
        X[half_rows + i * sp:half_rows + (i + 1) * sp, :] = G[0, i, :sp, :]

    def out_rows(step, carry):
        s = 3 - step
        rs = pl.ds(pl.multiple_of(s * LP, LP), LP)
        o = dot(M[rs, :], WO[...]).astype(BF).astype(F32)
        G[s] = scatter(s, (GD[rs, 0:1] * o).astype(BF)).astype(BF).reshape(2, LP, width)

        @pl.when(step == 0)
        def _():
            for cp in yD:
                cp.start()

        @pl.when(step == 2)
        def _():
            for cp in yP:
                cp.start()

        return carry

    with sc("o"):
        lax.fori_loop(0, 4, out_rows, 0)
    pass_o(1)
    late = attention_weights(3) + [
        lc(7, qa_h, M.at[pl.ds(0, rows)]), lc(8, c_h, M.at[pl.ds(rows, rows), pl.ds(0, width)])
    ] + [lc(9 + i, xb.at[i], GE.at[pl.ds(rows + i * sp, sp)]) for i in range(2)]
    late.append(lc(11, u_h, M.at[pl.ds(rows, rows), pl.ds(width, width)]))
    for cp in late:
        cp.start()
    with sc("combine_y"):
        for i in range(2):
            yD[i].wait_recv()
            G[2, i, :sp, :] = (G[2, i, :sp, :].astype(F32) + YD[i].astype(F32)).astype(BF)
            yO[i].start()
    take_o(2)
    for cp in late:
        cp.wait()

    with sc("wait_du"):
        for i in range(2):
            dP[i].wait_recv()
            dO[i].wait_recv()
        eP.wait_recv()
        eO.wait_recv()
    with sc("ln2_back"):
        router = jnp.zeros((width, 128), F32)
        gain2 = jnp.zeros((1, width), F32)
        bias2 = jnp.zeros((1, width), F32)
        for i in range(2):
            du = U[0, i, :sp, :].astype(F32) + RP[i].astype(F32) + RO[i].astype(F32)
            back = ES[0, i, :sp, :].astype(F32) + EP[i, :sp, :].astype(F32) + EO[i, :sp, :].astype(F32)
            back = back + pltpu.roll(back, 64, axis=1)
            own = M[rows + i * sp:rows + (i + 1) * sp, width:2 * width]
            r = dot_nt(own, WR[...])
            r = jnp.where(lane(r.shape) < experts, r, NEG)
            r = jnp.exp(r - jnp.max(r, axis=-1, keepdims=True))
            r = r / jnp.sum(r, axis=-1, keepdims=True)
            dl = (r * (back - jnp.sum(r * back, axis=-1, keepdims=True))).astype(BF)
            router = router + dot_tn(own, dl)
            du = du + dot(dl, WR[...])
            n2, inv2 = norm_parts(H[i])
            gain2 = gain2 + jnp.sum(du * n2, axis=0, keepdims=True)
            bias2 = bias2 + jnp.sum(du, axis=0, keepdims=True)
            on = (live[0] > i).astype(F32)
            dh = X[half_rows + i * sp:half_rows + (i + 1) * sp, :].astype(F32) * on + norm_backward(du * g2, n2, inv2)
            DH[i] = dh
            GE[i * sp:(i + 1) * sp, :] = dh.astype(BF)
        SM[...] = router.astype(BF)

    def part(e, b):
        return pl.ds(pl.multiple_of(e * shard, shard), shard), pl.ds(b * width, width)

    def cp_c(b, i):
        return rc("C", b * 2 + i, WI.at[part(i * 2 + 1 - core, b)], D.at[pl.ds(i * shard, shard), pl.ds(b * width, width)], to_p)

    def cp_y(b):
        return rc("Y", b, WI.at[part((1 - y) * 2 + core, b)], D.at[pl.ds(2 * shard, shard), pl.ds(b * width, width)], to_o)

    def own_rows(k=0, n=shard):
        return pl.ds(pl.multiple_of(ep * shard + k * block, block), n)

    def half(b, h):
        return pl.ds(pl.multiple_of(b * width + h * (width // 2), 128), width // 2)

    def rest(quarter, b, second):
        return D.at[pl.ds(quarter * shard, shard), pl.ds(b * width + second * (width // 2), width // 2)]

    def cp_x(b):
        return rc("X", b, WI.at[own_rows(), half(b, 1 - x)], rest(3, b, 0), to_x)

    def cp_r1(b):
        return rc("R1", b, WI.at[own_rows(), half(b, x)], rest(4, b, 0), to_mate)

    def cp_r2(b):
        return rc("R2", b, WI.at[own_rows(), half(b, x)], rest(4, b, 1), to_near)

    def cp_r3(b):
        return rc("R3", b, rest(0, b, 0), rest(0, b, 0), to_mate)

    def cp_ax(b):
        return rc("AX", b, rest(0, b, 0), rest(1, b, 0), to_x)

    def stage_c(b):
        for i in range(2):
            cp_c(b, i).start()

    def stage_y(b):
        with sc("stage_y%d" % b):
            for i in range(2):
                cp_c(b, i).wait_recv()
            for i in range(2):
                at = part(i * 2 + core, b)
                WI[at] = (WI[at].astype(F32) + D[i * shard:(i + 1) * shard, b * width:(b + 1) * width].astype(F32)).astype(BF)
            cp_y(b).start()

    def stage_x(b):
        with sc("stage_x%d" % b):
            cp_y(b).wait_recv()
            at = part(ep, b)
            WI[at] = (WI[at].astype(F32) + D[2 * shard:3 * shard, b * width:(b + 1) * width].astype(F32)).astype(BF)
            cp_x(b).start()

    def add_own(b, came):
        at = own_rows(), half(b, x)
        WI[at] = (WI[at].astype(F32) + came[...].astype(F32)).astype(BF)

    def stage_r1(b):
        with sc("stage_r1_%d" % b):
            cp_x(b).wait_recv()
            add_own(b, rest(3, b, 0))

            @pl.when(is_end)
            def _():
                cp_r1(b).start()

    def stage_r2(b):
        with sc("stage_r2_%d" % b):
            @pl.when(is_mid)
            def _():
                cp_r1(b).wait_recv()
                add_own(b, rest(4, b, 0))
                cp_r2(b).start()

    def stage_r3(b):
        with sc("stage_r3_%d" % b):
            @pl.when(is_mid)
            def _():
                cp_r2(b).wait_recv()
                total = WI[own_rows(), half(b, x)].astype(F32) + rest(4, b, 1)[...].astype(F32)
                rest(0, b, 0)[...] = total.astype(BF)
                cp_r3(b).start()

            @pl.when(is_end)
            def _():
                cp_r3(b).wait_recv()

            cp_ax(b).start()

    with sc("attn_out_grads"):
        X[half_rows:half_rows + rows, :] = dot_nt(GE[0:rows, :], WO[3 * width:, :]).astype(BF)
        WI[:, 3 * width:] = dot_tn(M[rows:2 * rows, 0:width], GE[0:rows, :]).astype(BF)
    with sc("wait_free"):
        pl.semaphore_wait(free, 6)
    stage_c(3)

    def pair_back(h, carry):
        def cols(n):
            return pl.ds(pl.multiple_of(h * 128 + n * width, 128), 128)

        for i in range(2):
            r0 = slice(i * sp, (i + 1) * sp)
            q, k, v = M[r0, cols(0)], M[r0, cols(1)], M[r0, cols(2)]
            dc = X[half_rows + i * sp:half_rows + (i + 1) * sp, cols(0)]
            parts = []
            for side in range(2):
                here = low if side == 0 else ~low
                zero = jnp.zeros_like(q)
                lse = jnp.sum(jnp.where(lane((sp, 128)) == 2 * h + side, LS[i], 0.0), axis=-1, keepdims=True)
                s = dot_nt(jnp.where(here, q, zero), k) * scaling
                p = jnp.exp(jnp.where(keys, s, NEG) - lse)
                dv = dot_tn(p.astype(BF), dc)
                dp_ = dot_nt(jnp.where(here, dc, zero), v)
                ds = (p * (dp_ - jnp.sum(p * dp_, axis=-1, keepdims=True))).astype(BF)
                parts.append((dot(ds, k) * scaling, dot_tn(ds, q) * scaling, dv))
            r1 = slice(rows + i * sp, rows + (i + 1) * sp)
            for n in range(3):
                M[r1, cols(n + 1)] = jnp.where(low, parts[0][n], parts[1][n]).astype(BF)
        return carry

    with sc("attention_back_a"):
        lax.fori_loop(0, width // 256, pair_back, 0)
    stage_y(3)
    pass_i(0)
    take_o(3)
    with sc("attention_back_b"):
        lax.fori_loop(width // 256, width // 128, pair_back, 0)
    for n in range(3):
        with sc("qkv_grads"):
            grads = M[rows:2 * rows, (n + 1) * width:(n + 2) * width]
            WI[:, n * width:(n + 1) * width] = dot_tn(M[0:rows, 3 * width:], grads).astype(BF)
        stage_c(n)
    stage_x(3)
    take_i(1)
    with sc("ln1_back"):
        gain1 = jnp.zeros((1, width), F32)
        bias1 = jnp.zeros((1, width), F32)
        for i in range(2):
            r1 = slice(rows + i * sp, rows + (i + 1) * sp)
            grad = dot_nt(M[r1, width:2 * width], WO[0:width, :])
            for n in range(1, 3):
                grad = grad + dot_nt(M[r1, (n + 1) * width:(n + 2) * width], WO[n * width:(n + 1) * width, :])
            n1, inv1 = norm_parts(GE[r1, :].astype(F32))
            gain1 = gain1 + jnp.sum(grad * n1, axis=0, keepdims=True)
            bias1 = bias1 + jnp.sum(grad, axis=0, keepdims=True)
            DH[i] = DH[i] + norm_backward(grad * g1, n1, inv1)
        vectors = jnp.concatenate([jnp.zeros((4, width), F32), gain1, bias1, gain2, bias2], axis=0)
        vectors = jnp.concatenate([vectors, jnp.zeros((120, width), F32)], axis=0)
        SM[...] = (SM[...].astype(F32) + jnp.transpose(vectors)).astype(BF)

    def small(e):
        return pl.ds(pl.multiple_of(e * shard, shard), shard)

    mC = [rc("mC", i, SM.at[small(i * 2 + 1 - core)], SMx.at[i], to_p) for i in range(2)]
    mY = rc("mY", 0, SM.at[small((1 - y) * 2 + core)], SMx.at[2], to_o)
    mX = rc("mX", 0, SM.at[small(ep)], SMx.at[3], to_x)
    mZ = [rc("mZ", k - 1, SMx.at[3], SMx.at[3 + k], to_z[k]) for k in range(1, 4)]
    for cp in mC:
        cp.start()
    for b in range(3):
        stage_y(b)
    with sc("small_y"):
        for i in range(2):
            mC[i].wait_recv()
            at = small(i * 2 + core)
            SM[at, :] = (SM[at, :].astype(F32) + SMx[i].astype(F32)).astype(BF)
        mY.start()
    with sc("block_out"):
        for i in range(2):
            yP[i].wait_recv()
            yO[i].wait_recv()
            on = (live[0] > i).astype(F32)
            mix = G[0, i, :sp, :].astype(F32) + YP[i].astype(F32) + YO[i].astype(F32)
            bo_o[i] = ((H[i] + mix) * on).astype(BF)
    cross_first()
    with sc("o_sum"):
        oz.wait_recv()
        rc("oc", 0, GOk.at[0], GOz.at[1], to_far, 0).wait_recv()
        total = GOk[3].astype(F32) + GOz[0].astype(F32) + GOz[1].astype(F32)
        GOk[3] = total.astype(BF)
        outs = [lc(0, GOk.at[3], wo_o)]
        outs[0].start()
    pass_i(1)
    take_i(2)
    stage_x(0)
    pass_i(2)
    stage_x(1)
    take_i(3)
    stage_x(2)
    with sc("small_x"):
        mY.wait_recv()
        at = small(ep)
        SM[at, :] = (SM[at, :].astype(F32) + SMx[2].astype(F32)).astype(BF)
        mX.start()
    stage_r1(3)
    stage_r1(0)
    pass_i(3)
    stage_r2(3)
    stage_r1(1)
    stage_r2(0)
    stage_r1(2)
    stage_r2(1)
    stage_r3(3)
    stage_r2(2)
    stage_r3(0)
    with sc("small_z"):
        mX.wait_recv()
        SMx[3] = (SM[small(ep), :].astype(F32) + SMx[3].astype(F32)).astype(BF)
        for cp in mZ:
            cp.start()
    stage_r3(1)
    stage_r3(2)
    for j in range(4):
        with sc("i_sum%d" % j):
            iz(j).wait_recv()
            ic(j, 0).wait_recv()
            total = GIk[j, z].astype(F32) + GIz[0, j].astype(F32) + GIz[1, j].astype(F32)
            if j == 0:
                ix0.wait_recv()
                total = total + GIx[0, 2].astype(F32)
            GIx[j, 3] = total.astype(BF)
            outs.append(lc(1 + j, GIx.at[j, 3], wi_o.at[:, pl.ds(j * width, width)]))
            outs[-1].start()
    with sc("small_sum"):
        for cp in mZ:
            cp.wait_recv()
        total = SMx[3].astype(F32) + SMx[4].astype(F32) + SMx[5].astype(F32) + SMx[6].astype(F32)
        sm_o[...] = jnp.transpose(total)[0:8, :]
    for b in (3, 0, 1, 2):
        with sc("wait_ax"):
            cp_ax(b).wait_recv()
            outs.append(lc(5 + b, rest(0, b, 0), sg_o.at[:, half(b, x)]))
            outs[-1].start()
            outs.append(lc(9 + b, rest(1, b, 0), sg_o.at[:, half(b, 1 - x)]))
            outs[-1].start()
    with sc("drain"):
        for cp in dP + dD + dO + yP + yD + yO + [sP, sO, sF, eP, eD, eO, mY, mX] + mC + mZ:
            cp.wait_send()
        for t in range(4):
            ox(t).wait_send()
            (ix(t) if t else ix0).wait_send()
            iz(t).wait_send()
            cp_y(t).wait_send()
            cp_x(t).wait_send()
            cp_ax(t).wait_send()
            for i in range(2):
                cp_c(t, i).wait_send()
        oz.wait_send()
        jz.wait_send()

        @pl.when(is_end)
        def _():
            for t in range(4):
                cp_r1(t).wait_send()
            for t in range(2):
                oq(t).wait_send()
                jq(t).wait_send()
                for j in range(4):
                    iq(j, t).wait_send()

        @pl.when(is_mid)
        def _():
            for t in range(4):
                cp_r2(t).wait_send()
                cp_r3(t).wait_send()
            for t in range(2):
                oc[t].wait_send()
                jc(t).wait_send()
                for j in range(4):
                    ic(j, t).wait_send()

        for cp in outs:
            cp.wait()


def fast_body(n_ep, tokens, live, routes, g1, b1, wqkv, wo, g2, b2, wr, w_in, w_out, cot):
    slots, seq, width = tokens.shape
    sp = (seq + 15) // 16 * 16
    f = w_in.shape[2]
    cap = n_ep * LP
    pads = ((0, 0), (0, sp - seq), (0, 0))
    gl = jnp.pad(cot, pads)
    xb = jnp.pad(tokens, pads)
    gains = jnp.stack([g1, b1, g2, b2])
    sds = jax.ShapeDtypeStruct
    vm = pl.BlockSpec(memory_space=pltpu.VMEM)
    anys = pl.BlockSpec(memory_space=pl.ANY)
    b = lambda *shape: pltpu.VMEM(shape, BF)
    g = lambda *shape: pltpu.VMEM(shape, F32)
    shard = width // n_ep
    bo, gt, sm, wo_t, wi, sg, _, _, _ = pl.pallas_call(
        functools.partial(layer_kernel, n_ep, seq),
        name="layer",
        out_shape=(
            sds((slots, sp, width), BF), sds((slots, sp, width), F32), sds((8, shard), F32),
            sds((width, f // 8), BF), sds((width // 8, f), BF), sds((shard, 4 * width), BF),
            sds((2 * sp, 4 * width), BF), sds((2 * sp, width), BF), sds((2 * sp, width), BF),
        ),
        in_specs=[pl.BlockSpec(memory_space=pltpu.SMEM)] + [vm] * 3 + [anys] * 6,
        out_specs=[vm] * 3 + [anys] * 6,
        scratch_shapes=[
            b(4, 2, LP, width), b(4, 2, LP, width), g(4, 2, 8, LP), b(128, width), b(width, f), b(f, width),
            b(cap, f), b(cap, f), b(cap, width), b(cap, width), b(width, cap),
            b(4, width, f // 8), b(4, width, f // 8), b(4, width, f // 8), b(2, width, f // 8),
            b(4, 4, width // 8, width), b(4, 4, width // 8, width), b(4, 4, width // 8, width),
            b(2, 4, width // 8, width), b(4, width // 8, width),
            g(slots, sp, width), g(slots, sp, 128), g(cap, 2),
            b(2, sp, width), b(2, sp, width), b(2, sp, width),
            b(2, LP, 128), b(2, LP, 128), b(2, LP, 128), b(4, 2, LP, 128),
            b(2, sp, width), b(2, sp, width), b(2, sp, width), b(width, 128), b(7, shard, 128),
            pltpu.SemaphoreType.DMA((N_COPIES,)), pltpu.SemaphoreType.DMA((N_COPIES,)),
            pltpu.SemaphoreType.DMA((14,)), pltpu.SemaphoreType.REGULAR, pltpu.SemaphoreType.REGULAR((2,)),
        ],
        compiler_params=pltpu.CompilerParams(
            collective_id=0, has_side_effects=True, vmem_limit_bytes=67043328),
    )(live, jnp.transpose(routes, (0, 2, 1)), gains, jnp.transpose(wr), xb, gl, w_in, w_out, wqkv, wo)
    return (
        bo[:, :seq], gt[:, :seq], sm[4], sm[5], sg[:, :3 * width].astype(F32), sg[:, 3 * width:].astype(F32),
        sm[6], sm[7], jnp.transpose(sm[:n_ep]), wi.astype(F32)[None], jnp.transpose(wo_t).astype(F32)[None],
    )


def general_body(
    tokens,
    live_images,
    routes,
    ln1_gain,
    ln1_bias,
    query_key_value_weight,
    attention_output_weight,
    ln2_gain,
    ln2_bias,
    w_router,
    w_in,
    w_out,
    cotangent,
):
    slot_count, seq_len, model_width = tokens.shape
    row_count = slot_count * seq_len
    expert_count = w_router.shape[1]
    hidden_width = w_in.shape[2]
    capacity = ((2 * row_count + expert_count - 1) // expert_count * 5 // 4 + 7) // 8 * 8
    scaling = HEAD_DIM ** (-0.5)
    inputs = tokens.astype(jnp.float32).reshape(row_count, model_width)
    normed1, inverse1 = norm_parts(inputs)
    attn_in = (normed1 * ln1_gain + ln1_bias).astype(jnp.bfloat16)
    qkv_rows = jnp.dot(attn_in, query_key_value_weight, preferred_element_type=jnp.float32).astype(
        jnp.bfloat16
    )
    qkv_heads = qkv_rows.reshape(slot_count, seq_len, 3, HEADS, HEAD_DIM)
    queries = qkv_heads[:, :, 0]
    keys_all = qkv_heads[:, :, 1]
    values_all = qkv_heads[:, :, 2]
    scores = (
        jnp.einsum("sqhc,skhc->shqk", queries, keys_all, preferred_element_type=jnp.float32)
        * scaling
    )
    row_peak = jnp.max(scores, axis=-1, keepdims=True)
    raised = jnp.exp(scores - row_peak)
    totals = jnp.sum(raised, axis=-1, keepdims=True)
    log_total = row_peak + jnp.log(totals)
    weights = (raised / totals).astype(jnp.bfloat16)
    attended_context = jnp.einsum(
        "shqk,skhc->sqhc", weights, values_all, preferred_element_type=jnp.float32
    )
    attended_context = attended_context.astype(jnp.bfloat16).reshape(row_count, model_width)
    hidden1 = inputs + jnp.dot(
        attended_context, attention_output_weight, preferred_element_type=jnp.float32
    )
    normed2, inverse2 = norm_parts(hidden1)
    moe_in = (normed2 * ln2_gain + ln2_bias).astype(jnp.bfloat16)
    router = jax.nn.softmax(jnp.dot(moe_in, w_router, preferred_element_type=jnp.float32), axis=-1)
    chosen = routes.reshape(row_count, 2)
    expert_ids = jnp.arange(expert_count, dtype=jnp.int32)
    picked = (chosen[:, :, None] == expert_ids[None, None, :]).astype(jnp.float32)
    gates = jnp.sum(picked * router[:, None, :], axis=-1)
    token_live = (jnp.arange(row_count, dtype=jnp.int32) // seq_len < live_images[0]).astype(
        jnp.float32
    )
    pair_ids = chosen.reshape(2 * row_count)
    pair_live = jnp.repeat(token_live, 2) > 0.5
    member = ((pair_ids[:, None] == expert_ids[None, :]) & pair_live[:, None]).astype(jnp.int32)
    position = jnp.sum((jnp.cumsum(member, axis=0) - 1) * member, axis=-1)
    slot_ids = jnp.where(pair_live, pair_ids * capacity + position, -1).reshape(row_count, 2)
    lanes = jnp.arange(expert_count * capacity, dtype=jnp.int32)
    placing = (jnp.transpose(slot_ids)[:, None, :] == lanes[None, :, None]).astype(jnp.bfloat16)
    outbox = jnp.einsum("jsr,rd->sd", placing, moe_in, preferred_element_type=jnp.float32)
    outbox = outbox.astype(jnp.bfloat16).reshape(expert_count, capacity, model_width)
    inbox = lax.all_to_all(outbox, "ep", split_axis=0, concat_axis=0, tiled=True)
    flat_in = inbox.reshape(-1, model_width)
    pre_act = jnp.dot(flat_in, w_in[0], preferred_element_type=jnp.float32)
    activated = jax.nn.gelu(pre_act).astype(jnp.bfloat16)
    produced = jnp.dot(activated, w_out[0], preferred_element_type=jnp.float32).astype(jnp.bfloat16)
    coming_back = lax.all_to_all(
        produced.reshape(inbox.shape), "ep", split_axis=0, concat_axis=0, tiled=True
    )
    coming_back, pre_act = (
        coming_back,
        pre_act.reshape(inbox.shape[0], inbox.shape[1], hidden_width),
    )
    arrived_rows = inbox.reshape(-1, model_width)
    pre_rows = pre_act.reshape(-1, hidden_width)
    returned_rows = coming_back.reshape(expert_count * capacity, model_width)
    taken = jnp.einsum("jsr,sd->rjd", placing, returned_rows, preferred_element_type=jnp.float32)
    mixture = jnp.sum(gates[:, :, None] * taken, axis=1)
    block_out = (
        ((hidden1 + mixture) * token_live[:, None]).astype(jnp.bfloat16).reshape(tokens.shape)
    )
    upstream = cotangent.astype(jnp.float32).reshape(row_count, model_width) * token_live[:, None]
    gate_grads = jnp.sum(taken * upstream[:, None, :], axis=-1)
    sent_grads = (gates[:, :, None] * upstream[:, None, :]).astype(jnp.bfloat16)
    grad_outbox = jnp.einsum("jsr,rjd->sd", placing, sent_grads, preferred_element_type=jnp.float32)
    grad_outbox = grad_outbox.astype(jnp.bfloat16).reshape(expert_count, capacity, model_width)
    grad_inbox = lax.all_to_all(grad_outbox, "ep", split_axis=0, concat_axis=0, tiled=True)
    grad_rows = grad_inbox.reshape(-1, model_width)
    activated_rows, gelu_pull = jax.vjp(jax.nn.gelu, pre_rows)
    activated_low = activated_rows.astype(jnp.bfloat16)
    grad_activated = jnp.einsum(
        "rd,fd->rf", grad_rows, w_out[0], preferred_element_type=jnp.float32
    )
    grad_pre = gelu_pull(grad_activated)[0].astype(jnp.bfloat16)
    columns = activated_low
    grad_w_out = lax.psum_scatter(
        jnp.einsum("rf,rd->fd", columns, grad_rows, preferred_element_type=jnp.float32).astype(
            jnp.bfloat16
        ),
        "dp",
        scatter_dimension=0,
        tiled=True,
    ).astype(jnp.float32)
    grad_back_rows = jnp.einsum(
        "rf,df->rd", grad_pre, w_in[0], preferred_element_type=jnp.float32
    ).astype(jnp.bfloat16)
    grad_back = lax.all_to_all(
        grad_back_rows.reshape(grad_inbox.shape), "ep", split_axis=0, concat_axis=0, tiled=True
    )
    columns = arrived_rows
    grad_w_in = lax.psum_scatter(
        jnp.einsum("rd,rf->df", columns, grad_pre, preferred_element_type=jnp.float32).astype(
            jnp.bfloat16
        ),
        "dp",
        scatter_dimension=0,
        tiled=True,
    ).astype(jnp.float32)
    grad_back_flat = grad_back.reshape(expert_count * capacity, model_width)
    expert_grad = jnp.einsum(
        "jsr,sd->rd", placing, grad_back_flat, preferred_element_type=jnp.float32
    )
    grad_router_probs = jnp.sum(gate_grads[:, :, None] * picked, axis=1)
    grad_logits = router * (
        grad_router_probs - jnp.sum(router * grad_router_probs, axis=-1, keepdims=True)
    )
    grad_logits = grad_logits.astype(jnp.bfloat16)
    grad_w_router = jnp.einsum("rd,re->de", moe_in, grad_logits, preferred_element_type=jnp.float32)
    grad_moe_in = expert_grad + jnp.einsum(
        "re,de->rd", grad_logits, w_router, preferred_element_type=jnp.float32
    )
    grad_ln2_gain = jnp.sum(grad_moe_in * normed2, axis=0)
    grad_ln2_bias = jnp.sum(grad_moe_in, axis=0)
    grad_hidden1 = upstream + norm_backward(grad_moe_in * ln2_gain, normed2, inverse2)
    grad_attn = grad_hidden1.astype(jnp.bfloat16)
    grad_w_attn_out = jnp.einsum(
        "rd,re->de", attended_context, grad_attn, preferred_element_type=jnp.float32
    )
    grad_context = jnp.einsum(
        "re,de->rd", grad_attn, attention_output_weight, preferred_element_type=jnp.float32
    )
    grad_context = grad_context.astype(jnp.bfloat16).reshape(slot_count, seq_len, HEADS, HEAD_DIM)
    again = (
        jnp.einsum("sqhc,skhc->shqk", queries, keys_all, preferred_element_type=jnp.float32)
        * scaling
    )
    probs_again = jnp.exp(again - log_total)
    probs_low = probs_again.astype(jnp.bfloat16)
    grad_values = jnp.einsum(
        "shqk,sqhc->skhc", probs_low, grad_context, preferred_element_type=jnp.float32
    )
    grad_probs = jnp.einsum(
        "sqhc,skhc->shqk", grad_context, values_all, preferred_element_type=jnp.float32
    )
    grad_scores = probs_again * (
        grad_probs - jnp.sum(probs_again * grad_probs, axis=-1, keepdims=True)
    )
    grad_scores = grad_scores.astype(jnp.bfloat16)
    grad_queries = (
        jnp.einsum("shqk,skhc->sqhc", grad_scores, keys_all, preferred_element_type=jnp.float32)
        * scaling
    )
    grad_keys = (
        jnp.einsum("shqk,sqhc->skhc", grad_scores, queries, preferred_element_type=jnp.float32)
        * scaling
    )
    grad_qkv = (
        jnp.stack([grad_queries, grad_keys, grad_values], axis=2)
        .astype(jnp.bfloat16)
        .reshape(row_count, 3 * model_width)
    )
    grad_w_qkv = jnp.einsum("rd,re->de", attn_in, grad_qkv, preferred_element_type=jnp.float32)
    grad_attn_in = jnp.einsum(
        "re,de->rd", grad_qkv, query_key_value_weight, preferred_element_type=jnp.float32
    )
    grad_ln1_gain = jnp.sum(grad_attn_in * normed1, axis=0)
    grad_ln1_bias = jnp.sum(grad_attn_in, axis=0)
    grad_inputs = grad_hidden1 + norm_backward(grad_attn_in * ln1_gain, normed1, inverse1)
    shared = (
        grad_w_qkv,
        grad_w_attn_out,
        grad_w_router,
        grad_ln1_gain,
        grad_ln1_bias,
        grad_ln2_gain,
        grad_ln2_bias,
    )
    partial_sums = (
        lax.psum_scatter(
            shared[0].astype(jnp.bfloat16), "ep", scatter_dimension=0, tiled=True
        ).astype(jnp.float32),
        lax.psum_scatter(
            shared[1].astype(jnp.bfloat16), "ep", scatter_dimension=0, tiled=True
        ).astype(jnp.float32),
        lax.psum_scatter(
            shared[2].astype(jnp.bfloat16), "ep", scatter_dimension=0, tiled=True
        ).astype(jnp.float32),
        lax.psum_scatter(
            shared[3].astype(jnp.bfloat16), "ep", scatter_dimension=0, tiled=True
        ).astype(jnp.float32),
        lax.psum_scatter(
            shared[4].astype(jnp.bfloat16), "ep", scatter_dimension=0, tiled=True
        ).astype(jnp.float32),
        lax.psum_scatter(
            shared[5].astype(jnp.bfloat16), "ep", scatter_dimension=0, tiled=True
        ).astype(jnp.float32),
        lax.psum_scatter(
            shared[6].astype(jnp.bfloat16), "ep", scatter_dimension=0, tiled=True
        ).astype(jnp.float32),
    )
    shares = (
        lax.psum(partial_sums[0].astype(jnp.bfloat16), "dp").astype(jnp.float32),
        lax.psum(partial_sums[1].astype(jnp.bfloat16), "dp").astype(jnp.float32),
        lax.psum(partial_sums[2].astype(jnp.bfloat16), "dp").astype(jnp.float32),
        lax.psum(partial_sums[3].astype(jnp.bfloat16), "dp").astype(jnp.float32),
        lax.psum(partial_sums[4].astype(jnp.bfloat16), "dp").astype(jnp.float32),
        lax.psum(partial_sums[5].astype(jnp.bfloat16), "dp").astype(jnp.float32),
        lax.psum(partial_sums[6].astype(jnp.bfloat16), "dp").astype(jnp.float32),
    )
    return (
        block_out,
        grad_inputs.reshape(tokens.shape),
        shares[3],
        shares[4],
        shares[0],
        shares[1],
        shares[5],
        shares[6],
        shares[2],
        grad_w_in[None],
        grad_w_out[None],
    )


def solution(mesh):
    in_specs = (
        P(("dp", "ep"), None, None),
        P(("dp", "ep")),
        P(("dp", "ep"), None, None),
        P(),
        P(),
        P(),
        P(),
        P(),
        P(),
        P(),
        P("ep", None, None),
        P("ep", None, None),
        P(("dp", "ep"), None, None),
    )
    out_specs = (
        P(("dp", "ep"), None, None),
        P(("dp", "ep"), None, None),
        P("ep"),
        P("ep"),
        P("ep", None),
        P("ep", None),
        P("ep"),
        P("ep"),
        P("ep", None),
        P("ep", "dp", None),
        P("ep", "dp", None),
    )
    n_dp, n_ep = mesh.shape["dp"], mesh.shape["ep"]
    body = functools.partial(fast_body, n_ep) if (n_dp, n_ep) == (8, 4) else general_body
    return jax.shard_map(body, mesh=mesh, in_specs=in_specs, out_specs=out_specs, check_vma=False)
```

```python
import contextlib
import functools

import jax
import jax.numpy as jnp
from jax import lax
from jax.experimental import pallas as pl
from jax.experimental.pallas import tpu as pltpu
from jax.sharding import PartitionSpec as P

HEADS = 12
HEAD_DIM = 64
MESH = pl.DeviceIdType.MESH
BF = jnp.bfloat16
F32 = jnp.float32
eps = 1e-06
NEG = -1e30
LP = 256


def dot(a, b):
    return jnp.dot(a, b, preferred_element_type=F32)


def dot_nt(a, b):
    return lax.dot_general(a, b, (((1,), (1,)), ((), ())), preferred_element_type=F32)


def dot_tn(a, b):
    return lax.dot_general(a, b, (((0,), (0,)), ((), ())), preferred_element_type=F32)


def lane(shape):
    return lax.broadcasted_iota(jnp.int32, shape, len(shape) - 1)


def sub(shape):
    return lax.broadcasted_iota(jnp.int32, shape, len(shape) - 2)


def norm_parts(v):
    centre = jnp.mean(v, axis=-1, keepdims=True)
    shifted = v - centre
    inverse = lax.rsqrt(jnp.mean(shifted * shifted, axis=-1, keepdims=True) + eps)
    return shifted * inverse, inverse


def norm_backward(y, n, inverse):
    middle = jnp.mean(y, axis=-1, keepdims=True)
    along = jnp.mean(y * n, axis=-1, keepdims=True)
    return (y - middle - n * along) * inverse


def sc(name):
    return contextlib.nullcontext()


COPIES = {}
for _name, _count in (
    ("uP", 2), ("uO", 2), ("uF", 2), ("sP", 1), ("sO", 1), ("sF", 1), ("gP", 2), ("gO", 2), ("gF", 2),
    ("ox", 4), ("oq", 2), ("oz", 1), ("oc", 2), ("ix", 4), ("iq", 8), ("iz", 4), ("ic", 8), ("jq", 2), ("jz", 1), ("jc", 2),
    ("dP", 2), ("dD", 2), ("dO", 2), ("eP", 1), ("eD", 1), ("eO", 1), ("yP", 2), ("yD", 2), ("yO", 2),
    ("C", 8), ("Y", 4), ("X", 4), ("R1", 4), ("R2", 4), ("R3", 4), ("AX", 4), ("mC", 2), ("mY", 1), ("mX", 1), ("mZ", 3),
):
    COPIES[_name] = sum(n for _, n in COPIES.values()), _count
N_COPIES = sum(n for _, n in COPIES.values())


def layer_kernel(
    experts, seq, live, routes, g1, b1, g2, b2, wrt, xb, gl, w_in, w_out, wqkv, wo,
    bo_o, DH, sm_o, wo_o, wi_o, sg_o, qa_h, c_h, u_h,
    U, G, SL, WR, WI, WO, M, D, X, GE, DT,
    GOs, GOk, GOx, GOz, GIs, GIk, GIx, GIz, GJ,
    H, LS, GD, RP, RD, RO, EP, ED, EO, ES, YP, YD, YO, SM, SMx,
    ssem, rsem, lsem, free, credit,
):
    f, width = WO.shape
    sp, rows, half_rows = 208, 416, 512
    shard, block = width // 4, width // 16
    dp, ep = lax.axis_index("dp"), lax.axis_index("ep")
    z, x = dp // 2, dp % 2
    y, core = ep // 2, ep % 2
    to_p = {"ep": y * 2 + 1 - core}
    to_o = {"ep": (1 - y) * 2 + core}
    to_x = {"dp": z * 2 + 1 - x}
    zs = [lax.rem(z + k, 4) for k in range(4)]
    to_z = [{"dp": zs[k] * 2 + x} for k in range(4)]
    side = z // 2
    mate, near, far = z + 1 - 2 * (z % 2), 2 - side, 3 - 3 * side
    is_end = z % 2 == side
    is_mid = z % 2 != side
    to_mate, to_near, to_far = ({"dp": other * 2 + x} for other in (mate, near, far))
    friends = (to_p, to_o, to_x, to_z[1], to_z[2], to_z[3])
    g1, b1, g2, b2 = (v[...].reshape(1, width) for v in (g1, b1, g2, b2))

    def rc(name, i, src, dst, dev, arrival=None):
        at = COPIES[name][0] + i
        to = at if arrival is None else COPIES[name][0] + arrival
        return pltpu.make_async_remote_copy(
            src_ref=src, dst_ref=dst, send_sem=ssem.at[at], recv_sem=rsem.at[to], device_id=dev, device_id_type=MESH)

    def lc(i, src, dst):
        return pltpu.make_async_copy(src, dst, lsem.at[i])

    top, sent = pl.ds(0, sp), pl.ds(0, (seq + 7) // 8 * 8)
    barrier = pltpu.get_barrier_semaphore()
    for dev in friends:
        pl.semaphore_signal(barrier, inc=1, device_id=dev, device_id_type=MESH)

    def attention_weights(first):
        cps = [lc(first + n, wqkv.at[:, pl.ds(n * width, width)], WO.at[pl.ds(n * width, width)]) for n in range(3)]
        return cps + [lc(first + 3, wo, WO.at[pl.ds(3 * width, width)])]

    load_x = [lc(i, xb.at[i], GE.at[pl.ds(i * sp, sp)]) for i in range(2)]
    load_w = attention_weights(2)
    load_g = [lc(6 + i, gl.at[i], G.at[0, i, top]) for i in range(2)]
    load_in = lc(8, w_in.at[0], WI)
    for cp in load_x + load_w + load_g + [load_in]:
        cp.start()

    shape = SL.shape[2:]
    before = (sub((LP, LP)) < lane((LP, LP))).astype(BF)
    base = jnp.zeros((shape[0], 1), F32)
    for i in range(2):
        r = jnp.concatenate([routes[i], jnp.full((2, LP - seq), -1, jnp.int32)], axis=1)
        member = (r[0:1, :] == sub(shape)) | (r[1:2, :] == sub(shape))
        member = member & (live[0] > i)
        m = member.astype(F32)
        place = dot(m.astype(BF), before) + base
        SL[0, i] = jnp.where(member, place, -1.0)
        base = base + jnp.sum(m, axis=1, keepdims=True)
    WR[...] = jnp.zeros(WR.shape, BF)
    WR[0:experts, :] = wrt[...]
    for s in range(4):
        for i in range(2):
            first = sent.size if s else sp
            U[s, i, first:, :] = jnp.zeros((LP - first, width), BF)
            G[s, i, first:, :] = jnp.zeros((LP - first, width), BF)

    uP = [rc("uP", i, U.at[0, i, sent], U.at[1, i, sent], to_p) for i in range(2)]
    uO = [rc("uO", i, U.at[0, i, sent], U.at[2, i, sent], to_o) for i in range(2)]
    uF = [rc("uF", i, U.at[2, i, sent], U.at[3, i, sent], to_p) for i in range(2)]
    gP = [rc("gP", i, G.at[0, i, sent], G.at[1, i, sent], to_p) for i in range(2)]
    gO = [rc("gO", i, G.at[0, i, sent], G.at[2, i, sent], to_o) for i in range(2)]
    gF = [rc("gF", i, G.at[2, i, sent], G.at[3, i, sent], to_p) for i in range(2)]
    sP = rc("sP", 0, SL.at[0], SL.at[1], to_p)
    sO = rc("sO", 0, SL.at[0], SL.at[2], to_o)
    sF = rc("sF", 0, SL.at[2], SL.at[3], to_p)

    low = lane((sp, 128)) < HEAD_DIM
    keys = lane((sp, sp)) < seq
    scaling = HEAD_DIM ** -0.5
    with sc("ln1"):
        for i in range(2):
            load_x[i].wait()
            r0 = slice(i * sp, (i + 1) * sp)
            n1, _ = norm_parts(GE[r0, :].astype(F32))
            D[r0, 3 * width:] = (n1 * g1 + b1).astype(BF)
    with sc("barrier"):
        pl.semaphore_wait(barrier, 6)
    sO.start()
    sP.start()
    for i in range(2):
        load_g[i].wait()
        gO[i].start()
        gP[i].start()
    with sc("qkv"):
        for n in range(3):
            load_w[n].wait()
            D[0:rows, n * width:(n + 1) * width] = dot(
                D[0:rows, 3 * width:], WO[n * width:(n + 1) * width, :]).astype(BF)
    LS[...] = jnp.zeros(LS.shape, F32)

    def attend(i, per):
        r0 = slice(i * sp, (i + 1) * sp)

        def pair(step, carry):
            lse = LS[i]
            for inner in range(per):
                h = step * per + inner

                def cols(n):
                    return pl.ds(pl.multiple_of(h * 128 + n * width, 128), 128)

                q, k, v = D[r0, cols(0)], D[r0, cols(1)], D[r0, cols(2)]
                outs = []
                for side in range(2):
                    mine = low if side == 0 else ~low
                    s = dot_nt(jnp.where(mine, q, jnp.zeros_like(q)), k) * scaling
                    s = jnp.where(keys, s, NEG)
                    peak = jnp.max(s, axis=-1, keepdims=True)
                    e = jnp.exp(s - peak)
                    total = jnp.sum(e, axis=-1, keepdims=True)
                    lse = jnp.where(lane((sp, 128)) == 2 * h + side, peak + jnp.log(total), lse)
                    outs.append(dot((e / total).astype(BF), v))
                D[rows + i * sp:rows + (i + 1) * sp, cols(0)] = jnp.where(low, outs[0], outs[1]).astype(BF)
            LS[i] = lse
            return carry

        lax.fori_loop(0, width // 128 // per, pair, 0)

    for i in range(2):
        with sc("attend"):
            attend(i, 2)
        with sc("proj_ln2"):
            if i == 0:
                load_w[3].wait()
            r1 = slice(rows + i * sp, rows + (i + 1) * sp)
            h1 = GE[i * sp:(i + 1) * sp, :].astype(F32) + dot(D[r1, 0:width], WO[3 * width:, :])
            H[i] = h1
            n2, _ = norm_parts(h1)
            U[0, i, :sp, :] = (n2 * g2 + b2).astype(BF)
        uO[i].start()
        uP[i].start()
    keep = [lc(0, D.at[pl.ds(0, rows)], qa_h), lc(1, D.at[pl.ds(rows, rows), pl.ds(0, width)], c_h)]
    keep += [lc(3 + i, U.at[0, i, top], u_h.at[pl.ds(i * sp, sp)]) for i in range(2)]
    load_out = lc(2, w_out.at[0], WO)
    for cp in keep + [load_out]:
        cp.start()

    def onehot(s):
        want = sub((LP, LP)).astype(F32)
        parts = [(want == SL[s, i, pl.ds(ep, 1), :]).astype(BF) for i in range(2)]
        return jnp.concatenate(parts, axis=1)

    def gather(s):
        X[s * LP:(s + 1) * LP, :] = dot(onehot(s), U[s].reshape(2 * LP, width)).astype(BF)

    tile = 512
    tiles = f // tile
    c0 = 0.7978845608028654
    c1 = c0 * 0.044715

    def hidden(rs, cols):
        v = dot(X[rs, :], WI[:, cols])
        w = v * v
        t = jnp.tanh(v * (c0 + c1 * w))
        h = 0.5 + 0.5 * t
        M[rs, cols] = (v * h).astype(BF)
        D[rs, cols] = (h + h * (1.0 - t) * (v * (c0 + 3.0 * c1 * w))).astype(BF)

    def gate(rs):
        r = dot_nt(X[rs, :], WR[...])
        r = jnp.where(lane(r.shape) < experts, r, NEG)
        r = jnp.exp(r - jnp.max(r, axis=-1, keepdims=True))
        r = r / jnp.sum(r, axis=-1, keepdims=True)
        GD[rs, 0:1] = jnp.sum(jnp.where(lane(r.shape) == ep, r, 0.0), axis=-1, keepdims=True)

    first_half, second_half = slice(0, half_rows), slice(half_rows, 2 * half_rows)

    def first_in(n, carry):
        hidden(first_half, pl.ds(pl.multiple_of(n * tile, tile), tile))
        return carry

    def gather_grads(s):
        rs = slice(s * LP, (s + 1) * LP)
        got = dot(onehot(s), G[s].reshape(2 * LP, width))
        GE[rs, :] = got.astype(BF)
        DT[:, rs] = jnp.transpose(GD[rs, 0:1] * got).astype(BF)

    with sc("wait_uP"):
        gather(0)
        sP.wait_recv()
        for i in range(2):
            uP[i].wait_recv()
        gather(1)
        load_in.wait()
        for cp in keep:
            cp.wait()
    with sc("expert_in_0"):
        gate(first_half)
        lax.fori_loop(0, tiles, first_in, 0)
    with sc("wait_gO"):
        sO.wait_recv()
        sF.start()
        for i in range(2):
            gO[i].wait_recv()
            gF[i].start()
        for i in range(2):
            gP[i].wait_recv()
        gather_grads(0)
        gather_grads(1)
    with sc("wait_uO"):
        for i in range(2):
            uO[i].wait_recv()
            uF[i].start()
        gather(2)
    with sc("wait_uF"):
        sF.wait_recv()
        for i in range(2):
            uF[i].wait_recv()
        gather(3)
        gate(second_half)
    with sc("wait_gF"):
        gather_grads(2)
        for i in range(2):
            gF[i].wait_recv()
        gather_grads(3)

    def ox(t):
        return rc("ox", t, GOs.at[t], GOx.at[t], to_x)

    def ix(j):
        return rc("ix", j, GIs.at[j], GIx.at[j], to_x)

    def oq(t):
        return rc("oq", t, GOk.at[t], DT.at[:, pl.ds(t * (width // 2), width // 2)], to_mate)

    oz = rc("oz", 0, GOk.at[2], GOz.at[0], to_mate)
    oc = [rc("oc", t, GOk.at[t], GOz.at[1], dev, 0) for t, dev in enumerate((to_far, to_near))]

    def iq(j, t):
        return rc("iq", j * 2 + t, GIk.at[j, (far, near)[t]], GJ.at[t] if j == 0 else
                  DT.at[pl.ds((j * 2 + t) * (width // 8), width // 8), pl.ds(0, width)], to_mate)

    def jq(t):
        return rc("jq", t, GIs.at[0, (far, near)[t]], GJ.at[2 + t], to_mate)

    jz = rc("jz", 0, GIs.at[0, mate], GIx.at[0, 0], to_mate)

    def jc(t):
        return rc("jc", t, GIs.at[0, (far, near)[t]], GIx.at[0, 1], (to_far, to_near)[t], 0)

    ix0 = rc("ix", 0, GIs.at[0, z], GIx.at[0, 2], to_x)

    def iz(j):
        return rc("iz", j, GIk.at[j, mate], GIz.at[0, j], to_mate)

    def ic(j, t):
        return rc("ic", j * 2 + t, GIk.at[j, (far, near)[t]], GIz.at[1, j], (to_far, to_near)[t], j * 2)

    def w_out_tile(t, carry):
        is0, is3 = (3 - t) // 3, t // 3
        is2 = t // 2 - is3
        zp = is0 * far + (1 - is0 - is2 - is3) * near + is2 * mate + is3 * z
        cols = pl.ds(pl.multiple_of(zp * width, width), width)
        for piece in range(3):
            hidden(second_half, pl.ds(pl.multiple_of(zp * width + piece * 256, 256), 256))
        r = dot(DT[...], M[:, cols])
        lo, hi = r[:, :width // 2], r[:, width // 2:]
        GOs[t] = jnp.where(x == 0, hi, lo).astype(BF)
        GOk[t] = jnp.where(x == 0, lo, hi).astype(BF)
        ox(t).start()
        return carry

    with sc("w_out_tiles"):
        lax.fori_loop(0, 4, w_out_tile, 0)
    pl.semaphore_signal(credit.at[0], inc=1, device_id=to_mate, device_id_type=MESH)

    def take_o(t):
        with sc("take_o%d" % t):
            ox(t).wait_recv()
            GOk[t] = (GOk[t].astype(F32) + GOx[t].astype(F32)).astype(BF)
            if t == 0:
                pl.semaphore_wait(credit.at[0], 1)
            if t < 2:
                @pl.when(is_end)
                def _():
                    oq(t).start()
            if t == 2:
                oz.start()

    def pass_o(t):
        with sc("pass_o%d" % t):
            @pl.when(is_mid)
            def _():
                oq(t).wait_recv()
                GOk[t] = (GOk[t].astype(F32) + DT[:, t * (width // 2):(t + 1) * (width // 2)].astype(F32)).astype(BF)
                oc[t].start()
            if t == 1:
                pl.semaphore_signal(credit.at[1], inc=1, device_id=to_mate, device_id_type=MESH)

    def take_i(j):
        with sc("take_i%d" % j):
            if j > 0:
                ix(j).wait_recv()
                GIk[j] = (GIk[j].astype(F32) + GIx[j].astype(F32)).astype(BF)
            if j == 1:
                pl.semaphore_wait(credit.at[1], 1)

            @pl.when(is_end)
            def _():
                for t in range(1 if j == 3 else 2):
                    iq(j, t).start()
                    if j == 0:
                        jq(t).start()

            if j < 3:
                iz(j).start()
            if j == 0:
                jz.start()

    def pass_i(j, which=(0, 1)):
        with sc("pass_i%d" % j):
            @pl.when(is_mid)
            def _():
                for t in which:
                    at = (far, near)[t]
                    iq(j, t).wait_recv()
                    if j == 0:
                        came = GJ[t]
                    else:
                        r0 = (j * 2 + t) * (width // 8)
                        came = DT[r0:r0 + width // 8, 0:width]
                    GIk[j, at] = (GIk[j, at].astype(F32) + came.astype(F32)).astype(BF)
                    ic(j, t).start()
                    if j == 0:
                        jq(t).wait_recv()
                        GIs[0, at] = (GIs[0, at].astype(F32) + GJ[2 + t].astype(F32)).astype(BF)
                        jc(t).start()

    def cross_first():
        with sc("cross_first"):
            jz.wait_recv()
            rc("jc", 0, GIs.at[0, far], GIx.at[0, 1], to_far, 0).wait_recv()
            total = GIs[0, z].astype(F32) + GIx[0, 0].astype(F32) + GIx[0, 1].astype(F32)
            GIs[0, z] = total.astype(BF)
            ix0.start()

    load_out.wait()
    GD[:, 1:2] = jnp.zeros((GD.shape[0], 1), F32)

    def expert_back(n, carry):
        cols = pl.ds(pl.multiple_of(n * tile, tile), tile)
        for first in (0, half_rows):
            rs = slice(first, first + half_rows)
            back = dot_nt(GE[rs, :], WO[cols, :])
            GD[rs, 1:2] += jnp.sum(back * M[rs, cols].astype(F32), axis=-1, keepdims=True)
            D[rs, cols] = (D[rs, cols].astype(F32) * (GD[rs, 0:1] * back)).astype(BF)
        return carry

    with sc("expert_back"):
        lax.fori_loop(0, tiles // 2, expert_back, 0)
    take_o(0)
    with sc("expert_back"):
        lax.fori_loop(tiles // 2, tiles, expert_back, 0)

    dP = [rc("dP", i, U.at[1, i, top], RP.at[i], to_p) for i in range(2)]
    dD = [rc("dD", i, U.at[3, i, top], RD.at[i], to_p) for i in range(2)]
    dO = [rc("dO", i, U.at[2, i, top], RO.at[i], to_o) for i in range(2)]
    eP = rc("eP", 0, ES.at[1], EP, to_p)
    eD = rc("eD", 0, ES.at[3], ED, to_p)
    eO = rc("eO", 0, ES.at[2], EO, to_o)
    yP = [rc("yP", i, G.at[1, i, top], YP.at[i], to_p) for i in range(2)]
    yD = [rc("yD", i, G.at[3, i, top], YD.at[i], to_p) for i in range(2)]
    yO = [rc("yO", i, G.at[2, i, top], YO.at[i], to_o) for i in range(2)]

    for cp in uP + uO + uF:
        cp.wait_send()

    def scatter(s, values):
        return dot_tn(onehot(s), values)

    def back_rows(step, carry):
        s = 3 - step
        rs = pl.ds(pl.multiple_of(s * LP, LP), LP)
        U[s] = scatter(s, dot_nt(D[rs, :], WI[...]).astype(BF)).astype(BF).reshape(2, LP, width)
        dg = GD[rs, 1:2]
        hi = dg.astype(BF)
        rest = (dg - hi.astype(F32)).astype(BF)
        at = lane((LP, 128))
        zero = jnp.zeros((LP, 128), BF)
        two = jnp.where(at == ep, hi, zero) + jnp.where(at == ep + 64, rest, zero)
        ES[s] = scatter(s, two).astype(BF).reshape(2, LP, 128)

        @pl.when(step == 0)
        def _():
            for cp in dD + [eD]:
                cp.start()

        @pl.when(step == 2)
        def _():
            for cp in dP + [eP]:
                cp.start()

        return carry

    with sc("du"):
        lax.fori_loop(0, 4, back_rows, 0)
    with sc("combine_du"):
        for i in range(2):
            dD[i].wait_recv()
            U[2, i, :sp, :] = (U[2, i, :sp, :].astype(F32) + RD[i].astype(F32)).astype(BF)
            dO[i].start()
        eD.wait_recv()
        ES[2] = ES[2] + ED[...]
        eO.start()
    pass_o(0)
    take_o(1)

    def w_in_tile(j, carry):
        r = dot_tn(X[...], D[:, pl.ds(pl.multiple_of(j * width, width), width)]).reshape(4, 2, width // 8, width)
        first, second = r[:, 0], r[:, 1]
        GIs[j] = jnp.where(x == 0, second, first).astype(BF)
        GIk[j] = jnp.where(x == 0, first, second).astype(BF)

        @pl.when(j > 0)
        def _():
            ix(j).start()

        return carry

    with sc("w_in_tiles"):
        lax.fori_loop(0, 4, w_in_tile, 0)
    take_i(0)
    for dev in friends:
        pl.semaphore_signal(free, inc=1, device_id=dev, device_id_type=MESH)

    for cp in gP + gO + gF:
        cp.wait_send()
    for i in range(2):
        X[half_rows + i * sp:half_rows + (i + 1) * sp, :] = G[0, i, :sp, :]

    def out_rows(step, carry):
        s = 3 - step
        rs = pl.ds(pl.multiple_of(s * LP, LP), LP)
        o = dot(M[rs, :], WO[...]).astype(BF).astype(F32)
        G[s] = scatter(s, (GD[rs, 0:1] * o).astype(BF)).astype(BF).reshape(2, LP, width)

        @pl.when(step == 0)
        def _():
            for cp in yD:
                cp.start()

        @pl.when(step == 2)
        def _():
            for cp in yP:
                cp.start()

        return carry

    with sc("o"):
        lax.fori_loop(0, 4, out_rows, 0)
    pass_o(1)
    late = attention_weights(3) + [
        lc(7, qa_h, M.at[pl.ds(0, rows)]), lc(8, c_h, M.at[pl.ds(rows, rows), pl.ds(0, width)])
    ] + [lc(9 + i, xb.at[i], GE.at[pl.ds(rows + i * sp, sp)]) for i in range(2)]
    late.append(lc(11, u_h, M.at[pl.ds(rows, rows), pl.ds(width, width)]))
    for cp in late:
        cp.start()
    with sc("combine_y"):
        for i in range(2):
            yD[i].wait_recv()
            G[2, i, :sp, :] = (G[2, i, :sp, :].astype(F32) + YD[i].astype(F32)).astype(BF)
            yO[i].start()
    take_o(2)
    for cp in late:
        cp.wait()

    with sc("wait_du"):
        for i in range(2):
            dP[i].wait_recv()
            dO[i].wait_recv()
        eP.wait_recv()
        eO.wait_recv()
    with sc("ln2_back"):
        router = jnp.zeros((width, 128), F32)
        gain2 = jnp.zeros((1, width), F32)
        bias2 = jnp.zeros((1, width), F32)
        for i in range(2):
            du = U[0, i, :sp, :].astype(F32) + RP[i].astype(F32) + RO[i].astype(F32)
            back = ES[0, i, :sp, :].astype(F32) + EP[i, :sp, :].astype(F32) + EO[i, :sp, :].astype(F32)
            back = back + pltpu.roll(back, 64, axis=1)
            own = M[rows + i * sp:rows + (i + 1) * sp, width:2 * width]
            r = dot_nt(own, WR[...])
            r = jnp.where(lane(r.shape) < experts, r, NEG)
            r = jnp.exp(r - jnp.max(r, axis=-1, keepdims=True))
            r = r / jnp.sum(r, axis=-1, keepdims=True)
            dl = (r * (back - jnp.sum(r * back, axis=-1, keepdims=True))).astype(BF)
            router = router + dot_tn(own, dl)
            du = du + dot(dl, WR[...])
            n2, inv2 = norm_parts(H[i])
            gain2 = gain2 + jnp.sum(du * n2, axis=0, keepdims=True)
            bias2 = bias2 + jnp.sum(du, axis=0, keepdims=True)
            on = (live[0] > i).astype(F32)
            dh = X[half_rows + i * sp:half_rows + (i + 1) * sp, :].astype(F32) * on + norm_backward(du * g2, n2, inv2)
            DH[i] = dh
            GE[i * sp:(i + 1) * sp, :] = dh.astype(BF)
        SM[...] = router.astype(BF)

    def part(e, b):
        return pl.ds(pl.multiple_of(e * shard, shard), shard), pl.ds(b * width, width)

    def cp_c(b, i):
        return rc("C", b * 2 + i, WI.at[part(i * 2 + 1 - core, b)], D.at[pl.ds(i * shard, shard), pl.ds(b * width, width)], to_p)

    def cp_y(b):
        return rc("Y", b, WI.at[part((1 - y) * 2 + core, b)], D.at[pl.ds(2 * shard, shard), pl.ds(b * width, width)], to_o)

    def own_rows(k=0, n=shard):
        return pl.ds(pl.multiple_of(ep * shard + k * block, block), n)

    def half(b, h):
        return pl.ds(pl.multiple_of(b * width + h * (width // 2), 128), width // 2)

    def rest(quarter, b, second):
        return D.at[pl.ds(quarter * shard, shard), pl.ds(b * width + second * (width // 2), width // 2)]

    def cp_x(b):
        return rc("X", b, WI.at[own_rows(), half(b, 1 - x)], rest(3, b, 0), to_x)

    def cp_r1(b):
        return rc("R1", b, WI.at[own_rows(), half(b, x)], rest(4, b, 0), to_mate)

    def cp_r2(b):
        return rc("R2", b, WI.at[own_rows(), half(b, x)], rest(4, b, 1), to_near)

    def cp_r3(b):
        return rc("R3", b, rest(0, b, 0), rest(0, b, 0), to_mate)

    def cp_ax(b):
        return rc("AX", b, rest(0, b, 0), rest(1, b, 0), to_x)

    def stage_c(b):
        for i in range(2):
            cp_c(b, i).start()

    def stage_y(b):
        with sc("stage_y%d" % b):
            for i in range(2):
                cp_c(b, i).wait_recv()
            for i in range(2):
                at = part(i * 2 + core, b)
                WI[at] = (WI[at].astype(F32) + D[i * shard:(i + 1) * shard, b * width:(b + 1) * width].astype(F32)).astype(BF)
            cp_y(b).start()

    def stage_x(b):
        with sc("stage_x%d" % b):
            cp_y(b).wait_recv()
            at = part(ep, b)
            WI[at] = (WI[at].astype(F32) + D[2 * shard:3 * shard, b * width:(b + 1) * width].astype(F32)).astype(BF)
            cp_x(b).start()

    def add_own(b, came):
        at = own_rows(), half(b, x)
        WI[at] = (WI[at].astype(F32) + came[...].astype(F32)).astype(BF)

    def stage_r1(b):
        with sc("stage_r1_%d" % b):
            cp_x(b).wait_recv()
            add_own(b, rest(3, b, 0))

            @pl.when(is_end)
            def _():
                cp_r1(b).start()

    def stage_r2(b):
        with sc("stage_r2_%d" % b):
            @pl.when(is_mid)
            def _():
                cp_r1(b).wait_recv()
                add_own(b, rest(4, b, 0))
                cp_r2(b).start()

    def stage_r3(b):
        with sc("stage_r3_%d" % b):
            @pl.when(is_mid)
            def _():
                cp_r2(b).wait_recv()
                total = WI[own_rows(), half(b, x)].astype(F32) + rest(4, b, 1)[...].astype(F32)
                rest(0, b, 0)[...] = total.astype(BF)
                cp_r3(b).start()

            @pl.when(is_end)
            def _():
                cp_r3(b).wait_recv()

            cp_ax(b).start()

    with sc("attn_out_grads"):
        X[half_rows:half_rows + rows, :] = dot_nt(GE[0:rows, :], WO[3 * width:, :]).astype(BF)
        WI[:, 3 * width:] = dot_tn(M[rows:2 * rows, 0:width], GE[0:rows, :]).astype(BF)
    with sc("wait_free"):
        pl.semaphore_wait(free, 6)
    stage_c(3)

    def pair_back(h, carry):
        def cols(n):
            return pl.ds(pl.multiple_of(h * 128 + n * width, 128), 128)

        for i in range(2):
            r0 = slice(i * sp, (i + 1) * sp)
            q, k, v = M[r0, cols(0)], M[r0, cols(1)], M[r0, cols(2)]
            dc = X[half_rows + i * sp:half_rows + (i + 1) * sp, cols(0)]
            parts = []
            for side in range(2):
                here = low if side == 0 else ~low
                zero = jnp.zeros_like(q)
                lse = jnp.sum(jnp.where(lane((sp, 128)) == 2 * h + side, LS[i], 0.0), axis=-1, keepdims=True)
                s = dot_nt(jnp.where(here, q, zero), k) * scaling
                p = jnp.exp(jnp.where(keys, s, NEG) - lse)
                dv = dot_tn(p.astype(BF), dc)
                dp_ = dot_nt(jnp.where(here, dc, zero), v)
                ds = (p * (dp_ - jnp.sum(p * dp_, axis=-1, keepdims=True))).astype(BF)
                parts.append((dot(ds, k) * scaling, dot_tn(ds, q) * scaling, dv))
            r1 = slice(rows + i * sp, rows + (i + 1) * sp)
            for n in range(3):
                M[r1, cols(n + 1)] = jnp.where(low, parts[0][n], parts[1][n]).astype(BF)
        return carry

    with sc("attention_back_a"):
        lax.fori_loop(0, width // 256, pair_back, 0)
    stage_y(3)
    pass_i(0)
    take_o(3)
    with sc("attention_back_b"):
        lax.fori_loop(width // 256, width // 128, pair_back, 0)
    for n in range(3):
        with sc("qkv_grads"):
            grads = M[rows:2 * rows, (n + 1) * width:(n + 2) * width]
            WI[:, n * width:(n + 1) * width] = dot_tn(M[0:rows, 3 * width:], grads).astype(BF)
        stage_c(n)
    stage_x(3)
    take_i(1)
    with sc("ln1_back"):
        gain1 = jnp.zeros((1, width), F32)
        bias1 = jnp.zeros((1, width), F32)
        for i in range(2):
            r1 = slice(rows + i * sp, rows + (i + 1) * sp)
            grad = dot_nt(M[r1, width:2 * width], WO[0:width, :])
            for n in range(1, 3):
                grad = grad + dot_nt(M[r1, (n + 1) * width:(n + 2) * width], WO[n * width:(n + 1) * width, :])
            n1, inv1 = norm_parts(GE[r1, :].astype(F32))
            gain1 = gain1 + jnp.sum(grad * n1, axis=0, keepdims=True)
            bias1 = bias1 + jnp.sum(grad, axis=0, keepdims=True)
            DH[i] = DH[i] + norm_backward(grad * g1, n1, inv1)
        vectors = jnp.concatenate([jnp.zeros((4, width), F32), gain1, bias1, gain2, bias2], axis=0)
        vectors = jnp.concatenate([vectors, jnp.zeros((120, width), F32)], axis=0)
        SM[...] = (SM[...].astype(F32) + jnp.transpose(vectors)).astype(BF)

    def small(e):
        return pl.ds(pl.multiple_of(e * shard, shard), shard)

    mC = [rc("mC", i, SM.at[small(i * 2 + 1 - core)], SMx.at[i], to_p) for i in range(2)]
    mY = rc("mY", 0, SM.at[small((1 - y) * 2 + core)], SMx.at[2], to_o)
    mX = rc("mX", 0, SM.at[small(ep)], SMx.at[3], to_x)
    mZ = [rc("mZ", k - 1, SMx.at[3], SMx.at[3 + k], to_z[k]) for k in range(1, 4)]
    for cp in mC:
        cp.start()
    for b in range(3):
        stage_y(b)
    with sc("small_y"):
        for i in range(2):
            mC[i].wait_recv()
            at = small(i * 2 + core)
            SM[at, :] = (SM[at, :].astype(F32) + SMx[i].astype(F32)).astype(BF)
        mY.start()
    with sc("block_out"):
        for i in range(2):
            yP[i].wait_recv()
            yO[i].wait_recv()
            on = (live[0] > i).astype(F32)
            mix = G[0, i, :sp, :].astype(F32) + YP[i].astype(F32) + YO[i].astype(F32)
            bo_o[i] = ((H[i] + mix) * on).astype(BF)
    cross_first()
    with sc("o_sum"):
        oz.wait_recv()
        rc("oc", 0, GOk.at[0], GOz.at[1], to_far, 0).wait_recv()
        total = GOk[3].astype(F32) + GOz[0].astype(F32) + GOz[1].astype(F32)
        GOk[3] = total.astype(BF)
        outs = [lc(0, GOk.at[3], wo_o)]
        outs[0].start()
    pass_i(1)
    take_i(2)
    stage_x(0)
    pass_i(2)
    stage_x(1)
    take_i(3)
    stage_x(2)
    with sc("small_x"):
        mY.wait_recv()
        at = small(ep)
        SM[at, :] = (SM[at, :].astype(F32) + SMx[2].astype(F32)).astype(BF)
        mX.start()
    stage_r1(3)

    @pl.when(is_end)
    def _():
        iq(3, 1).start()

    pass_i(3, (0,))
    stage_r1(0)
    stage_r2(3)
    pass_i(3, (1,))
    stage_r1(1)
    stage_r2(0)
    stage_r1(2)
    iz(3).start()
    with sc("small_z"):
        mX.wait_recv()
        SMx[3] = (SM[small(ep), :].astype(F32) + SMx[3].astype(F32)).astype(BF)
        for cp in mZ:
            cp.start()
    stage_r2(1)
    stage_r3(3)
    stage_r2(2)
    stage_r3(0)
    stage_r3(1)
    stage_r3(2)
    for j in range(4):
        with sc("i_sum%d" % j):
            iz(j).wait_recv()
            ic(j, 0).wait_recv()
            total = GIk[j, z].astype(F32) + GIz[0, j].astype(F32) + GIz[1, j].astype(F32)
            if j == 0:
                ix0.wait_recv()
                total = total + GIx[0, 2].astype(F32)
            GIx[j, 3] = total.astype(BF)
            outs.append(lc(1 + j, GIx.at[j, 3], wi_o.at[:, pl.ds(j * width, width)]))
            outs[-1].start()
    with sc("small_sum"):
        for cp in mZ:
            cp.wait_recv()
        total = SMx[3].astype(F32) + SMx[4].astype(F32) + SMx[5].astype(F32) + SMx[6].astype(F32)
        sm_o[...] = jnp.transpose(total)[0:8, :]
    for b in (3, 0, 1, 2):
        with sc("wait_ax"):
            cp_ax(b).wait_recv()
            outs.append(lc(5 + b, rest(0, b, 0), sg_o.at[:, half(b, x)]))
            outs[-1].start()
            outs.append(lc(9 + b, rest(1, b, 0), sg_o.at[:, half(b, 1 - x)]))
            outs[-1].start()
    with sc("drain"):
        for cp in dP + dD + dO + yP + yD + yO + [sP, sO, sF, eP, eD, eO, mY, mX] + mC + mZ:
            cp.wait_send()
        for t in range(4):
            ox(t).wait_send()
            (ix(t) if t else ix0).wait_send()
            iz(t).wait_send()
            cp_y(t).wait_send()
            cp_x(t).wait_send()
            cp_ax(t).wait_send()
            for i in range(2):
                cp_c(t, i).wait_send()
        oz.wait_send()
        jz.wait_send()

        @pl.when(is_end)
        def _():
            for t in range(4):
                cp_r1(t).wait_send()
            for t in range(2):
                oq(t).wait_send()
                jq(t).wait_send()
                for j in range(4):
                    iq(j, t).wait_send()

        @pl.when(is_mid)
        def _():
            for t in range(4):
                cp_r2(t).wait_send()
                cp_r3(t).wait_send()
            for t in range(2):
                oc[t].wait_send()
                jc(t).wait_send()
                for j in range(4):
                    ic(j, t).wait_send()

        for cp in outs:
            cp.wait()


def fast_body(n_ep, tokens, live, routes, g1, b1, wqkv, wo, g2, b2, wr, w_in, w_out, cot):
    slots, seq, width = tokens.shape
    sp = (seq + 15) // 16 * 16
    f = w_in.shape[2]
    cap = n_ep * LP
    pads = ((0, 0), (0, sp - seq), (0, 0))
    gl = jnp.pad(cot, pads)
    xb = jnp.pad(tokens, pads)
    sds = jax.ShapeDtypeStruct
    vm = pl.BlockSpec(memory_space=pltpu.VMEM)
    anys = pl.BlockSpec(memory_space=pl.ANY)
    b = lambda *shape: pltpu.VMEM(shape, BF)
    g = lambda *shape: pltpu.VMEM(shape, F32)
    shard = width // n_ep
    bo, gt, sm, wo_t, wi, sg, _, _, _ = pl.pallas_call(
        functools.partial(layer_kernel, n_ep, seq),
        name="layer",
        out_shape=(
            sds((slots, sp, width), BF), sds((slots, sp, width), F32), sds((8, shard), F32),
            sds((width, f // 8), BF), sds((width // 8, f), BF), sds((shard, 4 * width), BF),
            sds((2 * sp, 4 * width), BF), sds((2 * sp, width), BF), sds((2 * sp, width), BF),
        ),
        in_specs=[pl.BlockSpec(memory_space=pltpu.SMEM)] + [vm] * 6 + [anys] * 6,
        out_specs=[vm] * 3 + [anys] * 6,
        scratch_shapes=[
            b(4, 2, LP, width), b(4, 2, LP, width), g(4, 2, 8, LP), b(128, width), b(width, f), b(f, width),
            b(cap, f), b(cap, f), b(cap, width), b(cap, width), b(width, cap),
            b(4, width, f // 8), b(4, width, f // 8), b(4, width, f // 8), b(2, width, f // 8),
            b(4, 4, width // 8, width), b(4, 4, width // 8, width), b(4, 4, width // 8, width),
            b(2, 4, width // 8, width), b(4, width // 8, width),
            g(slots, sp, width), g(slots, sp, 128), g(cap, 2),
            b(2, sp, width), b(2, sp, width), b(2, sp, width),
            b(2, LP, 128), b(2, LP, 128), b(2, LP, 128), b(4, 2, LP, 128),
            b(2, sp, width), b(2, sp, width), b(2, sp, width), b(width, 128), b(7, shard, 128),
            pltpu.SemaphoreType.DMA((N_COPIES,)), pltpu.SemaphoreType.DMA((N_COPIES,)),
            pltpu.SemaphoreType.DMA((14,)), pltpu.SemaphoreType.REGULAR, pltpu.SemaphoreType.REGULAR((2,)),
        ],
        compiler_params=pltpu.CompilerParams(
            collective_id=0, has_side_effects=True, vmem_limit_bytes=67043328),
    )(live, jnp.transpose(routes, (0, 2, 1)), g1, b1, g2, b2, jnp.transpose(wr), xb, gl, w_in, w_out, wqkv, wo)
    return (
        bo[:, :seq], gt[:, :seq], sm[4], sm[5], sg[:, :3 * width].astype(F32), sg[:, 3 * width:].astype(F32),
        sm[6], sm[7], jnp.transpose(sm[:n_ep]), wi.astype(F32)[None], jnp.transpose(wo_t).astype(F32)[None],
    )


def general_body(
    tokens,
    live_images,
    routes,
    ln1_gain,
    ln1_bias,
    query_key_value_weight,
    attention_output_weight,
    ln2_gain,
    ln2_bias,
    w_router,
    w_in,
    w_out,
    cotangent,
):
    slot_count, seq_len, model_width = tokens.shape
    row_count = slot_count * seq_len
    expert_count = w_router.shape[1]
    hidden_width = w_in.shape[2]
    capacity = ((2 * row_count + expert_count - 1) // expert_count * 5 // 4 + 7) // 8 * 8
    scaling = HEAD_DIM ** (-0.5)
    inputs = tokens.astype(jnp.float32).reshape(row_count, model_width)
    normed1, inverse1 = norm_parts(inputs)
    attn_in = (normed1 * ln1_gain + ln1_bias).astype(jnp.bfloat16)
    qkv_rows = jnp.dot(attn_in, query_key_value_weight, preferred_element_type=jnp.float32).astype(
        jnp.bfloat16
    )
    qkv_heads = qkv_rows.reshape(slot_count, seq_len, 3, HEADS, HEAD_DIM)
    queries = qkv_heads[:, :, 0]
    keys_all = qkv_heads[:, :, 1]
    values_all = qkv_heads[:, :, 2]
    scores = (
        jnp.einsum("sqhc,skhc->shqk", queries, keys_all, preferred_element_type=jnp.float32)
        * scaling
    )
    row_peak = jnp.max(scores, axis=-1, keepdims=True)
    raised = jnp.exp(scores - row_peak)
    totals = jnp.sum(raised, axis=-1, keepdims=True)
    log_total = row_peak + jnp.log(totals)
    weights = (raised / totals).astype(jnp.bfloat16)
    attended_context = jnp.einsum(
        "shqk,skhc->sqhc", weights, values_all, preferred_element_type=jnp.float32
    )
    attended_context = attended_context.astype(jnp.bfloat16).reshape(row_count, model_width)
    hidden1 = inputs + jnp.dot(
        attended_context, attention_output_weight, preferred_element_type=jnp.float32
    )
    normed2, inverse2 = norm_parts(hidden1)
    moe_in = (normed2 * ln2_gain + ln2_bias).astype(jnp.bfloat16)
    router = jax.nn.softmax(jnp.dot(moe_in, w_router, preferred_element_type=jnp.float32), axis=-1)
    chosen = routes.reshape(row_count, 2)
    expert_ids = jnp.arange(expert_count, dtype=jnp.int32)
    picked = (chosen[:, :, None] == expert_ids[None, None, :]).astype(jnp.float32)
    gates = jnp.sum(picked * router[:, None, :], axis=-1)
    token_live = (jnp.arange(row_count, dtype=jnp.int32) // seq_len < live_images[0]).astype(
        jnp.float32
    )
    pair_ids = chosen.reshape(2 * row_count)
    pair_live = jnp.repeat(token_live, 2) > 0.5
    member = ((pair_ids[:, None] == expert_ids[None, :]) & pair_live[:, None]).astype(jnp.int32)
    position = jnp.sum((jnp.cumsum(member, axis=0) - 1) * member, axis=-1)
    slot_ids = jnp.where(pair_live, pair_ids * capacity + position, -1).reshape(row_count, 2)
    lanes = jnp.arange(expert_count * capacity, dtype=jnp.int32)
    placing = (jnp.transpose(slot_ids)[:, None, :] == lanes[None, :, None]).astype(jnp.bfloat16)
    outbox = jnp.einsum("jsr,rd->sd", placing, moe_in, preferred_element_type=jnp.float32)
    outbox = outbox.astype(jnp.bfloat16).reshape(expert_count, capacity, model_width)
    inbox = lax.all_to_all(outbox, "ep", split_axis=0, concat_axis=0, tiled=True)
    flat_in = inbox.reshape(-1, model_width)
    pre_act = jnp.dot(flat_in, w_in[0], preferred_element_type=jnp.float32)
    activated = jax.nn.gelu(pre_act).astype(jnp.bfloat16)
    produced = jnp.dot(activated, w_out[0], preferred_element_type=jnp.float32).astype(jnp.bfloat16)
    coming_back = lax.all_to_all(
        produced.reshape(inbox.shape), "ep", split_axis=0, concat_axis=0, tiled=True
    )
    coming_back, pre_act = (
        coming_back,
        pre_act.reshape(inbox.shape[0], inbox.shape[1], hidden_width),
    )
    arrived_rows = inbox.reshape(-1, model_width)
    pre_rows = pre_act.reshape(-1, hidden_width)
    returned_rows = coming_back.reshape(expert_count * capacity, model_width)
    taken = jnp.einsum("jsr,sd->rjd", placing, returned_rows, preferred_element_type=jnp.float32)
    mixture = jnp.sum(gates[:, :, None] * taken, axis=1)
    block_out = (
        ((hidden1 + mixture) * token_live[:, None]).astype(jnp.bfloat16).reshape(tokens.shape)
    )
    upstream = cotangent.astype(jnp.float32).reshape(row_count, model_width) * token_live[:, None]
    gate_grads = jnp.sum(taken * upstream[:, None, :], axis=-1)
    sent_grads = (gates[:, :, None] * upstream[:, None, :]).astype(jnp.bfloat16)
    grad_outbox = jnp.einsum("jsr,rjd->sd", placing, sent_grads, preferred_element_type=jnp.float32)
    grad_outbox = grad_outbox.astype(jnp.bfloat16).reshape(expert_count, capacity, model_width)
    grad_inbox = lax.all_to_all(grad_outbox, "ep", split_axis=0, concat_axis=0, tiled=True)
    grad_rows = grad_inbox.reshape(-1, model_width)
    activated_rows, gelu_pull = jax.vjp(jax.nn.gelu, pre_rows)
    activated_low = activated_rows.astype(jnp.bfloat16)
    grad_activated = jnp.einsum(
        "rd,fd->rf", grad_rows, w_out[0], preferred_element_type=jnp.float32
    )
    grad_pre = gelu_pull(grad_activated)[0].astype(jnp.bfloat16)
    columns = activated_low
    grad_w_out = lax.psum_scatter(
        jnp.einsum("rf,rd->fd", columns, grad_rows, preferred_element_type=jnp.float32).astype(
            jnp.bfloat16
        ),
        "dp",
        scatter_dimension=0,
        tiled=True,
    ).astype(jnp.float32)
    grad_back_rows = jnp.einsum(
        "rf,df->rd", grad_pre, w_in[0], preferred_element_type=jnp.float32
    ).astype(jnp.bfloat16)
    grad_back = lax.all_to_all(
        grad_back_rows.reshape(grad_inbox.shape), "ep", split_axis=0, concat_axis=0, tiled=True
    )
    columns = arrived_rows
    grad_w_in = lax.psum_scatter(
        jnp.einsum("rd,rf->df", columns, grad_pre, preferred_element_type=jnp.float32).astype(
            jnp.bfloat16
        ),
        "dp",
        scatter_dimension=0,
        tiled=True,
    ).astype(jnp.float32)
    grad_back_flat = grad_back.reshape(expert_count * capacity, model_width)
    expert_grad = jnp.einsum(
        "jsr,sd->rd", placing, grad_back_flat, preferred_element_type=jnp.float32
    )
    grad_router_probs = jnp.sum(gate_grads[:, :, None] * picked, axis=1)
    grad_logits = router * (
        grad_router_probs - jnp.sum(router * grad_router_probs, axis=-1, keepdims=True)
    )
    grad_logits = grad_logits.astype(jnp.bfloat16)
    grad_w_router = jnp.einsum("rd,re->de", moe_in, grad_logits, preferred_element_type=jnp.float32)
    grad_moe_in = expert_grad + jnp.einsum(
        "re,de->rd", grad_logits, w_router, preferred_element_type=jnp.float32
    )
    grad_ln2_gain = jnp.sum(grad_moe_in * normed2, axis=0)
    grad_ln2_bias = jnp.sum(grad_moe_in, axis=0)
    grad_hidden1 = upstream + norm_backward(grad_moe_in * ln2_gain, normed2, inverse2)
    grad_attn = grad_hidden1.astype(jnp.bfloat16)
    grad_w_attn_out = jnp.einsum(
        "rd,re->de", attended_context, grad_attn, preferred_element_type=jnp.float32
    )
    grad_context = jnp.einsum(
        "re,de->rd", grad_attn, attention_output_weight, preferred_element_type=jnp.float32
    )
    grad_context = grad_context.astype(jnp.bfloat16).reshape(slot_count, seq_len, HEADS, HEAD_DIM)
    again = (
        jnp.einsum("sqhc,skhc->shqk", queries, keys_all, preferred_element_type=jnp.float32)
        * scaling
    )
    probs_again = jnp.exp(again - log_total)
    probs_low = probs_again.astype(jnp.bfloat16)
    grad_values = jnp.einsum(
        "shqk,sqhc->skhc", probs_low, grad_context, preferred_element_type=jnp.float32
    )
    grad_probs = jnp.einsum(
        "sqhc,skhc->shqk", grad_context, values_all, preferred_element_type=jnp.float32
    )
    grad_scores = probs_again * (
        grad_probs - jnp.sum(probs_again * grad_probs, axis=-1, keepdims=True)
    )
    grad_scores = grad_scores.astype(jnp.bfloat16)
    grad_queries = (
        jnp.einsum("shqk,skhc->sqhc", grad_scores, keys_all, preferred_element_type=jnp.float32)
        * scaling
    )
    grad_keys = (
        jnp.einsum("shqk,sqhc->skhc", grad_scores, queries, preferred_element_type=jnp.float32)
        * scaling
    )
    grad_qkv = (
        jnp.stack([grad_queries, grad_keys, grad_values], axis=2)
        .astype(jnp.bfloat16)
        .reshape(row_count, 3 * model_width)
    )
    grad_w_qkv = jnp.einsum("rd,re->de", attn_in, grad_qkv, preferred_element_type=jnp.float32)
    grad_attn_in = jnp.einsum(
        "re,de->rd", grad_qkv, query_key_value_weight, preferred_element_type=jnp.float32
    )
    grad_ln1_gain = jnp.sum(grad_attn_in * normed1, axis=0)
    grad_ln1_bias = jnp.sum(grad_attn_in, axis=0)
    grad_inputs = grad_hidden1 + norm_backward(grad_attn_in * ln1_gain, normed1, inverse1)
    shared = (
        grad_w_qkv,
        grad_w_attn_out,
        grad_w_router,
        grad_ln1_gain,
        grad_ln1_bias,
        grad_ln2_gain,
        grad_ln2_bias,
    )
    partial_sums = (
        lax.psum_scatter(
            shared[0].astype(jnp.bfloat16), "ep", scatter_dimension=0, tiled=True
        ).astype(jnp.float32),
        lax.psum_scatter(
            shared[1].astype(jnp.bfloat16), "ep", scatter_dimension=0, tiled=True
        ).astype(jnp.float32),
        lax.psum_scatter(
            shared[2].astype(jnp.bfloat16), "ep", scatter_dimension=0, tiled=True
        ).astype(jnp.float32),
        lax.psum_scatter(
            shared[3].astype(jnp.bfloat16), "ep", scatter_dimension=0, tiled=True
        ).astype(jnp.float32),
        lax.psum_scatter(
            shared[4].astype(jnp.bfloat16), "ep", scatter_dimension=0, tiled=True
        ).astype(jnp.float32),
        lax.psum_scatter(
            shared[5].astype(jnp.bfloat16), "ep", scatter_dimension=0, tiled=True
        ).astype(jnp.float32),
        lax.psum_scatter(
            shared[6].astype(jnp.bfloat16), "ep", scatter_dimension=0, tiled=True
        ).astype(jnp.float32),
    )
    shares = (
        lax.psum(partial_sums[0].astype(jnp.bfloat16), "dp").astype(jnp.float32),
        lax.psum(partial_sums[1].astype(jnp.bfloat16), "dp").astype(jnp.float32),
        lax.psum(partial_sums[2].astype(jnp.bfloat16), "dp").astype(jnp.float32),
        lax.psum(partial_sums[3].astype(jnp.bfloat16), "dp").astype(jnp.float32),
        lax.psum(partial_sums[4].astype(jnp.bfloat16), "dp").astype(jnp.float32),
        lax.psum(partial_sums[5].astype(jnp.bfloat16), "dp").astype(jnp.float32),
        lax.psum(partial_sums[6].astype(jnp.bfloat16), "dp").astype(jnp.float32),
    )
    return (
        block_out,
        grad_inputs.reshape(tokens.shape),
        shares[3],
        shares[4],
        shares[0],
        shares[1],
        shares[5],
        shares[6],
        shares[2],
        grad_w_in[None],
        grad_w_out[None],
    )


def solution(mesh):
    in_specs = (
        P(("dp", "ep"), None, None),
        P(("dp", "ep")),
        P(("dp", "ep"), None, None),
        P(),
        P(),
        P(),
        P(),
        P(),
        P(),
        P(),
        P("ep", None, None),
        P("ep", None, None),
        P(("dp", "ep"), None, None),
    )
    out_specs = (
        P(("dp", "ep"), None, None),
        P(("dp", "ep"), None, None),
        P("ep"),
        P("ep"),
        P("ep", None),
        P("ep", None),
        P("ep"),
        P("ep"),
        P("ep", None),
        P("ep", "dp", None),
        P("ep", "dp", None),
    )
    n_dp, n_ep = mesh.shape["dp"], mesh.shape["ep"]
    body = functools.partial(fast_body, n_ep) if (n_dp, n_ep) == (8, 4) else general_body
    return jax.shard_map(body, mesh=mesh, in_specs=in_specs, out_specs=out_specs, check_vma=False)
```

```python
import contextlib
import functools

import jax
import jax.numpy as jnp
from jax import lax
from jax.experimental import pallas as pl
from jax.experimental.pallas import tpu as pltpu
from jax.sharding import PartitionSpec as P

HEADS = 12
HEAD_DIM = 64
MESH = pl.DeviceIdType.MESH
BF = jnp.bfloat16
F32 = jnp.float32
eps = 1e-06
NEG = -1e30
LP = 256


def dot(a, b):
    return jnp.dot(a, b, preferred_element_type=F32)


def dot_nt(a, b):
    return lax.dot_general(a, b, (((1,), (1,)), ((), ())), preferred_element_type=F32)


def dot_tn(a, b):
    return lax.dot_general(a, b, (((0,), (0,)), ((), ())), preferred_element_type=F32)


def lane(shape):
    return lax.broadcasted_iota(jnp.int32, shape, len(shape) - 1)


def sub(shape):
    return lax.broadcasted_iota(jnp.int32, shape, len(shape) - 2)


def norm_parts(v):
    centre = jnp.mean(v, axis=-1, keepdims=True)
    shifted = v - centre
    inverse = lax.rsqrt(jnp.mean(shifted * shifted, axis=-1, keepdims=True) + eps)
    return shifted * inverse, inverse


def norm_backward(y, n, inverse):
    middle = jnp.mean(y, axis=-1, keepdims=True)
    along = jnp.mean(y * n, axis=-1, keepdims=True)
    return (y - middle - n * along) * inverse


def sc(name):
    return contextlib.nullcontext()


COPIES = {}
for _name, _count in (
    ("uP", 2), ("uO", 2), ("uF", 2), ("sP", 1), ("sO", 1), ("sF", 1), ("gP", 2), ("gO", 2), ("gF", 2),
    ("ox", 4), ("oq", 2), ("oz", 1), ("oc", 2), ("ix", 4), ("iq", 8), ("iz", 4), ("ic", 8), ("jq", 2), ("jz", 1), ("jc", 2),
    ("dP", 2), ("dD", 2), ("dO", 2), ("eP", 1), ("eD", 1), ("eO", 1), ("yP", 2), ("yD", 2), ("yO", 2),
    ("C", 8), ("Y", 4), ("X", 4), ("R1", 4), ("R2", 4), ("R3", 4), ("AX", 4), ("mC", 2), ("mY", 1), ("mX", 1), ("mZ", 3),
):
    COPIES[_name] = sum(n for _, n in COPIES.values()), _count
N_COPIES = sum(n for _, n in COPIES.values())


def layer_kernel(
    experts, seq, live, routes, g1, b1, g2, b2, wrt, xb, gl, w_in, w_out, wqkv, wo,
    bo_o, gt_o, sm_o, wo_o, wi_o, sg_o, qa_h, c_h, u_h,
    U, G, SL, WR, WI, WO, M, D, X, GE, DT,
    GOs, GOk, GOx, GOz, GIs, GIk, GIx, GIz, GJ,
    H, DH, LS, GD, RP, RD, RO, EP, ED, EO, ES, YP, YD, YO, SM, SMx, SZ,
    ssem, rsem, lsem, free, credit,
):
    f, width = WO.shape
    sp, rows, half_rows = 208, 416, 512
    shard, block = width // 4, width // 16
    dp, ep = lax.axis_index("dp"), lax.axis_index("ep")
    z, x = dp // 2, dp % 2
    y, core = ep // 2, ep % 2
    to_p = {"ep": y * 2 + 1 - core}
    to_o = {"ep": (1 - y) * 2 + core}
    to_x = {"dp": z * 2 + 1 - x}
    zs = [lax.rem(z + k, 4) for k in range(4)]
    to_z = [{"dp": zs[k] * 2 + x} for k in range(4)]
    side = z // 2
    mate, near, far = z + 1 - 2 * (z % 2), 2 - side, 3 - 3 * side
    is_end = z % 2 == side
    is_mid = z % 2 != side
    to_mate, to_near, to_far = ({"dp": other * 2 + x} for other in (mate, near, far))
    friends = (to_p, to_o, to_x, to_z[1], to_z[2], to_z[3])
    g1, b1, g2, b2 = (v[...].reshape(1, width) for v in (g1, b1, g2, b2))

    def rc(name, i, src, dst, dev, arrival=None):
        at = COPIES[name][0] + i
        to = at if arrival is None else COPIES[name][0] + arrival
        return pltpu.make_async_remote_copy(
            src_ref=src, dst_ref=dst, send_sem=ssem.at[at], recv_sem=rsem.at[to], device_id=dev, device_id_type=MESH)

    def lc(i, src, dst):
        return pltpu.make_async_copy(src, dst, lsem.at[i])

    top, sent = pl.ds(0, sp), pl.ds(0, (seq + 7) // 8 * 8)
    barrier = pltpu.get_barrier_semaphore()
    for dev in friends:
        pl.semaphore_signal(barrier, inc=1, device_id=dev, device_id_type=MESH)

    def attention_weights(first):
        cps = [lc(first + n, wqkv.at[:, pl.ds(n * width, width)], WO.at[pl.ds(n * width, width)]) for n in range(3)]
        return cps + [lc(first + 3, wo, WO.at[pl.ds(3 * width, width)])]

    load_x = [lc(i, xb.at[i], GE.at[pl.ds(i * sp, sp)]) for i in range(2)]
    load_w = attention_weights(2)
    load_g = [lc(6 + i, gl.at[i], G.at[0, i, top]) for i in range(2)]
    load_in = lc(8, w_in.at[0], WI)
    for cp in load_x + load_w + load_g + [load_in]:
        cp.start()

    shape = SL.shape[2:]
    before = (sub((LP, LP)) < lane((LP, LP))).astype(BF)
    base = jnp.zeros((shape[0], 1), F32)
    for i in range(2):
        r = jnp.concatenate([routes[i], jnp.full((2, LP - seq), -1, jnp.int32)], axis=1)
        member = (r[0:1, :] == sub(shape)) | (r[1:2, :] == sub(shape))
        member = member & (live[0] > i)
        m = member.astype(F32)
        place = dot(m.astype(BF), before) + base
        SL[0, i] = jnp.where(member, place, -1.0)
        base = base + jnp.sum(m, axis=1, keepdims=True)
    WR[...] = jnp.zeros(WR.shape, BF)
    WR[0:experts, :] = wrt[...]
    for s in range(4):
        for i in range(2):
            first = sent.size if s else sp
            U[s, i, first:, :] = jnp.zeros((LP - first, width), BF)
            G[s, i, first:, :] = jnp.zeros((LP - first, width), BF)

    uP = [rc("uP", i, U.at[0, i, sent], U.at[1, i, sent], to_p) for i in range(2)]
    uO = [rc("uO", i, U.at[0, i, sent], U.at[2, i, sent], to_o) for i in range(2)]
    uF = [rc("uF", i, U.at[2, i, sent], U.at[3, i, sent], to_p) for i in range(2)]
    gP = [rc("gP", i, G.at[0, i, sent], G.at[1, i, sent], to_p) for i in range(2)]
    gO = [rc("gO", i, G.at[0, i, sent], G.at[2, i, sent], to_o) for i in range(2)]
    gF = [rc("gF", i, G.at[2, i, sent], G.at[3, i, sent], to_p) for i in range(2)]
    sP = rc("sP", 0, SL.at[0], SL.at[1], to_p)
    sO = rc("sO", 0, SL.at[0], SL.at[2], to_o)
    sF = rc("sF", 0, SL.at[2], SL.at[3], to_p)

    low = lane((sp, 128)) < HEAD_DIM
    keys = lane((sp, sp)) < seq
    scaling = HEAD_DIM ** -0.5
    with sc("ln1"):
        for i in range(2):
            load_x[i].wait()
            r0 = slice(i * sp, (i + 1) * sp)
            n1, _ = norm_parts(GE[r0, :].astype(F32))
            D[r0, 3 * width:] = (n1 * g1 + b1).astype(BF)
    with sc("barrier"):
        pl.semaphore_wait(barrier, 6)
    sO.start()
    sP.start()
    for i in range(2):
        load_g[i].wait()
        gO[i].start()
        gP[i].start()
    with sc("qkv"):
        for n in range(3):
            load_w[n].wait()
            D[0:rows, n * width:(n + 1) * width] = dot(
                D[0:rows, 3 * width:], WO[n * width:(n + 1) * width, :]).astype(BF)
    LS[...] = jnp.zeros(LS.shape, F32)

    def attend(i, per):
        r0 = slice(i * sp, (i + 1) * sp)

        def pair(step, carry):
            lse = LS[i]
            for inner in range(per):
                h = step * per + inner

                def cols(n):
                    return pl.ds(pl.multiple_of(h * 128 + n * width, 128), 128)

                q, k, v = D[r0, cols(0)], D[r0, cols(1)], D[r0, cols(2)]
                outs = []
                for side in range(2):
                    mine = low if side == 0 else ~low
                    s = dot_nt(jnp.where(mine, q, jnp.zeros_like(q)), k) * scaling
                    s = jnp.where(keys, s, NEG)
                    peak = jnp.max(s, axis=-1, keepdims=True)
                    e = jnp.exp(s - peak)
                    total = jnp.sum(e, axis=-1, keepdims=True)
                    lse = jnp.where(lane((sp, 128)) == 2 * h + side, peak + jnp.log(total), lse)
                    outs.append(dot((e / total).astype(BF), v))
                D[rows + i * sp:rows + (i + 1) * sp, cols(0)] = jnp.where(low, outs[0], outs[1]).astype(BF)
            LS[i] = lse
            return carry

        lax.fori_loop(0, width // 128 // per, pair, 0)

    for i in range(2):
        with sc("attend"):
            attend(i, 2)
        with sc("proj_ln2"):
            if i == 0:
                load_w[3].wait()
            r1 = slice(rows + i * sp, rows + (i + 1) * sp)
            h1 = GE[i * sp:(i + 1) * sp, :].astype(F32) + dot(D[r1, 0:width], WO[3 * width:, :])
            H[i] = h1
            n2, _ = norm_parts(h1)
            U[0, i, :sp, :] = (n2 * g2 + b2).astype(BF)
        uO[i].start()
        uP[i].start()
    keep = [lc(0, D.at[pl.ds(0, rows)], qa_h), lc(1, D.at[pl.ds(rows, rows), pl.ds(0, width)], c_h)]
    keep += [lc(3 + i, U.at[0, i, top], u_h.at[pl.ds(i * sp, sp)]) for i in range(2)]
    load_out = lc(2, w_out.at[0], WO)
    for cp in keep + [load_out]:
        cp.start()

    def onehot(s):
        want = sub((LP, LP)).astype(F32)
        parts = [(want == SL[s, i, pl.ds(ep, 1), :]).astype(BF) for i in range(2)]
        return jnp.concatenate(parts, axis=1)

    def gather(s):
        X[s * LP:(s + 1) * LP, :] = dot(onehot(s), U[s].reshape(2 * LP, width)).astype(BF)

    tile = 512
    tiles = f // tile
    c0 = 0.7978845608028654
    c1 = c0 * 0.044715

    def hidden(rs, cols):
        v = dot(X[rs, :], WI[:, cols])
        w = v * v
        t = jnp.tanh(v * (c0 + c1 * w))
        h = 0.5 + 0.5 * t
        M[rs, cols] = (v * h).astype(BF)
        D[rs, cols] = (h + h * (1.0 - t) * (v * (c0 + 3.0 * c1 * w))).astype(BF)

    def gate(rs):
        r = dot_nt(X[rs, :], WR[...])
        r = jnp.where(lane(r.shape) < experts, r, NEG)
        r = jnp.exp(r - jnp.max(r, axis=-1, keepdims=True))
        r = r / jnp.sum(r, axis=-1, keepdims=True)
        GD[rs, 0:1] = jnp.sum(jnp.where(lane(r.shape) == ep, r, 0.0), axis=-1, keepdims=True)

    first_half, second_half = slice(0, half_rows), slice(half_rows, 2 * half_rows)

    def first_in(n, carry):
        hidden(first_half, pl.ds(pl.multiple_of(n * tile, tile), tile))
        return carry

    def gather_grads(s):
        rs = slice(s * LP, (s + 1) * LP)
        got = dot(onehot(s), G[s].reshape(2 * LP, width))
        GE[rs, :] = got.astype(BF)
        DT[:, rs] = jnp.transpose(GD[rs, 0:1] * got).astype(BF)

    with sc("wait_uP"):
        gather(0)
        sP.wait_recv()
        for i in range(2):
            uP[i].wait_recv()
        gather(1)
        load_in.wait()
        for cp in keep:
            cp.wait()
    with sc("expert_in_0"):
        gate(first_half)
        lax.fori_loop(0, tiles, first_in, 0)
    with sc("wait_gO"):
        sO.wait_recv()
        sF.start()
        for i in range(2):
            gO[i].wait_recv()
            gF[i].start()
        for i in range(2):
            gP[i].wait_recv()
        gather_grads(0)
        gather_grads(1)
    with sc("wait_uO"):
        for i in range(2):
            uO[i].wait_recv()
            uF[i].start()
        gather(2)
    with sc("wait_uF"):
        sF.wait_recv()
        for i in range(2):
            uF[i].wait_recv()
        gather(3)
        gate(second_half)
    with sc("wait_gF"):
        gather_grads(2)
        for i in range(2):
            gF[i].wait_recv()
        gather_grads(3)

    def ox(t):
        return rc("ox", t, GOs.at[t], GOx.at[t], to_x)

    def ix(j):
        return rc("ix", j, GIs.at[j], GIx.at[j], to_x)

    def oq(t):
        return rc("oq", t, GOk.at[t], DT.at[:, pl.ds(t * (width // 2), width // 2)], to_mate)

    oz = rc("oz", 0, GOk.at[2], GOz.at[0], to_mate)
    oc = [rc("oc", t, GOk.at[t], GOz.at[1], dev, 0) for t, dev in enumerate((to_far, to_near))]

    def iq(j, t):
        return rc("iq", j * 2 + t, GIk.at[j, (far, near)[t]], GJ.at[t] if j == 0 else
                  DT.at[pl.ds((j * 2 + t) * (width // 8), width // 8), pl.ds(0, width)], to_mate)

    def jq(t):
        return rc("jq", t, GIs.at[0, (far, near)[t]], GJ.at[2 + t], to_mate)

    jz = rc("jz", 0, GIs.at[0, mate], GIx.at[0, 0], to_mate)

    def jc(t):
        return rc("jc", t, GIs.at[0, (far, near)[t]], GIx.at[0, 1], (to_far, to_near)[t], 0)

    ix0 = rc("ix", 0, GIs.at[0, z], GIx.at[0, 2], to_x)

    def iz(j):
        return rc("iz", j, GIk.at[j, mate], GIz.at[0, j], to_mate)

    def ic(j, t):
        return rc("ic", j * 2 + t, GIk.at[j, (far, near)[t]], GIz.at[1, j], (to_far, to_near)[t], j * 2)

    def w_out_tile(t, carry):
        is0, is3 = (3 - t) // 3, t // 3
        is2 = t // 2 - is3
        zp = is0 * far + (1 - is0 - is2 - is3) * near + is2 * mate + is3 * z
        cols = pl.ds(pl.multiple_of(zp * width, width), width)
        for piece in range(3):
            hidden(second_half, pl.ds(pl.multiple_of(zp * width + piece * 256, 256), 256))
        r = dot(DT[...], M[:, cols])
        lo, hi = r[:, :width // 2], r[:, width // 2:]
        GOs[t] = jnp.where(x == 0, hi, lo).astype(BF)
        GOk[t] = jnp.where(x == 0, lo, hi).astype(BF)
        ox(t).start()
        return carry

    with sc("w_out_tiles"):
        lax.fori_loop(0, 4, w_out_tile, 0)
    pl.semaphore_signal(credit.at[0], inc=1, device_id=to_mate, device_id_type=MESH)

    def take_o(t):
        with sc("take_o%d" % t):
            ox(t).wait_recv()
            GOk[t] = (GOk[t].astype(F32) + GOx[t].astype(F32)).astype(BF)
            if t == 0:
                pl.semaphore_wait(credit.at[0], 1)
            if t < 2:
                @pl.when(is_end)
                def _():
                    oq(t).start()
            if t == 2:
                oz.start()

    def pass_o(t):
        with sc("pass_o%d" % t):
            @pl.when(is_mid)
            def _():
                oq(t).wait_recv()
                GOk[t] = (GOk[t].astype(F32) + DT[:, t * (width // 2):(t + 1) * (width // 2)].astype(F32)).astype(BF)
                oc[t].start()
            if t == 1:
                pl.semaphore_signal(credit.at[1], inc=1, device_id=to_mate, device_id_type=MESH)

    def take_i(j):
        with sc("take_i%d" % j):
            if j > 0:
                ix(j).wait_recv()
                GIk[j] = (GIk[j].astype(F32) + GIx[j].astype(F32)).astype(BF)
            if j == 1:
                pl.semaphore_wait(credit.at[1], 1)

            @pl.when(is_end)
            def _():
                for t in range(1 if j == 3 else 2):
                    iq(j, t).start()
                    if j == 0:
                        jq(t).start()

            if j < 3:
                iz(j).start()
            if j == 0:
                jz.start()

    def pass_i(j, which=(0, 1)):
        with sc("pass_i%d" % j):
            @pl.when(is_mid)
            def _():
                for t in which:
                    at = (far, near)[t]
                    iq(j, t).wait_recv()
                    if j == 0:
                        came = GJ[t]
                    else:
                        r0 = (j * 2 + t) * (width // 8)
                        came = DT[r0:r0 + width // 8, 0:width]
                    GIk[j, at] = (GIk[j, at].astype(F32) + came.astype(F32)).astype(BF)
                    ic(j, t).start()
                    if j == 0:
                        jq(t).wait_recv()
                        GIs[0, at] = (GIs[0, at].astype(F32) + GJ[2 + t].astype(F32)).astype(BF)
                        jc(t).start()

    def cross_first():
        with sc("cross_first"):
            jz.wait_recv()
            rc("jc", 0, GIs.at[0, far], GIx.at[0, 1], to_far, 0).wait_recv()
            total = GIs[0, z].astype(F32) + GIx[0, 0].astype(F32) + GIx[0, 1].astype(F32)
            GIs[0, z] = total.astype(BF)
            ix0.start()

    load_out.wait()
    GD[:, 1:2] = jnp.zeros((GD.shape[0], 1), F32)

    def expert_back(n, carry):
        @pl.when(n == tiles // 2)
        def _():
            take_o(0)

        cols = pl.ds(pl.multiple_of(n * tile, tile), tile)
        for first in (0, half_rows):
            rs = slice(first, first + half_rows)
            back = dot_nt(GE[rs, :], WO[cols, :])
            GD[rs, 1:2] += jnp.sum(back * M[rs, cols].astype(F32), axis=-1, keepdims=True)
            D[rs, cols] = (D[rs, cols].astype(F32) * (GD[rs, 0:1] * back)).astype(BF)
        return carry

    with sc("expert_back"):
        lax.fori_loop(0, tiles, expert_back, 0)

    dP = [rc("dP", i, U.at[1, i, top], RP.at[i], to_p) for i in range(2)]
    dD = [rc("dD", i, U.at[3, i, top], RD.at[i], to_p) for i in range(2)]
    dO = [rc("dO", i, U.at[2, i, top], RO.at[i], to_o) for i in range(2)]
    eP = rc("eP", 0, ES.at[1], EP, to_p)
    eD = rc("eD", 0, ES.at[3], ED, to_p)
    eO = rc("eO", 0, ES.at[2], EO, to_o)
    yP = [rc("yP", i, G.at[1, i, top], YP.at[i], to_p) for i in range(2)]
    yD = [rc("yD", i, G.at[3, i, top], YD.at[i], to_p) for i in range(2)]
    yO = [rc("yO", i, G.at[2, i, top], YO.at[i], to_o) for i in range(2)]

    for cp in uP + uO + uF:
        cp.wait_send()

    def scatter(s, values):
        return dot_tn(onehot(s), values)

    def back_rows(step, carry):
        s = 3 - step
        rs = pl.ds(pl.multiple_of(s * LP, LP), LP)
        U[s] = scatter(s, dot_nt(D[rs, :], WI[...]).astype(BF)).astype(BF).reshape(2, LP, width)
        dg = GD[rs, 1:2]
        hi = dg.astype(BF)
        rest = (dg - hi.astype(F32)).astype(BF)
        at = lane((LP, 128))
        zero = jnp.zeros((LP, 128), BF)
        two = jnp.where(at == ep, hi, zero) + jnp.where(at == ep + 64, rest, zero)
        ES[s] = scatter(s, two).astype(BF).reshape(2, LP, 128)

        @pl.when(step == 0)
        def _():
            for cp in dD + [eD]:
                cp.start()

        @pl.when(step == 2)
        def _():
            for cp in dP + [eP]:
                cp.start()

        return carry

    with sc("du"):
        lax.fori_loop(0, 4, back_rows, 0)
    with sc("combine_du"):
        for i in range(2):
            dD[i].wait_recv()
            U[2, i, :sp, :] = (U[2, i, :sp, :].astype(F32) + RD[i].astype(F32)).astype(BF)
            dO[i].start()
        eD.wait_recv()
        ES[2] = ES[2] + ED[...]
        eO.start()
    pass_o(0)
    take_o(1)

    def w_in_tile(j, carry):
        r = dot_tn(X[...], D[:, pl.ds(pl.multiple_of(j * width, width), width)]).reshape(4, 2, width // 8, width)
        first, second = r[:, 0], r[:, 1]
        GIs[j] = jnp.where(x == 0, second, first).astype(BF)
        GIk[j] = jnp.where(x == 0, first, second).astype(BF)

        @pl.when(j > 0)
        def _():
            ix(j).start()

        return carry

    with sc("w_in_tiles"):
        lax.fori_loop(0, 4, w_in_tile, 0)
    take_i(0)
    for dev in friends:
        pl.semaphore_signal(free, inc=1, device_id=dev, device_id_type=MESH)

    for cp in gP + gO + gF:
        cp.wait_send()
    for i in range(2):
        X[half_rows + i * sp:half_rows + (i + 1) * sp, :] = G[0, i, :sp, :]

    def out_rows(step, carry):
        s = 3 - step
        rs = pl.ds(pl.multiple_of(s * LP, LP), LP)
        o = dot(M[rs, :], WO[...]).astype(BF).astype(F32)
        G[s] = scatter(s, (GD[rs, 0:1] * o).astype(BF)).astype(BF).reshape(2, LP, width)

        @pl.when(step == 0)
        def _():
            for cp in yD:
                cp.start()

        @pl.when(step == 2)
        def _():
            for cp in yP:
                cp.start()

        return carry

    with sc("o"):
        lax.fori_loop(0, 4, out_rows, 0)
    pass_o(1)
    late = attention_weights(3) + [
        lc(7, qa_h, M.at[pl.ds(0, rows)]), lc(8, c_h, M.at[pl.ds(rows, rows), pl.ds(0, width)])
    ] + [lc(9 + i, xb.at[i], GE.at[pl.ds(rows + i * sp, sp)]) for i in range(2)]
    late.append(lc(11, u_h, M.at[pl.ds(rows, rows), pl.ds(width, width)]))
    for cp in late:
        cp.start()
    with sc("combine_y"):
        for i in range(2):
            yD[i].wait_recv()
            G[2, i, :sp, :] = (G[2, i, :sp, :].astype(F32) + YD[i].astype(F32)).astype(BF)
            yO[i].start()
    take_o(2)
    for cp in late:
        cp.wait()

    with sc("wait_du"):
        for i in range(2):
            dP[i].wait_recv()
            dO[i].wait_recv()
        eP.wait_recv()
        eO.wait_recv()
    with sc("ln2_back"):
        router = jnp.zeros((width, 128), F32)
        gain2 = jnp.zeros((1, width), F32)
        bias2 = jnp.zeros((1, width), F32)
        for i in range(2):
            du = U[0, i, :sp, :].astype(F32) + RP[i].astype(F32) + RO[i].astype(F32)
            back = ES[0, i, :sp, :].astype(F32) + EP[i, :sp, :].astype(F32) + EO[i, :sp, :].astype(F32)
            back = back + pltpu.roll(back, 64, axis=1)
            own = M[rows + i * sp:rows + (i + 1) * sp, width:2 * width]
            r = dot_nt(own, WR[...])
            r = jnp.where(lane(r.shape) < experts, r, NEG)
            r = jnp.exp(r - jnp.max(r, axis=-1, keepdims=True))
            r = r / jnp.sum(r, axis=-1, keepdims=True)
            dl = (r * (back - jnp.sum(r * back, axis=-1, keepdims=True))).astype(BF)
            router = router + dot_tn(own, dl)
            du = du + dot(dl, WR[...])
            n2, inv2 = norm_parts(H[i])
            gain2 = gain2 + jnp.sum(du * n2, axis=0, keepdims=True)
            bias2 = bias2 + jnp.sum(du, axis=0, keepdims=True)
            on = (live[0] > i).astype(F32)
            dh = X[half_rows + i * sp:half_rows + (i + 1) * sp, :].astype(F32) * on + norm_backward(du * g2, n2, inv2)
            DH[i] = dh
            GE[i * sp:(i + 1) * sp, :] = dh.astype(BF)
        SM[...] = router.astype(BF)

    def part(e, b):
        return pl.ds(pl.multiple_of(e * shard, shard), shard), pl.ds(b * width, width)

    def cp_c(b, i):
        return rc("C", b * 2 + i, WI.at[part(i * 2 + 1 - core, b)], D.at[pl.ds(i * shard, shard), pl.ds(b * width, width)], to_p)

    def cp_y(b):
        return rc("Y", b, WI.at[part((1 - y) * 2 + core, b)], D.at[pl.ds(2 * shard, shard), pl.ds(b * width, width)], to_o)

    def own_rows(k=0, n=shard):
        return pl.ds(pl.multiple_of(ep * shard + k * block, block), n)

    def half(b, h):
        return pl.ds(pl.multiple_of(b * width + h * (width // 2), 128), width // 2)

    def rest(quarter, b, second):
        return D.at[pl.ds(quarter * shard, shard), pl.ds(b * width + second * (width // 2), width // 2)]

    def cp_x(b):
        return rc("X", b, WI.at[own_rows(), half(b, 1 - x)], rest(3, b, 0), to_x)

    def cp_r1(b):
        return rc("R1", b, WI.at[own_rows(), half(b, x)], rest(4, b, 0), to_mate)

    def cp_r2(b):
        return rc("R2", b, WI.at[own_rows(), half(b, x)], rest(4, b, 1), to_near)

    def cp_r3(b):
        return rc("R3", b, rest(0, b, 0), rest(0, b, 0), to_mate)

    def cp_ax(b):
        return rc("AX", b, rest(0, b, 0), rest(1, b, 0), to_x)

    def stage_c(b):
        for i in range(2):
            cp_c(b, i).start()

    def stage_y(b):
        with sc("stage_y%d" % b):
            for i in range(2):
                cp_c(b, i).wait_recv()
            for i in range(2):
                at = part(i * 2 + core, b)
                WI[at] = (WI[at].astype(F32) + D[i * shard:(i + 1) * shard, b * width:(b + 1) * width].astype(F32)).astype(BF)
            cp_y(b).start()

    def stage_x(b):
        with sc("stage_x%d" % b):
            cp_y(b).wait_recv()
            at = part(ep, b)
            WI[at] = (WI[at].astype(F32) + D[2 * shard:3 * shard, b * width:(b + 1) * width].astype(F32)).astype(BF)
            cp_x(b).start()

    def add_own(b, came):
        at = own_rows(), half(b, x)
        WI[at] = (WI[at].astype(F32) + came[...].astype(F32)).astype(BF)

    def stage_r1(b):
        with sc("stage_r1_%d" % b):
            cp_x(b).wait_recv()
            add_own(b, rest(3, b, 0))

            @pl.when(is_end)
            def _():
                cp_r1(b).start()

    def stage_r2(b):
        with sc("stage_r2_%d" % b):
            @pl.when(is_mid)
            def _():
                cp_r1(b).wait_recv()
                add_own(b, rest(4, b, 0))
                cp_r2(b).start()

    def stage_r3(b):
        with sc("stage_r3_%d" % b):
            @pl.when(is_mid)
            def _():
                cp_r2(b).wait_recv()
                total = WI[own_rows(), half(b, x)].astype(F32) + rest(4, b, 1)[...].astype(F32)
                rest(0, b, 0)[...] = total.astype(BF)
                cp_r3(b).start()
                cp_ax(b).start()

    def stage_r4(b):
        with sc("stage_r4_%d" % b):
            @pl.when(is_end)
            def _():
                cp_r3(b).wait_recv()
                cp_ax(b).start()

    with sc("attn_out_grads"):
        X[half_rows:half_rows + rows, :] = dot_nt(GE[0:rows, :], WO[3 * width:, :]).astype(BF)
        WI[:, 3 * width:] = dot_tn(M[rows:2 * rows, 0:width], GE[0:rows, :]).astype(BF)
    with sc("wait_free"):
        pl.semaphore_wait(free, 6)
    stage_c(3)

    def pair_back(h, carry):
        @pl.when(h == width // 256)
        def _():
            stage_y(3)
            pass_i(0)
            take_o(3)

        def cols(n):
            return pl.ds(pl.multiple_of(h * 128 + n * width, 128), 128)

        for i in range(2):
            r0 = slice(i * sp, (i + 1) * sp)
            q, k, v = M[r0, cols(0)], M[r0, cols(1)], M[r0, cols(2)]
            dc = X[half_rows + i * sp:half_rows + (i + 1) * sp, cols(0)]
            parts = []
            for side in range(2):
                here = low if side == 0 else ~low
                zero = jnp.zeros_like(q)
                lse = jnp.sum(jnp.where(lane((sp, 128)) == 2 * h + side, LS[i], 0.0), axis=-1, keepdims=True)
                s = dot_nt(jnp.where(here, q, zero), k) * scaling
                p = jnp.exp(jnp.where(keys, s, NEG) - lse)
                dv = dot_tn(p.astype(BF), dc)
                dp_ = dot_nt(jnp.where(here, dc, zero), v)
                ds = (p * (dp_ - jnp.sum(p * dp_, axis=-1, keepdims=True))).astype(BF)
                parts.append((dot(ds, k) * scaling, dot_tn(ds, q) * scaling, dv))
            r1 = slice(rows + i * sp, rows + (i + 1) * sp)
            for n in range(3):
                M[r1, cols(n + 1)] = jnp.where(low, parts[0][n], parts[1][n]).astype(BF)
        return carry

    with sc("attention_back"):
        lax.fori_loop(0, width // 128, pair_back, 0)
    for n in range(3):
        with sc("qkv_grads"):
            grads = M[rows:2 * rows, (n + 1) * width:(n + 2) * width]
            WI[:, n * width:(n + 1) * width] = dot_tn(M[0:rows, 3 * width:], grads).astype(BF)
        stage_c(n)
    stage_x(3)
    take_i(1)
    with sc("ln1_back"):
        gain1 = jnp.zeros((1, width), F32)
        bias1 = jnp.zeros((1, width), F32)
        for i in range(2):
            r1 = slice(rows + i * sp, rows + (i + 1) * sp)
            grad = dot_nt(M[r1, width:2 * width], WO[0:width, :])
            for n in range(1, 3):
                grad = grad + dot_nt(M[r1, (n + 1) * width:(n + 2) * width], WO[n * width:(n + 1) * width, :])
            n1, inv1 = norm_parts(GE[r1, :].astype(F32))
            gain1 = gain1 + jnp.sum(grad * n1, axis=0, keepdims=True)
            bias1 = bias1 + jnp.sum(grad, axis=0, keepdims=True)
            DH[i] = DH[i] + norm_backward(grad * g1, n1, inv1)
        vectors = jnp.concatenate([jnp.zeros((4, width), F32), gain1, bias1, gain2, bias2], axis=0)
        vectors = jnp.concatenate([vectors, jnp.zeros((120, width), F32)], axis=0)
        SM[...] = (SM[...].astype(F32) + jnp.transpose(vectors)).astype(BF)

    def small(e):
        return pl.ds(pl.multiple_of(e * shard, shard), shard)

    mC = [rc("mC", i, SM.at[small(i * 2 + 1 - core)], SMx.at[i], to_p) for i in range(2)]
    mY = rc("mY", 0, SM.at[small((1 - y) * 2 + core)], SMx.at[2], to_o)
    mX = rc("mX", 0, SM.at[small(ep)], SMx.at[3], to_x)
    mZ = [rc("mZ", k - 1, SZ.at[0], SZ.at[k], to_z[k]) for k in range(1, 4)]
    for cp in mC:
        cp.start()
    for b in range(3):
        stage_y(b)
    with sc("small_y"):
        for i in range(2):
            mC[i].wait_recv()
            at = small(i * 2 + core)
            SM[at, :] = (SM[at, :].astype(F32) + SMx[i].astype(F32)).astype(BF)
        mY.start()
    with sc("block_out"):
        for i in range(2):
            yP[i].wait_recv()
            yO[i].wait_recv()
            on = (live[0] > i).astype(F32)
            mix = G[0, i, :sp, :].astype(F32) + YP[i].astype(F32) + YO[i].astype(F32)
            bo_o[i] = ((H[i] + mix) * on).astype(BF)
    cross_first()
    with sc("o_sum"):
        oz.wait_recv()
        rc("oc", 0, GOk.at[0], GOz.at[1], to_far, 0).wait_recv()
        total = GOk[3].astype(F32) + GOz[0].astype(F32) + GOz[1].astype(F32)
        GOk[3] = total.astype(BF)
        outs = [lc(0, GOk.at[3], wo_o)]
        outs[0].start()
    pass_i(1)
    take_i(2)
    stage_x(0)
    with sc("rows_out"):
        for i in range(2):
            gt_o[:, i, :] = DH[i, :seq, :]
    pass_i(2)
    stage_x(1)
    take_i(3)
    stage_x(2)
    with sc("small_x"):
        mY.wait_recv()
        at = small(ep)
        SM[at, :] = (SM[at, :].astype(F32) + SMx[2].astype(F32)).astype(BF)
        mX.start()
    stage_r1(3)

    @pl.when(is_end)
    def _():
        iq(3, 1).start()

    pass_i(3, (0,))
    stage_r1(0)
    stage_r2(3)
    pass_i(3, (1,))
    stage_r1(1)
    stage_r2(0)
    stage_r3(3)
    stage_r1(2)

    @pl.when(is_end)
    def _():
        iz(3).start()

    stage_r2(1)
    stage_r3(0)
    stage_r2(2)
    with sc("small_z"):
        mX.wait_recv()
        total = jnp.transpose(SM[small(ep), :].astype(F32) + SMx[3].astype(F32))
        SZ[0, :, :shard] = total[0:8, :]
        SZ[0, :, shard:] = jnp.zeros((8, LP - shard), F32)
        for cp in mZ:
            cp.start()
    stage_r3(1)
    stage_r3(2)

    @pl.when(is_mid)
    def _():
        iz(3).start()

    for b in (3, 0, 1, 2):
        stage_r4(b)
    for j in range(4):
        with sc("i_sum%d" % j):
            iz(j).wait_recv()
            ic(j, 0).wait_recv()
            total = GIk[j, z].astype(F32) + GIz[0, j].astype(F32) + GIz[1, j].astype(F32)
            if j == 0:
                ix0.wait_recv()
                total = total + GIx[0, 2].astype(F32)
            GIx[j, 3] = total.astype(BF)
            outs.append(lc(1 + j, GIx.at[j, 3], wi_o.at[:, pl.ds(j * width, width)]))
            outs[-1].start()
    with sc("small_sum"):
        for cp in mZ:
            cp.wait_recv()
        sm_o[...] = (SZ[0] + SZ[1] + SZ[2] + SZ[3])[:, :shard]
    for b in (3, 0, 1, 2):
        with sc("wait_ax"):
            cp_ax(b).wait_recv()
            outs.append(lc(5 + b, rest(0, b, 0), sg_o.at[:, half(b, x)]))
            outs[-1].start()
            outs.append(lc(9 + b, rest(1, b, 0), sg_o.at[:, half(b, 1 - x)]))
            outs[-1].start()
    with sc("drain"):
        for cp in dP + dD + dO + yP + yD + yO + [sP, sO, sF, eP, eD, eO, mY, mX] + mC + mZ:
            cp.wait_send()
        for t in range(4):
            ox(t).wait_send()
            (ix(t) if t else ix0).wait_send()
            iz(t).wait_send()
            cp_y(t).wait_send()
            cp_x(t).wait_send()
            cp_ax(t).wait_send()
            for i in range(2):
                cp_c(t, i).wait_send()
        oz.wait_send()
        jz.wait_send()

        @pl.when(is_end)
        def _():
            for t in range(4):
                cp_r1(t).wait_send()
            for t in range(2):
                oq(t).wait_send()
                jq(t).wait_send()
                for j in range(4):
                    iq(j, t).wait_send()

        @pl.when(is_mid)
        def _():
            for t in range(4):
                cp_r2(t).wait_send()
                cp_r3(t).wait_send()
            for t in range(2):
                oc[t].wait_send()
                jc(t).wait_send()
                for j in range(4):
                    ic(j, t).wait_send()

        for cp in outs:
            cp.wait()


def fast_body(n_ep, tokens, live, routes, g1, b1, wqkv, wo, g2, b2, wr, w_in, w_out, cot):
    slots, seq, width = tokens.shape
    sp = (seq + 15) // 16 * 16
    f = w_in.shape[2]
    cap = n_ep * LP
    pads = ((0, 0), (0, sp - seq), (0, 0))
    gl = jnp.pad(cot, pads)
    xb = jnp.pad(tokens, pads)
    sds = jax.ShapeDtypeStruct
    vm = pl.BlockSpec(memory_space=pltpu.VMEM)
    anys = pl.BlockSpec(memory_space=pl.ANY)
    b = lambda *shape: pltpu.VMEM(shape, BF)
    g = lambda *shape: pltpu.VMEM(shape, F32)
    shard = width // n_ep
    bo, gt, sm, wo_t, wi, sg, _, _, _ = pl.pallas_call(
        functools.partial(layer_kernel, n_ep, seq),
        name="layer",
        out_shape=(
            sds((slots, sp, width), BF), sds((seq, slots, width), F32), sds((8, shard), F32),
            sds((width, f // 8), BF), sds((width // 8, f), BF), sds((shard, 4 * width), BF),
            sds((2 * sp, 4 * width), BF), sds((2 * sp, width), BF), sds((2 * sp, width), BF),
        ),
        in_specs=[pl.BlockSpec(memory_space=pltpu.SMEM)] + [vm] * 6 + [anys] * 6,
        out_specs=[vm] * 3 + [anys] * 6,
        scratch_shapes=[
            b(4, 2, LP, width), b(4, 2, LP, width), g(4, 2, 8, LP), b(128, width), b(width, f), b(f, width),
            b(cap, f), b(cap, f), b(cap, width), b(cap, width), b(width, cap),
            b(4, width, f // 8), b(4, width, f // 8), b(4, width, f // 8), b(2, width, f // 8),
            b(4, 4, width // 8, width), b(4, 4, width // 8, width), b(4, 4, width // 8, width),
            b(2, 4, width // 8, width), b(4, width // 8, width),
            g(slots, sp, width), g(slots, sp, width), g(slots, sp, 128), g(cap, 2),
            b(2, sp, width), b(2, sp, width), b(2, sp, width),
            b(2, LP, 128), b(2, LP, 128), b(2, LP, 128), b(4, 2, LP, 128),
            b(2, sp, width), b(2, sp, width), b(2, sp, width), b(width, 128), b(4, shard, 128), g(4, 8, LP),
            pltpu.SemaphoreType.DMA((N_COPIES,)), pltpu.SemaphoreType.DMA((N_COPIES,)),
            pltpu.SemaphoreType.DMA((14,)), pltpu.SemaphoreType.REGULAR, pltpu.SemaphoreType.REGULAR((2,)),
        ],
        compiler_params=pltpu.CompilerParams(
            collective_id=0, has_side_effects=True, vmem_limit_bytes=67043328),
    )(live, jnp.transpose(routes, (0, 2, 1)), g1, b1, g2, b2, jnp.transpose(wr), xb, gl, w_in, w_out, wqkv, wo)
    return (
        bo[:, :seq], jnp.transpose(gt, (1, 0, 2)), sm[4], sm[5], sg[:, :3 * width].astype(F32), sg[:, 3 * width:].astype(F32),
        sm[6], sm[7], jnp.transpose(sm[:n_ep]), wi.astype(F32)[None], jnp.transpose(wo_t).astype(F32)[None],
    )


def general_body(
    tokens,
    live_images,
    routes,
    ln1_gain,
    ln1_bias,
    query_key_value_weight,
    attention_output_weight,
    ln2_gain,
    ln2_bias,
    w_router,
    w_in,
    w_out,
    cotangent,
):
    slot_count, seq_len, model_width = tokens.shape
    row_count = slot_count * seq_len
    expert_count = w_router.shape[1]
    hidden_width = w_in.shape[2]
    capacity = ((2 * row_count + expert_count - 1) // expert_count * 5 // 4 + 7) // 8 * 8
    scaling = HEAD_DIM ** (-0.5)
    inputs = tokens.astype(jnp.float32).reshape(row_count, model_width)
    normed1, inverse1 = norm_parts(inputs)
    attn_in = (normed1 * ln1_gain + ln1_bias).astype(jnp.bfloat16)
    qkv_rows = jnp.dot(attn_in, query_key_value_weight, preferred_element_type=jnp.float32).astype(
        jnp.bfloat16
    )
    qkv_heads = qkv_rows.reshape(slot_count, seq_len, 3, HEADS, HEAD_DIM)
    queries = qkv_heads[:, :, 0]
    keys_all = qkv_heads[:, :, 1]
    values_all = qkv_heads[:, :, 2]
    scores = (
        jnp.einsum("sqhc,skhc->shqk", queries, keys_all, preferred_element_type=jnp.float32)
        * scaling
    )
    row_peak = jnp.max(scores, axis=-1, keepdims=True)
    raised = jnp.exp(scores - row_peak)
    totals = jnp.sum(raised, axis=-1, keepdims=True)
    log_total = row_peak + jnp.log(totals)
    weights = (raised / totals).astype(jnp.bfloat16)
    attended_context = jnp.einsum(
        "shqk,skhc->sqhc", weights, values_all, preferred_element_type=jnp.float32
    )
    attended_context = attended_context.astype(jnp.bfloat16).reshape(row_count, model_width)
    hidden1 = inputs + jnp.dot(
        attended_context, attention_output_weight, preferred_element_type=jnp.float32
    )
    normed2, inverse2 = norm_parts(hidden1)
    moe_in = (normed2 * ln2_gain + ln2_bias).astype(jnp.bfloat16)
    router = jax.nn.softmax(jnp.dot(moe_in, w_router, preferred_element_type=jnp.float32), axis=-1)
    chosen = routes.reshape(row_count, 2)
    expert_ids = jnp.arange(expert_count, dtype=jnp.int32)
    picked = (chosen[:, :, None] == expert_ids[None, None, :]).astype(jnp.float32)
    gates = jnp.sum(picked * router[:, None, :], axis=-1)
    token_live = (jnp.arange(row_count, dtype=jnp.int32) // seq_len < live_images[0]).astype(
        jnp.float32
    )
    pair_ids = chosen.reshape(2 * row_count)
    pair_live = jnp.repeat(token_live, 2) > 0.5
    member = ((pair_ids[:, None] == expert_ids[None, :]) & pair_live[:, None]).astype(jnp.int32)
    position = jnp.sum((jnp.cumsum(member, axis=0) - 1) * member, axis=-1)
    slot_ids = jnp.where(pair_live, pair_ids * capacity + position, -1).reshape(row_count, 2)
    lanes = jnp.arange(expert_count * capacity, dtype=jnp.int32)
    placing = (jnp.transpose(slot_ids)[:, None, :] == lanes[None, :, None]).astype(jnp.bfloat16)
    outbox = jnp.einsum("jsr,rd->sd", placing, moe_in, preferred_element_type=jnp.float32)
    outbox = outbox.astype(jnp.bfloat16).reshape(expert_count, capacity, model_width)
    inbox = lax.all_to_all(outbox, "ep", split_axis=0, concat_axis=0, tiled=True)
    flat_in = inbox.reshape(-1, model_width)
    pre_act = jnp.dot(flat_in, w_in[0], preferred_element_type=jnp.float32)
    activated = jax.nn.gelu(pre_act).astype(jnp.bfloat16)
    produced = jnp.dot(activated, w_out[0], preferred_element_type=jnp.float32).astype(jnp.bfloat16)
    coming_back = lax.all_to_all(
        produced.reshape(inbox.shape), "ep", split_axis=0, concat_axis=0, tiled=True
    )
    coming_back, pre_act = (
        coming_back,
        pre_act.reshape(inbox.shape[0], inbox.shape[1], hidden_width),
    )
    arrived_rows = inbox.reshape(-1, model_width)
    pre_rows = pre_act.reshape(-1, hidden_width)
    returned_rows = coming_back.reshape(expert_count * capacity, model_width)
    taken = jnp.einsum("jsr,sd->rjd", placing, returned_rows, preferred_element_type=jnp.float32)
    mixture = jnp.sum(gates[:, :, None] * taken, axis=1)
    block_out = (
        ((hidden1 + mixture) * token_live[:, None]).astype(jnp.bfloat16).reshape(tokens.shape)
    )
    upstream = cotangent.astype(jnp.float32).reshape(row_count, model_width) * token_live[:, None]
    gate_grads = jnp.sum(taken * upstream[:, None, :], axis=-1)
    sent_grads = (gates[:, :, None] * upstream[:, None, :]).astype(jnp.bfloat16)
    grad_outbox = jnp.einsum("jsr,rjd->sd", placing, sent_grads, preferred_element_type=jnp.float32)
    grad_outbox = grad_outbox.astype(jnp.bfloat16).reshape(expert_count, capacity, model_width)
    grad_inbox = lax.all_to_all(grad_outbox, "ep", split_axis=0, concat_axis=0, tiled=True)
    grad_rows = grad_inbox.reshape(-1, model_width)
    activated_rows, gelu_pull = jax.vjp(jax.nn.gelu, pre_rows)
    activated_low = activated_rows.astype(jnp.bfloat16)
    grad_activated = jnp.einsum(
        "rd,fd->rf", grad_rows, w_out[0], preferred_element_type=jnp.float32
    )
    grad_pre = gelu_pull(grad_activated)[0].astype(jnp.bfloat16)
    columns = activated_low
    grad_w_out = lax.psum_scatter(
        jnp.einsum("rf,rd->fd", columns, grad_rows, preferred_element_type=jnp.float32).astype(
            jnp.bfloat16
        ),
        "dp",
        scatter_dimension=0,
        tiled=True,
    ).astype(jnp.float32)
    grad_back_rows = jnp.einsum(
        "rf,df->rd", grad_pre, w_in[0], preferred_element_type=jnp.float32
    ).astype(jnp.bfloat16)
    grad_back = lax.all_to_all(
        grad_back_rows.reshape(grad_inbox.shape), "ep", split_axis=0, concat_axis=0, tiled=True
    )
    columns = arrived_rows
    grad_w_in = lax.psum_scatter(
        jnp.einsum("rd,rf->df", columns, grad_pre, preferred_element_type=jnp.float32).astype(
            jnp.bfloat16
        ),
        "dp",
        scatter_dimension=0,
        tiled=True,
    ).astype(jnp.float32)
    grad_back_flat = grad_back.reshape(expert_count * capacity, model_width)
    expert_grad = jnp.einsum(
        "jsr,sd->rd", placing, grad_back_flat, preferred_element_type=jnp.float32
    )
    grad_router_probs = jnp.sum(gate_grads[:, :, None] * picked, axis=1)
    grad_logits = router * (
        grad_router_probs - jnp.sum(router * grad_router_probs, axis=-1, keepdims=True)
    )
    grad_logits = grad_logits.astype(jnp.bfloat16)
    grad_w_router = jnp.einsum("rd,re->de", moe_in, grad_logits, preferred_element_type=jnp.float32)
    grad_moe_in = expert_grad + jnp.einsum(
        "re,de->rd", grad_logits, w_router, preferred_element_type=jnp.float32
    )
    grad_ln2_gain = jnp.sum(grad_moe_in * normed2, axis=0)
    grad_ln2_bias = jnp.sum(grad_moe_in, axis=0)
    grad_hidden1 = upstream + norm_backward(grad_moe_in * ln2_gain, normed2, inverse2)
    grad_attn = grad_hidden1.astype(jnp.bfloat16)
    grad_w_attn_out = jnp.einsum(
        "rd,re->de", attended_context, grad_attn, preferred_element_type=jnp.float32
    )
    grad_context = jnp.einsum(
        "re,de->rd", grad_attn, attention_output_weight, preferred_element_type=jnp.float32
    )
    grad_context = grad_context.astype(jnp.bfloat16).reshape(slot_count, seq_len, HEADS, HEAD_DIM)
    again = (
        jnp.einsum("sqhc,skhc->shqk", queries, keys_all, preferred_element_type=jnp.float32)
        * scaling
    )
    probs_again = jnp.exp(again - log_total)
    probs_low = probs_again.astype(jnp.bfloat16)
    grad_values = jnp.einsum(
        "shqk,sqhc->skhc", probs_low, grad_context, preferred_element_type=jnp.float32
    )
    grad_probs = jnp.einsum(
        "sqhc,skhc->shqk", grad_context, values_all, preferred_element_type=jnp.float32
    )
    grad_scores = probs_again * (
        grad_probs - jnp.sum(probs_again * grad_probs, axis=-1, keepdims=True)
    )
    grad_scores = grad_scores.astype(jnp.bfloat16)
    grad_queries = (
        jnp.einsum("shqk,skhc->sqhc", grad_scores, keys_all, preferred_element_type=jnp.float32)
        * scaling
    )
    grad_keys = (
        jnp.einsum("shqk,sqhc->skhc", grad_scores, queries, preferred_element_type=jnp.float32)
        * scaling
    )
    grad_qkv = (
        jnp.stack([grad_queries, grad_keys, grad_values], axis=2)
        .astype(jnp.bfloat16)
        .reshape(row_count, 3 * model_width)
    )
    grad_w_qkv = jnp.einsum("rd,re->de", attn_in, grad_qkv, preferred_element_type=jnp.float32)
    grad_attn_in = jnp.einsum(
        "re,de->rd", grad_qkv, query_key_value_weight, preferred_element_type=jnp.float32
    )
    grad_ln1_gain = jnp.sum(grad_attn_in * normed1, axis=0)
    grad_ln1_bias = jnp.sum(grad_attn_in, axis=0)
    grad_inputs = grad_hidden1 + norm_backward(grad_attn_in * ln1_gain, normed1, inverse1)
    shared = (
        grad_w_qkv,
        grad_w_attn_out,
        grad_w_router,
        grad_ln1_gain,
        grad_ln1_bias,
        grad_ln2_gain,
        grad_ln2_bias,
    )
    partial_sums = (
        lax.psum_scatter(
            shared[0].astype(jnp.bfloat16), "ep", scatter_dimension=0, tiled=True
        ).astype(jnp.float32),
        lax.psum_scatter(
            shared[1].astype(jnp.bfloat16), "ep", scatter_dimension=0, tiled=True
        ).astype(jnp.float32),
        lax.psum_scatter(
            shared[2].astype(jnp.bfloat16), "ep", scatter_dimension=0, tiled=True
        ).astype(jnp.float32),
        lax.psum_scatter(
            shared[3].astype(jnp.bfloat16), "ep", scatter_dimension=0, tiled=True
        ).astype(jnp.float32),
        lax.psum_scatter(
            shared[4].astype(jnp.bfloat16), "ep", scatter_dimension=0, tiled=True
        ).astype(jnp.float32),
        lax.psum_scatter(
            shared[5].astype(jnp.bfloat16), "ep", scatter_dimension=0, tiled=True
        ).astype(jnp.float32),
        lax.psum_scatter(
            shared[6].astype(jnp.bfloat16), "ep", scatter_dimension=0, tiled=True
        ).astype(jnp.float32),
    )
    shares = (
        lax.psum(partial_sums[0].astype(jnp.bfloat16), "dp").astype(jnp.float32),
        lax.psum(partial_sums[1].astype(jnp.bfloat16), "dp").astype(jnp.float32),
        lax.psum(partial_sums[2].astype(jnp.bfloat16), "dp").astype(jnp.float32),
        lax.psum(partial_sums[3].astype(jnp.bfloat16), "dp").astype(jnp.float32),
        lax.psum(partial_sums[4].astype(jnp.bfloat16), "dp").astype(jnp.float32),
        lax.psum(partial_sums[5].astype(jnp.bfloat16), "dp").astype(jnp.float32),
        lax.psum(partial_sums[6].astype(jnp.bfloat16), "dp").astype(jnp.float32),
    )
    return (
        block_out,
        grad_inputs.reshape(tokens.shape),
        shares[3],
        shares[4],
        shares[0],
        shares[1],
        shares[5],
        shares[6],
        shares[2],
        grad_w_in[None],
        grad_w_out[None],
    )


def solution(mesh):
    in_specs = (
        P(("dp", "ep"), None, None),
        P(("dp", "ep")),
        P(("dp", "ep"), None, None),
        P(),
        P(),
        P(),
        P(),
        P(),
        P(),
        P(),
        P("ep", None, None),
        P("ep", None, None),
        P(("dp", "ep"), None, None),
    )
    out_specs = (
        P(("dp", "ep"), None, None),
        P(("dp", "ep"), None, None),
        P("ep"),
        P("ep"),
        P("ep", None),
        P("ep", None),
        P("ep"),
        P("ep"),
        P("ep", None),
        P("ep", "dp", None),
        P("ep", "dp", None),
    )
    n_dp, n_ep = mesh.shape["dp"], mesh.shape["ep"]
    body = functools.partial(fast_body, n_ep) if (n_dp, n_ep) == (8, 4) else general_body
    return jax.shard_map(body, mesh=mesh, in_specs=in_specs, out_specs=out_specs, check_vma=False)
```
